32 devices in a mesh: band: 8 (over z, y), grid: 4 (over x, core).
Axes of the slice: x: 2, y: 2, z: 4, core: 2. Of those that a mesh axis runs over, the one named last changes fastest.
Arguments:
- orbitals: float32 [32, 110592], P('band', 'grid'), may hold values from -6 to 6
Outputs:
- exchange_vectors: float32 [32, 110592], P('band', 'grid')
- margin: float32 [32, 32], P('grid', 'band')
The draws below stay inside these ranges and needn't reach their ends.
All inputs are finite; a program needn't handle non-finite values.
Results may differ from the reference program's by a relative error of at most 0.00012.
Values sent between devices are 32-bit elements; how exact they have to be, the bound alone decides.
A program may use at most 128 MiB of HBM per device.

```python
import jax
import jax.numpy as jnp
from jax import lax

NG = 48
BAND_DEV = 4
NBANDS = 32
NCELL = 110592
N_BAND = 8


def steps_of(rng, dims, split, least, top_value):
    gain, own = 1.0, jax.random.fold_in(rng, 6)
    for position, shards_of in split:
        heights = jnp.exp(jax.random.uniform(jax.random.fold_in(own, position), (shards_of,), jnp.float32, least / len(split), top_value / len(split)))
        gain = gain * jnp.repeat(heights, dims[position] // shards_of).reshape([-1 if axis == position else 1 for axis in range(len(dims))])
    return gain


def normal_values(stream_key, shape, deviation, reach, split=(), kind=jnp.bfloat16):
    result = jax.random.normal(stream_key, shape, jnp.float32) * deviation
    if len(split) > 0:
        result = steps_of(stream_key, shape, split, -0.22, 0.18) * result
    return jnp.clip(result, min=-reach, max=reach).astype(kind)


def setup_inputs(seed: int = 0) -> dict:
    streams_of = jax.random.split(jax.random.key(seed), 2)
    orbitals = normal_values(streams_of[0], (NBANDS, NCELL), 1.0, 6.0, ((0, 8), (1, 4)), jnp.float32)
    return dict(orbitals=orbitals)


def folded_freq(count):
    indices = jnp.arange(count)
    return ((indices + count // 2) % count - count // 2).astype(jnp.float32)


def kernel_table():
    freqs = folded_freq(NG)
    squares = freqs[:, None, None] ** 2 + freqs[None, :, None] ** 2 + freqs[None, None, :] ** 2
    safe_sq = jnp.where(squares > 0, squares, jnp.float32(1.0))
    return jnp.where(squares > 0, 40.0 * (1.0 - jnp.exp(-squares / 16.0)) / safe_sq, jnp.float32(0.0))


def reference(orbitals):
    kernel = kernel_table()
    blocks = orbitals.reshape(N_BAND, BAND_DEV, NCELL)
    window = jnp.concatenate([blocks, jnp.roll(blocks, 1, axis=0), jnp.roll(blocks, -1, axis=0)], axis=1)

    def per_band(single, partners):
        density = (single[None, :] * partners).reshape(-1, NG, NG, NG)
        spectrum = jnp.fft.fftn(density, axes=(1, 2, 3))
        potential = jnp.real(jnp.fft.ifftn(spectrum * kernel, axes=(1, 2, 3))).reshape(-1, NCELL)
        return -jnp.sum(partners * potential, axis=0)

    def per_block(args):
        own_block, partners = args
        return lax.map(lambda single: per_band(single, partners), own_block)

    vectors = lax.map(per_block, (blocks, window)).reshape(NBANDS, NCELL).astype(jnp.float32)
    margin = jnp.dot(orbitals, vectors.T, precision=lax.Precision.HIGHEST, preferred_element_type=jnp.float32) / NCELL
    return vectors, margin
```

```python
import functools

import jax
import jax.numpy as jnp
import numpy as np
from jax import lax
from jax.experimental import pallas as pl
from jax.experimental.pallas import tpu as pltpu
from jax.sharding import PartitionSpec as P


def kernel_values(ng):
    freqs = ((np.arange(ng) + ng // 2) % ng - ng // 2).astype(np.float32)
    sq = freqs[: ng // 2 + 1, None, None] ** 2 + freqs[None, :, None] ** 2 + freqs[None, None, :] ** 2
    safe = np.where(sq > 0, sq, np.float32(1.0))
    return np.where(sq > 0, 40.0 * (1.0 - np.exp(-sq / 16.0)) / safe, 0.0)


def hartley(ng):
    k = np.arange(ng)
    ang = (k[:, None] * k[None, :] % ng) * (2.0 * np.pi / ng)
    return np.cos(ang) + np.sin(ang)


def split_const(table):
    table = np.asarray(table, np.float32)
    hi = table.astype(jnp.bfloat16)
    lo = (table - hi.astype(np.float32)).astype(jnp.bfloat16)
    return hi, lo


def rfft(xs):
    n = len(xs)
    if n == 3:
        s = xs[1] + xs[2]
        d = xs[1] - xs[2]
        return [(xs[0] + s, None), (xs[0] - 0.5 * s, d * (-np.sqrt(3.0) / 2))]
    even, odd = rfft(xs[0::2]), rfft(xs[1::2])
    half = n // 2
    out = [None] * (half + 1)
    for k in range(half // 2 + 1):
        er, ei = even[k]
        orr, oi = odd[k]
        if k == 0:
            out[0] = (er + orr, None)
            out[half] = (er - orr, None)
            continue
        c, s = np.cos(2 * np.pi * k / n), -np.sin(2 * np.pi * k / n)
        if 2 * k == half:
            out[k] = (er, -orr)
            continue
        tr, ti = cmul(orr, oi, c, s)
        out[k] = (er + tr, addo(ei, ti))
        out[half - k] = (er - tr, subo(ti, ei))
    return out


def addo(a, b):
    return b if a is None else a + b


def subo(a, b):
    return a if b is None else a - b


def cmul(r, i, c, s):
    if i is None:
        return r * c, r * s
    if abs(abs(c) - abs(s)) < 1e-9:
        if s < 0 < c:
            return (r + i) * c, (i - r) * c
        return (r - i) * c, (r + i) * c
    return r * c - i * s, r * s + i * c


def irfft(spec, n):
    if n == 3:
        dc, (r, i) = spec[0][0], spec[1]
        base = dc - r
        t = i * np.sqrt(3.0)
        return [dc + 2.0 * r, base - t, base + t]
    half = n // 2
    even, odd = [None] * (half // 2 + 1), [None] * (half // 2 + 1)
    for k in range(half // 2 + 1):
        yr, yi = spec[k]
        if k == 0:
            hr = spec[half][0]
            even[0] = (yr + hr, None)
            odd[0] = (yr - hr, None)
            continue
        if 2 * k == half:
            even[k] = (yr + yr, None)
            odd[k] = (-(yi + yi), None)
            continue
        zr, zi = spec[half - k]
        er, ei = yr + zr, yi - zi
        dr, di = yr - zr, yi + zi
        c, s = np.cos(2 * np.pi * k / n), np.sin(2 * np.pi * k / n)
        even[k] = (er, ei)
        odd[k] = cmul(dr, di, c, s)
    ev, od = irfft(even, half), irfft(odd, half)
    out = [None] * n
    out[0::2], out[1::2] = ev, od
    return out


def split(v):
    hi = v.astype(jnp.bfloat16)
    lo = (v - hi.astype(jnp.float32)).astype(jnp.bfloat16)
    return hi, lo


def mm(a, b):
    return jnp.dot(a, b, preferred_element_type=jnp.float32)


def solve_kernel(ng, ncell, own_ref, k1_ref, k2_ref, zt_ref, ty_ref, cp_ref, s_ref, st_ref, hot_ref,
                 o_ref, m_ref, store, amp, acc, work, vec, recv, sel, rows_buf, mine, marg,
                 rsem, ssem, gsem, ysem, usem, dsem, wsem, osem, orsem, msem, mrsem, lsem):
    planes, _, width = own_ref.shape
    groups = vec.shape[0]
    me = lax.axis_index("grid")
    band, nband = lax.axis_index("band"), lax.axis_size("band")
    chip, core = me // 2, me % 2
    sib = chip * 2 + (1 - core)
    cross = (1 - chip) * 2 + core
    far = (1 - chip) * 2 + (1 - core)
    length = nband // 2
    side, pos = band % 2, band // 2
    pair = band + 1 - 2 * side
    third = (band + nband - 1 + 2 * side) % nband
    first, last = band == 0, band == nband - 1
    ends = jnp.logical_or(first, last)
    wrap = jnp.where(first, nband - 1, 0)
    has_up, has_down = pos < length - 1, pos > 0
    up, down = jnp.where(has_up, band + 2, band), jnp.where(has_down, band - 2, band)
    mesh_id = pl.DeviceIdType.MESH
    flat = planes * ng

    def remote(src, dst, send, recv_sem, device):
        return pltpu.make_async_remote_copy(
            src_ref=src, dst_ref=dst, send_sem=send, recv_sem=recv_sem,
            device_id=device, device_id_type=mesh_id,
        )

    def partner(blk):
        return jnp.where(blk == 0, band, jnp.where(blk == 1, pair, third))

    def place(blk, slot):
        return jnp.where(slot == me, partner(blk), nband + blk * groups + slot)

    def share(blk, lane, slot, src, target):
        return remote(src, store.at[nband + blk * groups + slot], ssem.at[blk, lane], rsem.at[blk, slot], (band, target))

    def along(block, sems, device):
        return remote(store.at[block], store.at[block], sems.at[block], gsem.at[block], (device, me))

    def came(block):
        along(block, ysem, pair).wait_recv()

    def greet(device):
        pl.semaphore_signal(barrier, inc=1, device_id=device, device_id_type=mesh_id)

    barrier = pltpu.get_barrier_semaphore()
    for device in ((band, sib), (band, cross), (band, far), (pair, me)):
        greet(device)

    @pl.when(has_up)
    def _():
        greet((up, me))

    @pl.when(has_down)
    def _():
        greet((down, me))

    @pl.when(ends)
    def _():
        greet((wrap, me))

    count = 4 + has_up.astype(jnp.int32) + has_down.astype(jnp.int32) + ends.astype(jnp.int32)
    pl.semaphore_wait(barrier, count)

    def start_own(sems, device):
        return remote(own_ref, store.at[band], sems.at[band], gsem.at[band], (device, me))

    share(0, 1, me, own_ref, cross).start()
    share(0, 0, me, own_ref, sib).start()
    start_own(ysem, pair).start()

    @pl.when(ends)
    def _():
        start_own(wsem, wrap).start()

    @pl.when(has_up)
    def _():
        start_own(usem, up).start()

    @pl.when(has_down)
    def _():
        start_own(dsem, down).start()

    local = pltpu.make_async_copy(own_ref, store.at[band], lsem)
    local.start()

    def arrived(blk, slot):
        share(blk, 0, slot, own_ref, sib).wait_recv()

    def relay(blk):
        arrived(blk, cross)
        share(blk, 2, cross, store.at[nband + blk * groups + cross], sib).start()

    def spread(blk):
        came(partner(blk))
        share(blk, 1, me, store.at[partner(blk)], cross).start()
        share(blk, 0, me, store.at[partner(blk)], sib).start()

    def skipped(block):
        return jnp.logical_or(
            jnp.logical_and(pair == 0, block == nband - 1), jnp.logical_and(pair == nband - 1, block == 0)
        )

    def line(d, act):
        lower, upper = band - 2 * d, band + 2 * d
        has_lower, has_upper = pos - d >= 0, pos + d <= length - 1

        def pass_on(block, exists, on, sems, device):
            @pl.when(exists)
            def _():
                if act == "go":
                    came(block)

                @pl.when(on)
                def _():
                    copy = along(block, sems, device)
                    copy.start() if act == "go" else copy.wait_send()

                @pl.when(jnp.logical_not(skipped(block)))
                def _():
                    copy = along(block, ysem, pair)
                    copy.start() if act == "go" else copy.wait_send()

        @pl.when(side == 1)
        def _():
            pass_on(lower, has_lower, has_up, usem, up)
            pass_on(upper, has_upper, has_down, dsem, down)

        @pl.when(side == 0)
        def _():
            pass_on(upper, has_upper, has_down, dsem, down)
            pass_on(lower, has_lower, has_up, usem, up)

    def ztrans(v):
        hi, lo = split(v)
        parts = []
        for h in range(2):
            a, b = (jnp.concatenate([t[:, 128 * h:128 * h + 128], t[:, 256:]], axis=1) for t in (hi, lo))
            parts.append(mm(a, zt_ref[h, 0]) + mm(b, zt_ref[h, 0]) + mm(a, zt_ref[h, 1]))
        return jnp.concatenate([parts[0][:, :128], parts[1][:, :128], parts[0][:, 128:] + parts[1][:, 128:]], axis=1)

    def ytrans(v):
        hi, lo = split(v)
        return mm(ty_ref[...], jnp.concatenate([hi, lo, hi], axis=0))

    def slot_of(s):
        return ((chip + s // 2) % 2) * 2 + (core + s % 2) % 2

    def amplitude(slot):
        hi, lo = split(store[place(0, slot)].reshape(flat, width))
        parts = []
        for h in range(2):
            a, b = (jnp.concatenate([t[:, 128 * h:128 * h + 128], t[:, 256:]], axis=1) for t in (hi, lo))
            parts.append(mm(a, sel[h]) + mm(b, sel[h]))
        out = jnp.concatenate([parts[0][:, :128], parts[1][:, :128], parts[0][:, 128:] + parts[1][:, 128:]], axis=1)
        amp[slot] = out.reshape(planes, ng, width)

    for h in range(2):
        mark = (me + 1).astype(jnp.float32)
        sel[h] = jnp.where(cp_ref[h].astype(jnp.float32) == mark, 1.0, 0.0).astype(jnp.bfloat16)

    def forward(blk, s):
        slot = slot_of(s)

        @pl.when(s == 1)
        def _():
            arrived(blk, sib)

        @pl.when(s == 2)
        def _():
            relay(blk)

            @pl.when(blk == 0)
            def _():
                spread(1)
                line(1, "go")

            @pl.when(blk == 1)
            def _():
                spread(2)
                line(2, "go")

        @pl.when(s == 3)
        def _():
            arrived(blk, far)

        @pl.when(blk == 0)
        def _():
            amplitude(slot)

        p = (amp[slot] * store[place(blk, slot)]).reshape(flat, width)
        q = ztrans(p).reshape(planes, ng, width)
        for r in range(planes):
            work[slot, r] = ytrans(q[r])

    def conv(vals, kern):
        spec = rfft(vals)
        out = []
        for k, (re, im) in enumerate(spec):
            kv = kern(k)
            out.append((re * kv, None if im is None else im * kv))
        return irfft(out, ng)

    def xconv(t):
        order = [(g, h, r) for g in range(4) for h in range(2) for r in range(planes)]
        for i in range(2):
            rows = pl.ds(pl.multiple_of(t * 16 + 8 * i, 8), 8)
            res = conv([work[g, r, rows, h * 128:h * 128 + 128] for g, h, r in order],
                       lambda k: k1_ref[k, rows, :])
            for (g, h, r), v in zip(order, res):
                work[g, r, rows, h * 128:h * 128 + 128] = v
        ra = pl.ds(pl.multiple_of(t * 16, 8), 8)
        rb = pl.ds(pl.multiple_of(t * 16 + 8, 8), 8)
        left = lax.broadcasted_iota(jnp.int32, (8, 128), 1) < 64

        def half(g, h, r):
            u, w = work[g, r, ra, 256:384], work[g, r, rb, 256:384]
            if h == 0:
                return jnp.where(left, u, pltpu.roll(w, 64, 1))
            return jnp.where(left, pltpu.roll(u, 64, 1), w)

        rk = pl.ds(pl.multiple_of(t * 8, 8), 8)
        res = dict(zip(order, conv([half(*o) for o in order], lambda k: k2_ref[k, rk, :])))
        for g in range(4):
            for r in range(planes):
                a, b = res[(g, 0, r)], res[(g, 1, r)]
                work[g, r, ra, 256:384] = jnp.where(left, a, pltpu.roll(b, 64, 1))
                work[g, r, rb, 256:384] = jnp.where(left, pltpu.roll(a, 64, 1), b)

    def push(slot):
        return remote(vec.at[slot], recv.at[me], osem.at[slot], orsem.at[me], (band, slot))

    def inverse(blk, s):
        slot = ((chip + 1 - s // 2) % 2) * 2 + (core + s % 2 + s // 2) % 2
        q = jnp.concatenate([ytrans(work[slot, r]) for r in range(planes)], axis=0)
        w = ztrans(q).reshape(planes, ng, width) * store[place(blk, slot)]

        @pl.when(blk == 0)
        def _():
            acc[slot] = w

        @pl.when(blk == 1)
        def _():
            acc[slot] += w

        @pl.when(blk == 2)
        def _():
            hi, lo = split((acc[slot] + w).reshape(flat, width))
            out = -(mm(hi, s_ref[...]) + mm(lo, s_ref[...]))
            vec[slot] = out.reshape(planes, ng, s_ref.shape[-1])

            @pl.when(s < 3)
            def _():
                push(slot).start()

    def block(blk, _):
        @pl.when(blk == 0)
        def _():
            local.wait()

        def fwd(s, _):
            forward(blk, s)
            return 0

        def mid(t, _):
            xconv(t)
            return 0

        def inv(s, _):
            inverse(blk, s)
            return 0

        lax.fori_loop(0, 4, fwd, 0)

        @pl.when(blk == 2)
        def _():
            def more(d, _):
                line(d, "go")
                return 0

            lax.fori_loop(3, length, more, 0)

        lax.fori_loop(0, ng // 16, mid, 0)
        lax.fori_loop(0, 4, inv, 0)
        return 0

    lax.fori_loop(0, 3, block, 0)

    def settle(block, _):
        known = jnp.logical_or(block == band, jnp.logical_or(block == pair, block == third))
        relayed = block % 2 == side

        @pl.when(jnp.logical_not(jnp.logical_or(known, relayed)))
        def _():
            came(block)

        return 0

    lax.fori_loop(0, nband, settle, 0)

    def spread_out(v):
        hi, lo = split(v.reshape(flat, v.shape[-1]))
        return (mm(hi, st_ref[...]) + mm(lo, st_ref[...])).reshape(planes, ng, width)

    def column(slot):
        amp[0] = spread_out(o_ref[slot])

        def one(block, _):
            total = jnp.sum(store[block].reshape(flat // 8, 8, width) * amp[0].reshape(flat // 8, 8, width), axis=0)
            rows_buf[block, slot] = total
            return 0

        lax.fori_loop(0, nband, one, 0)

    o_ref[me] = vec[me]
    column(me)
    for slot in (sib, cross, far):
        remote(vec.at[slot], recv.at[slot], osem.at[slot], orsem.at[slot], (band, slot)).wait()
        o_ref[slot] = recv[slot]
        column(slot)

    lanes = jnp.sum(rows_buf[...], axis=2).reshape(groups * nband, width)
    rest = lanes
    terms = jnp.zeros((groups * nband, hot_ref.shape[-1]), jnp.float32)
    for _ in range(3):
        hi = rest.astype(jnp.bfloat16)
        terms += mm(hi, hot_ref[...])
        rest = rest - hi.astype(jnp.float32)
    mine[...] = (terms / ncell).reshape(groups, nband, terms.shape[-1])

    def give(slot):
        return remote(mine.at[slot], marg.at[me], msem.at[slot], mrsem.at[me], (band, slot))

    for slot in (cross, far, sib):
        give(slot).start()
    total = mine[me]
    for slot in (sib, cross, far):
        remote(mine.at[slot], marg.at[slot], msem.at[slot], mrsem.at[slot], (band, slot)).wait()
        total += marg[slot]
    m_ref[...] = total

    for blk in range(3):
        for lane, target in ((0, sib), (1, cross), (2, sib)):
            share(blk, lane, me, own_ref, target).wait_send()
    start_own(ysem, pair).wait_send()

    @pl.when(ends)
    def _():
        start_own(wsem, wrap).wait_send()

    @pl.when(has_up)
    def _():
        start_own(usem, up).wait_send()

    @pl.when(has_down)
    def _():
        start_own(dsem, down).wait_send()

    def finish(d, _):
        line(d, "end")
        return 0

    lax.fori_loop(1, length, finish, 0)


def lane_tables(ng, bands):
    w = bands * ng
    half, bz = [], []
    for lo, hi in ((0, 128), (128, w)):
        for h in range(2):
            half.append(np.full(hi - lo, h))
            bz.append(np.arange(lo, hi))
    half, bz = np.concatenate(half), np.concatenate(bz)
    return half, bz // ng, bz % ng


def tiles(table, half):
    out = []
    for h in range(2):
        pick = np.concatenate([np.arange(128 * h, 128 * h + 128), np.arange(256, len(half))])
        live = half[pick] == h
        out.append(np.where(live[:, None] & live[None, :], table[pick][:, pick], 0.0))
    return np.stack(out)


def solve(own, bands, groups, nband):
    planes, ng, width = own.shape
    half, bnd, zed = lane_tables(ng, bands)
    ht = hartley(ng)
    th, tl = split_const(ht)
    same = (half[:, None] == half[None, :])
    zmat = np.where(same & (bnd[:, None] == bnd[None, :]), ht[zed[:, None], zed[None, :]], 0.0)
    zt = np.stack(split_const(tiles(zmat, half)), axis=1)
    ty = np.concatenate([th, th, tl], axis=1)
    cp = tiles(np.where(same & (zed[:, None] == zed[None, :]), bnd[:, None] + 1.0, 0.0), half)
    s = np.zeros((width, 128), np.float32)
    s[np.arange(width), half * ng + zed] = 1.0
    hot = np.zeros((width, 128), np.float32)
    hot[np.arange(width), bnd] = 1.0
    kv = kernel_values(ng).astype(np.float32) / np.float32(ng**3)
    kb = np.tile(kv, (1, 1, bands))
    k1 = kb[:, :, :128]
    rest = kb[:, :, 128:].reshape(kb.shape[0], ng // 16, 2, 8, 64)
    k2 = np.concatenate([rest[:, :, 0], rest[:, :, 1]], axis=-1).reshape(kb.shape[0], ng // 2, 128)
    b16 = jnp.bfloat16
    consts = [k1, k2, zt, ty, cp.astype(b16), s.astype(b16), s.T.astype(b16), hot.astype(b16)]
    full = (groups, planes, ng, width)
    f32, dma = jnp.float32, pltpu.SemaphoreType.DMA
    return pl.pallas_call(
        functools.partial(solve_kernel, ng, ng**3),
        out_shape=(
            jax.ShapeDtypeStruct((groups, planes, ng, 128), f32), jax.ShapeDtypeStruct((nband, 128), f32)
        ),
        in_specs=[pl.BlockSpec(memory_space=pltpu.VMEM)] * 9,
        out_specs=(pl.BlockSpec(memory_space=pltpu.VMEM),) * 2,
        scratch_shapes=[
            pltpu.VMEM((nband + 3 * groups,) + full[1:], f32),
            pltpu.VMEM(full, f32), pltpu.VMEM(full, f32), pltpu.VMEM(full, f32),
            pltpu.VMEM((groups, planes, ng, 128), f32), pltpu.VMEM((groups, planes, ng, 128), f32),
            pltpu.VMEM((2, 256, 256), b16), pltpu.VMEM((nband, groups, 8, width), f32),
            pltpu.VMEM((groups, nband, 128), f32), pltpu.VMEM((groups, nband, 128), f32),
            dma((3, groups)), dma((3, 3)), dma((nband,)), dma((nband,)), dma((nband,)), dma((nband,)), dma((nband,)),
            dma((groups,)), dma((groups,)), dma((groups,)), dma((groups,)), dma(()),
        ],
        compiler_params=pltpu.CompilerParams(
            vmem_limit_bytes=60 * 1024 * 1024, collective_id=0, has_side_effects=True
        ),
        cost_estimate=pl.CostEstimate(flops=10**11, bytes_accessed=10**7, transcendentals=0),
        name="solve",
    )(own, *[jnp.asarray(c) for c in consts])


def on_device(orbitals):
    groups, nband = lax.axis_size("grid"), lax.axis_size("band")
    bands, local = orbitals.shape
    ncell = local * groups
    ng = round(ncell ** (1 / 3))
    xs = local // (ng * ng)
    planes = xs // 2
    t = orbitals.reshape(bands, 2, planes, ng, ng).transpose(2, 3, 1, 0, 4).reshape(planes, ng, 2, bands * ng)
    own = jnp.concatenate([t[:, :, 0, :128], t[:, :, 1, :128], t[:, :, 0, 128:], t[:, :, 1, 128:]], axis=-1)
    out, marg = solve(own, bands, groups, nband)
    vec = out[..., : 2 * ng].reshape(groups, planes, ng, 2, ng).transpose(0, 3, 1, 2, 4)
    vectors = vec.reshape(bands, local)
    margin = marg[:, :bands].reshape(nband // groups, groups, bands).transpose(0, 2, 1).reshape(nband, groups)
    return (vectors, margin)


def solution(mesh):
    return jax.shard_map(
        on_device,
        mesh=mesh,
        in_specs=(P("band", "grid"),),
        out_specs=(P("band", "grid"), P("grid", "band")),
        check_vma=False,
    )
```

```python
import functools

import jax
import jax.numpy as jnp
import numpy as np
from jax import lax
from jax.experimental import pallas as pl
from jax.experimental.pallas import tpu as pltpu
from jax.sharding import PartitionSpec as P


def kernel_values(ng):
    freqs = ((np.arange(ng) + ng // 2) % ng - ng // 2).astype(np.float32)
    sq = freqs[: ng // 2 + 1, None, None] ** 2 + freqs[None, :, None] ** 2 + freqs[None, None, :] ** 2
    safe = np.where(sq > 0, sq, np.float32(1.0))
    return np.where(sq > 0, 40.0 * (1.0 - np.exp(-sq / 16.0)) / safe, 0.0)


def hartley(ng):
    k = np.arange(ng)
    ang = (k[:, None] * k[None, :] % ng) * (2.0 * np.pi / ng)
    return np.cos(ang) + np.sin(ang)


def split_const(table):
    table = np.asarray(table, np.float32)
    hi = table.astype(jnp.bfloat16)
    lo = (table - hi.astype(np.float32)).astype(jnp.bfloat16)
    return hi, lo


def rfft(xs):
    n = len(xs)
    if n == 3:
        s = xs[1] + xs[2]
        d = xs[1] - xs[2]
        return [(xs[0] + s, None), (xs[0] - 0.5 * s, d * (-np.sqrt(3.0) / 2))]
    even, odd = rfft(xs[0::2]), rfft(xs[1::2])
    half = n // 2
    out = [None] * (half + 1)
    for k in range(half // 2 + 1):
        er, ei = even[k]
        orr, oi = odd[k]
        if k == 0:
            out[0] = (er + orr, None)
            out[half] = (er - orr, None)
            continue
        c, s = np.cos(2 * np.pi * k / n), -np.sin(2 * np.pi * k / n)
        if 2 * k == half:
            out[k] = (er, -orr)
            continue
        tr, ti = cmul(orr, oi, c, s)
        out[k] = (er + tr, addo(ei, ti))
        out[half - k] = (er - tr, subo(ti, ei))
    return out


def addo(a, b):
    return b if a is None else a + b


def subo(a, b):
    return a if b is None else a - b


def cmul(r, i, c, s):
    if i is None:
        return r * c, r * s
    if abs(abs(c) - abs(s)) < 1e-9:
        if s < 0 < c:
            return (r + i) * c, (i - r) * c
        return (r - i) * c, (r + i) * c
    return r * c - i * s, r * s + i * c


def irfft(spec, n):
    if n == 3:
        dc, (r, i) = spec[0][0], spec[1]
        base = dc - r
        t = i * np.sqrt(3.0)
        return [dc + 2.0 * r, base - t, base + t]
    half = n // 2
    even, odd = [None] * (half // 2 + 1), [None] * (half // 2 + 1)
    for k in range(half // 2 + 1):
        yr, yi = spec[k]
        if k == 0:
            hr = spec[half][0]
            even[0] = (yr + hr, None)
            odd[0] = (yr - hr, None)
            continue
        if 2 * k == half:
            even[k] = (yr + yr, None)
            odd[k] = (-(yi + yi), None)
            continue
        zr, zi = spec[half - k]
        er, ei = yr + zr, yi - zi
        dr, di = yr - zr, yi + zi
        c, s = np.cos(2 * np.pi * k / n), np.sin(2 * np.pi * k / n)
        even[k] = (er, ei)
        odd[k] = cmul(dr, di, c, s)
    ev, od = irfft(even, half), irfft(odd, half)
    out = [None] * n
    out[0::2], out[1::2] = ev, od
    return out


def split(v):
    hi = v.astype(jnp.bfloat16)
    lo = (v - hi.astype(jnp.float32)).astype(jnp.bfloat16)
    return hi, lo


def mm(a, b):
    return jnp.dot(a, b, preferred_element_type=jnp.float32)


def solve_kernel(ng, ncell, own_ref, k1_ref, k2_ref, zt_ref, ty_ref, cp_ref, s_ref, st_ref, hot_ref,
                 o_ref, m_ref, store, amp, acc, work, vec, recv, sel, rows_buf, mine, marg,
                 rsem, ssem, gsem, ysem, usem, dsem, wsem, osem, orsem, msem, mrsem, lsem):
    planes, _, width = own_ref.shape
    groups = vec.shape[0]
    me = lax.axis_index("grid")
    band, nband = lax.axis_index("band"), lax.axis_size("band")
    chip, core = me // 2, me % 2
    sib = chip * 2 + (1 - core)
    cross = (1 - chip) * 2 + core
    far = (1 - chip) * 2 + (1 - core)
    length = nband // 2
    side, pos = band % 2, band // 2
    pair = band + 1 - 2 * side
    third = (band + nband - 1 + 2 * side) % nband
    first, last = band == 0, band == nband - 1
    ends = jnp.logical_or(first, last)
    wrap = jnp.where(first, nband - 1, 0)
    has_up, has_down = pos < length - 1, pos > 0
    up, down = jnp.where(has_up, band + 2, band), jnp.where(has_down, band - 2, band)
    mesh_id = pl.DeviceIdType.MESH
    flat = planes * ng
    part = planes // 2

    def remote(src, dst, send, recv_sem, device):
        return pltpu.make_async_remote_copy(
            src_ref=src, dst_ref=dst, send_sem=send, recv_sem=recv_sem,
            device_id=device, device_id_type=mesh_id,
        )

    def partner(blk):
        return jnp.where(blk == 0, band, jnp.where(blk == 1, pair, third))

    def place(blk, slot):
        return jnp.where(slot == me, partner(blk), nband + blk * groups + slot)

    def piece(ref, c):
        return ref.at[pl.ds(c * part, part)]

    def share(blk, lane, slot, src, target, c):
        dst = store.at[nband + blk * groups + slot]
        return remote(piece(src, c), piece(dst, c), ssem.at[blk, lane, c], rsem.at[blk, slot, c], (band, target))

    def along(block, sems, device, c, src=None):
        dst = store.at[block]
        src = dst if src is None else src
        return remote(piece(src, c), piece(dst, c), sems.at[block, c], gsem.at[block, c], (device, me))

    def came(block, c):
        along(block, ysem, pair, c).wait_recv()

    def greet(device):
        pl.semaphore_signal(barrier, inc=1, device_id=device, device_id_type=mesh_id)

    barrier = pltpu.get_barrier_semaphore()
    for device in ((band, sib), (band, cross), (band, far), (pair, me)):
        greet(device)

    @pl.when(has_up)
    def _():
        greet((up, me))

    @pl.when(has_down)
    def _():
        greet((down, me))

    @pl.when(ends)
    def _():
        greet((wrap, me))

    count = 4 + has_up.astype(jnp.int32) + has_down.astype(jnp.int32) + ends.astype(jnp.int32)
    pl.semaphore_wait(barrier, count)

    def own_copies(c, act):
        def go(copy):
            copy.start() if act == "go" else copy.wait_send()

        go(share(0, 1, me, own_ref, cross, c))
        go(share(0, 0, me, own_ref, sib, c))
        go(along(band, ysem, pair, c, own_ref))

        @pl.when(has_up)
        def _():
            go(along(band, usem, up, c, own_ref))

        @pl.when(has_down)
        def _():
            go(along(band, dsem, down, c, own_ref))

    def wrap_copies(act):
        @pl.when(ends)
        def _():
            for c in range(2):
                copy = along(band, wsem, wrap, c, own_ref)
                copy.start() if act == "go" else copy.wait_send()

    for c in range(2):
        own_copies(c, "go")
    wrap_copies("go")
    local = pltpu.make_async_copy(own_ref, store.at[band], lsem)
    local.start()

    def arrived(blk, slot, c):
        share(blk, 0, slot, own_ref, sib, c).wait_recv()

    def relay(blk, c):
        arrived(blk, cross, c)
        share(blk, 2, cross, store.at[nband + blk * groups + cross], sib, c).start()

    def spread(blk, c):
        came(partner(blk), c)
        share(blk, 1, me, store.at[partner(blk)], cross, c).start()
        share(blk, 0, me, store.at[partner(blk)], sib, c).start()

    def skipped(block):
        return jnp.logical_or(
            jnp.logical_and(pair == 0, block == nband - 1), jnp.logical_and(pair == nband - 1, block == 0)
        )

    def line(d, c, near, act):
        def pass_on(block, exists, on, sems, device):
            @pl.when(exists)
            def _():
                if act == "go":
                    came(block, c)

                def one(copy):
                    copy.start() if act == "go" else copy.wait_send()

                @pl.when(jnp.logical_not(skipped(block)))
                def _():
                    one(along(block, ysem, pair, c))

                @pl.when(on)
                def _():
                    one(along(block, sems, device, c))

        upward = (side == 1) == near
        pass_on(band - 2 * d, jnp.logical_and(upward, pos - d >= 0), has_up, usem, up)
        pass_on(
            band + 2 * d, jnp.logical_and(jnp.logical_not(upward), pos + d <= length - 1), has_down, dsem, down
        )

    def serve(blk, c):
        @pl.when(blk < 2)
        def _():
            spread(blk + 1, c)

        line(blk + 1, c, True, "go")

    def ztrans(v):
        hi, lo = split(v)
        parts = []
        for h in range(2):
            a, b = (jnp.concatenate([t[:, 128 * h:128 * h + 128], t[:, 256:]], axis=1) for t in (hi, lo))
            parts.append(mm(a, zt_ref[h, 0]) + mm(b, zt_ref[h, 0]) + mm(a, zt_ref[h, 1]))
        return jnp.concatenate([parts[0][:, :128], parts[1][:, :128], parts[0][:, 128:] + parts[1][:, 128:]], axis=1)

    def ytrans(v):
        hi, lo = split(v)
        return mm(ty_ref[...], jnp.concatenate([hi, lo, hi], axis=0))

    def amplitude(slot, rows):
        hi, lo = split(store[place(0, slot), rows].reshape(part * ng, width))
        parts = []
        for h in range(2):
            a, b = (jnp.concatenate([t[:, 128 * h:128 * h + 128], t[:, 256:]], axis=1) for t in (hi, lo))
            parts.append(mm(a, sel[h]) + mm(b, sel[h]))
        out = jnp.concatenate([parts[0][:, :128], parts[1][:, :128], parts[0][:, 128:] + parts[1][:, 128:]], axis=1)
        amp[slot, rows] = out.reshape(part, ng, width)

    for h in range(2):
        mark = (me + 1).astype(jnp.float32)
        sel[h] = jnp.where(cp_ref[h].astype(jnp.float32) == mark, 1.0, 0.0).astype(jnp.bfloat16)

    def forward(blk, i):
        slot = ((chip + i // 4) % 2) * 2 + (core + i % 2) % 2
        c = (i // 2) % 2
        rows = pl.ds(c * part, part)

        @pl.when(jnp.logical_or(i == 1, i == 3))
        def _():
            arrived(blk, sib, c)

        @pl.when(jnp.logical_or(i == 4, i == 6))
        def _():
            @pl.when(jnp.logical_or(blk == 0, i == 6))
            def _():
                serve(blk, c)

            relay(blk, c)

            @pl.when(jnp.logical_and(blk > 0, i == 6))
            def _():
                line(blk, c, False, "go")

        @pl.when(jnp.logical_or(i == 5, i == 7))
        def _():
            arrived(blk, far, c)

        @pl.when(blk == 0)
        def _():
            amplitude(slot, rows)

        p = (amp[slot, rows] * store[place(blk, slot), rows]).reshape(part * ng, width)
        q = ztrans(p).reshape(part, ng, width)
        for r in range(part):
            work[slot, c * part + r] = ytrans(q[r])

    def conv(vals, kern):
        spec = rfft(vals)
        out = []
        for k, (re, im) in enumerate(spec):
            kv = kern(k)
            out.append((re * kv, None if im is None else im * kv))
        return irfft(out, ng)

    def xconv(t):
        order = [(g, h, r) for g in range(4) for h in range(2) for r in range(planes)]
        for i in range(2):
            rows = pl.ds(pl.multiple_of(t * 16 + 8 * i, 8), 8)
            res = conv([work[g, r, rows, h * 128:h * 128 + 128] for g, h, r in order],
                       lambda k: k1_ref[k, rows, :])
            for (g, h, r), v in zip(order, res):
                work[g, r, rows, h * 128:h * 128 + 128] = v
        ra = pl.ds(pl.multiple_of(t * 16, 8), 8)
        rb = pl.ds(pl.multiple_of(t * 16 + 8, 8), 8)
        left = lax.broadcasted_iota(jnp.int32, (8, 128), 1) < 64

        def half(g, h, r):
            u, w = work[g, r, ra, 256:384], work[g, r, rb, 256:384]
            if h == 0:
                return jnp.where(left, u, pltpu.roll(w, 64, 1))
            return jnp.where(left, pltpu.roll(u, 64, 1), w)

        rk = pl.ds(pl.multiple_of(t * 8, 8), 8)
        res = dict(zip(order, conv([half(*o) for o in order], lambda k: k2_ref[k, rk, :])))
        for g in range(4):
            for r in range(planes):
                a, b = res[(g, 0, r)], res[(g, 1, r)]
                work[g, r, ra, 256:384] = jnp.where(left, a, pltpu.roll(b, 64, 1))
                work[g, r, rb, 256:384] = jnp.where(left, pltpu.roll(a, 64, 1), b)

    def push(slot):
        return remote(vec.at[slot], recv.at[me], osem.at[slot], orsem.at[me], (band, slot))

    def inverse(blk, s):
        slot = ((chip + 1 - s // 2) % 2) * 2 + (core + s % 2 + s // 2) % 2
        q = jnp.concatenate([ytrans(work[slot, r]) for r in range(planes)], axis=0)
        w = ztrans(q).reshape(planes, ng, width) * store[place(blk, slot)]

        @pl.when(jnp.logical_and(blk < 2, s == 2))
        def _():
            serve(blk + 1, 0)
            line(blk + 1, 0, False, "go")

        @pl.when(blk == 0)
        def _():
            acc[slot] = w

        @pl.when(blk == 1)
        def _():
            acc[slot] += w

        @pl.when(blk == 2)
        def _():
            hi, lo = split((acc[slot] + w).reshape(flat, width))
            out = -(mm(hi, s_ref[...]) + mm(lo, s_ref[...]))
            vec[slot] = out.reshape(planes, ng, s_ref.shape[-1])

            @pl.when(s < 3)
            def _():
                push(slot).start()

    def block(blk, _):
        @pl.when(blk == 0)
        def _():
            local.wait()

        def fwd(i, _):
            forward(blk, i)
            return 0

        def mid(t, _):
            xconv(t)
            return 0

        def inv(s, _):
            inverse(blk, s)
            return 0

        lax.fori_loop(0, 8, fwd, 0)
        lax.fori_loop(0, ng // 16, mid, 0)
        lax.fori_loop(0, 4, inv, 0)
        return 0

    lax.fori_loop(0, 3, block, 0)

    def later(d, _):
        for c in range(2):
            line(d, c, False, "go")
            line(d + 1, c, True, "go")
        return 0

    lax.fori_loop(3, length, later, 0)

    def settle(block, _):
        known = jnp.logical_or(block == band, jnp.logical_or(block == pair, block == third))
        relayed = block % 2 == side

        @pl.when(jnp.logical_not(jnp.logical_or(known, relayed)))
        def _():
            for c in range(2):
                came(block, c)

        return 0

    lax.fori_loop(0, nband, settle, 0)

    def spread_out(v):
        hi, lo = split(v.reshape(flat, v.shape[-1]))
        return (mm(hi, st_ref[...]) + mm(lo, st_ref[...])).reshape(planes, ng, width)

    def column(slot):
        amp[0] = spread_out(o_ref[slot])

        def one(block, _):
            total = jnp.sum(store[block].reshape(flat // 8, 8, width) * amp[0].reshape(flat // 8, 8, width), axis=0)
            rows_buf[block, slot] = total
            return 0

        lax.fori_loop(0, nband, one, 0)

    o_ref[me] = vec[me]
    column(me)
    for slot in (sib, cross, far):
        remote(vec.at[slot], recv.at[slot], osem.at[slot], orsem.at[slot], (band, slot)).wait()
        o_ref[slot] = recv[slot]
        column(slot)

    lanes = jnp.sum(rows_buf[...], axis=2).reshape(groups * nband, width)
    rest = lanes
    terms = jnp.zeros((groups * nband, hot_ref.shape[-1]), jnp.float32)
    for _ in range(3):
        hi = rest.astype(jnp.bfloat16)
        terms += mm(hi, hot_ref[...])
        rest = rest - hi.astype(jnp.float32)
    mine[...] = (terms / ncell).reshape(groups, nband, terms.shape[-1])

    def give(slot):
        return remote(mine.at[slot], marg.at[me], msem.at[slot], mrsem.at[me], (band, slot))

    for slot in (cross, far, sib):
        give(slot).start()
    total = mine[me]
    for slot in (sib, cross, far):
        remote(mine.at[slot], marg.at[slot], msem.at[slot], mrsem.at[slot], (band, slot)).wait()
        total += marg[slot]
    m_ref[...] = total

    wrap_copies("end")
    for c in range(2):
        own_copies(c, "end")

    def finish(i, _):
        blk, c = 1 + i // 2, i % 2
        for lane, target in ((0, sib), (1, cross)):
            share(blk, lane, me, own_ref, target, c).wait_send()
        return 0

    def finish_relay(i, _):
        share(i // 2, 2, me, own_ref, sib, i % 2).wait_send()
        return 0

    def finish_line(i, _):
        line(1 + i // 2, i % 2, True, "end")
        line(1 + i // 2, i % 2, False, "end")
        return 0

    lax.fori_loop(0, 4, finish, 0)
    lax.fori_loop(0, 6, finish_relay, 0)
    lax.fori_loop(0, 2 * (length - 1), finish_line, 0)


def lane_tables(ng, bands):
    w = bands * ng
    half, bz = [], []
    for lo, hi in ((0, 128), (128, w)):
        for h in range(2):
            half.append(np.full(hi - lo, h))
            bz.append(np.arange(lo, hi))
    half, bz = np.concatenate(half), np.concatenate(bz)
    return half, bz // ng, bz % ng


def tiles(table, half):
    out = []
    for h in range(2):
        pick = np.concatenate([np.arange(128 * h, 128 * h + 128), np.arange(256, len(half))])
        live = half[pick] == h
        out.append(np.where(live[:, None] & live[None, :], table[pick][:, pick], 0.0))
    return np.stack(out)


def solve(own, bands, groups, nband):
    planes, ng, width = own.shape
    half, bnd, zed = lane_tables(ng, bands)
    ht = hartley(ng)
    th, tl = split_const(ht)
    same = (half[:, None] == half[None, :])
    zmat = np.where(same & (bnd[:, None] == bnd[None, :]), ht[zed[:, None], zed[None, :]], 0.0)
    zt = np.stack(split_const(tiles(zmat, half)), axis=1)
    ty = np.concatenate([th, th, tl], axis=1)
    cp = tiles(np.where(same & (zed[:, None] == zed[None, :]), bnd[:, None] + 1.0, 0.0), half)
    s = np.zeros((width, 128), np.float32)
    s[np.arange(width), half * ng + zed] = 1.0
    hot = np.zeros((width, 128), np.float32)
    hot[np.arange(width), bnd] = 1.0
    kv = kernel_values(ng).astype(np.float32) / np.float32(ng**3)
    kb = np.tile(kv, (1, 1, bands))
    k1 = kb[:, :, :128]
    rest = kb[:, :, 128:].reshape(kb.shape[0], ng // 16, 2, 8, 64)
    k2 = np.concatenate([rest[:, :, 0], rest[:, :, 1]], axis=-1).reshape(kb.shape[0], ng // 2, 128)
    b16 = jnp.bfloat16
    consts = [k1, k2, zt, ty, cp.astype(b16), s.astype(b16), s.T.astype(b16), hot.astype(b16)]
    full = (groups, planes, ng, width)
    f32, dma = jnp.float32, pltpu.SemaphoreType.DMA
    return pl.pallas_call(
        functools.partial(solve_kernel, ng, ng**3),
        out_shape=(
            jax.ShapeDtypeStruct((groups, planes, ng, 128), f32), jax.ShapeDtypeStruct((nband, 128), f32)
        ),
        in_specs=[pl.BlockSpec(memory_space=pltpu.VMEM)] * 9,
        out_specs=(pl.BlockSpec(memory_space=pltpu.VMEM),) * 2,
        scratch_shapes=[
            pltpu.VMEM((nband + 3 * groups,) + full[1:], f32),
            pltpu.VMEM(full, f32), pltpu.VMEM(full, f32), pltpu.VMEM(full, f32),
            pltpu.VMEM((groups, planes, ng, 128), f32), pltpu.VMEM((groups, planes, ng, 128), f32),
            pltpu.VMEM((2, 256, 256), b16), pltpu.VMEM((nband, groups, 8, width), f32),
            pltpu.VMEM((groups, nband, 128), f32), pltpu.VMEM((groups, nband, 128), f32),
            dma((3, groups, 2)), dma((3, 3, 2)), dma((nband, 2)), dma((nband, 2)), dma((nband, 2)), dma((nband, 2)),
            dma((nband, 2)),
            dma((groups,)), dma((groups,)), dma((groups,)), dma((groups,)), dma(()),
        ],
        compiler_params=pltpu.CompilerParams(
            vmem_limit_bytes=60 * 1024 * 1024, collective_id=0, has_side_effects=True
        ),
        cost_estimate=pl.CostEstimate(flops=10**11, bytes_accessed=10**7, transcendentals=0),
        name="solve",
    )(own, *[jnp.asarray(c) for c in consts])


def on_device(orbitals):
    groups, nband = lax.axis_size("grid"), lax.axis_size("band")
    bands, local = orbitals.shape
    ncell = local * groups
    ng = round(ncell ** (1 / 3))
    xs = local // (ng * ng)
    planes = xs // 2
    t = orbitals.reshape(bands, 2, planes, ng, ng).transpose(2, 3, 1, 0, 4).reshape(planes, ng, 2, bands * ng)
    own = jnp.concatenate([t[:, :, 0, :128], t[:, :, 1, :128], t[:, :, 0, 128:], t[:, :, 1, 128:]], axis=-1)
    out, marg = solve(own, bands, groups, nband)
    vec = out[..., : 2 * ng].reshape(groups, planes, ng, 2, ng).transpose(0, 3, 1, 2, 4)
    vectors = vec.reshape(bands, local)
    margin = marg[:, :bands].reshape(nband // groups, groups, bands).transpose(0, 2, 1).reshape(nband, groups)
    return (vectors, margin)


def solution(mesh):
    return jax.shard_map(
        on_device,
        mesh=mesh,
        in_specs=(P("band", "grid"),),
        out_specs=(P("band", "grid"), P("grid", "band")),
        check_vma=False,
    )
```

```python
import functools

import jax
import jax.numpy as jnp
import numpy as np
from jax import lax
from jax.experimental import pallas as pl
from jax.experimental.pallas import tpu as pltpu
from jax.sharding import PartitionSpec as P


def kernel_values(ng):
    freqs = ((np.arange(ng) + ng // 2) % ng - ng // 2).astype(np.float32)
    sq = freqs[: ng // 2 + 1, None, None] ** 2 + freqs[None, :, None] ** 2 + freqs[None, None, :] ** 2
    safe = np.where(sq > 0, sq, np.float32(1.0))
    return np.where(sq > 0, 40.0 * (1.0 - np.exp(-sq / 16.0)) / safe, 0.0)


def hartley(ng):
    k = np.arange(ng)
    ang = (k[:, None] * k[None, :] % ng) * (2.0 * np.pi / ng)
    return np.cos(ang) + np.sin(ang)


def split_const(table):
    table = np.asarray(table, np.float32)
    hi = table.astype(jnp.bfloat16)
    lo = (table - hi.astype(np.float32)).astype(jnp.bfloat16)
    return hi, lo


def rfft(xs):
    n = len(xs)
    if n == 3:
        s = xs[1] + xs[2]
        d = xs[1] - xs[2]
        return [(xs[0] + s, None), (xs[0] - 0.5 * s, d * (-np.sqrt(3.0) / 2))]
    even, odd = rfft(xs[0::2]), rfft(xs[1::2])
    half = n // 2
    out = [None] * (half + 1)
    for k in range(half // 2 + 1):
        er, ei = even[k]
        orr, oi = odd[k]
        if k == 0:
            out[0] = (er + orr, None)
            out[half] = (er - orr, None)
            continue
        c, s = np.cos(2 * np.pi * k / n), -np.sin(2 * np.pi * k / n)
        if 2 * k == half:
            out[k] = (er, -orr)
            continue
        tr, ti = cmul(orr, oi, c, s)
        out[k] = (er + tr, addo(ei, ti))
        out[half - k] = (er - tr, subo(ti, ei))
    return out


def addo(a, b):
    return b if a is None else a + b


def subo(a, b):
    return a if b is None else a - b


def cmul(r, i, c, s):
    if i is None:
        return r * c, r * s
    if abs(abs(c) - abs(s)) < 1e-9:
        if s < 0 < c:
            return (r + i) * c, (i - r) * c
        return (r - i) * c, (r + i) * c
    return r * c - i * s, r * s + i * c


def irfft(spec, n):
    if n == 3:
        dc, (r, i) = spec[0][0], spec[1]
        base = dc - r
        t = i * np.sqrt(3.0)
        return [dc + 2.0 * r, base - t, base + t]
    half = n // 2
    even, odd = [None] * (half // 2 + 1), [None] * (half // 2 + 1)
    for k in range(half // 2 + 1):
        yr, yi = spec[k]
        if k == 0:
            hr = spec[half][0]
            even[0] = (yr + hr, None)
            odd[0] = (yr - hr, None)
            continue
        if 2 * k == half:
            even[k] = (yr + yr, None)
            odd[k] = (-(yi + yi), None)
            continue
        zr, zi = spec[half - k]
        er, ei = yr + zr, yi - zi
        dr, di = yr - zr, yi + zi
        c, s = np.cos(2 * np.pi * k / n), np.sin(2 * np.pi * k / n)
        even[k] = (er, ei)
        odd[k] = cmul(dr, di, c, s)
    ev, od = irfft(even, half), irfft(odd, half)
    out = [None] * n
    out[0::2], out[1::2] = ev, od
    return out


def split(v):
    hi = v.astype(jnp.bfloat16)
    lo = (v - hi.astype(jnp.float32)).astype(jnp.bfloat16)
    return hi, lo


def mm(a, b):
    return jnp.dot(a, b, preferred_element_type=jnp.float32)


def solve_kernel(ng, ncell, nat_ref, *refs):
    tables, refs = refs[:7], refs[7:]
    (o_ref, m_ref, k1_ref, k2_ref, zt_ref, ty_ref, cp_ref, s_ref, hot_ref, own_ref, store, amp, acc, work, vec, recv, sel,
     rows_buf, mine, marg, rsem, ssem, gsem, ysem, usem, dsem, wsem, osem, orsem, msem, mrsem, lsem, csem, esem, tmp, ebuf) = refs
    kept = (k1_ref, k2_ref, zt_ref, ty_ref, cp_ref, s_ref, hot_ref)
    loads = [pltpu.make_async_copy(src, dst, csem.at[n]) for n, (src, dst) in enumerate(zip(tables, kept))]
    for n in (4, 2, 3, 0, 1, 5, 6):
        loads[n].start()
    bands = nat_ref.shape[0]
    flat, width = own_ref.shape
    planes = flat // ng
    groups = vec.shape[0]
    me = lax.axis_index("grid")
    band, nband = lax.axis_index("band"), lax.axis_size("band")
    chip, core = me // 2, me % 2
    sib = chip * 2 + (1 - core)
    cross = (1 - chip) * 2 + core
    far = (1 - chip) * 2 + (1 - core)
    length = nband // 2
    side, pos = band % 2, band // 2
    pair = band + 1 - 2 * side
    third = (band + nband - 1 + 2 * side) % nband
    first, last = band == 0, band == nband - 1
    ends = jnp.logical_or(first, last)
    wrap = jnp.where(first, nband - 1, 0)
    has_up, has_down = pos < length - 1, pos > 0
    up, down = jnp.where(has_up, band + 2, band), jnp.where(has_down, band - 2, band)
    mesh_id = pl.DeviceIdType.MESH
    part = planes // 2

    def remote(src, dst, send, recv_sem, device):
        return pltpu.make_async_remote_copy(
            src_ref=src, dst_ref=dst, send_sem=send, recv_sem=recv_sem,
            device_id=device, device_id_type=mesh_id,
        )

    def partner(blk):
        return jnp.where(blk == 0, band, jnp.where(blk == 1, pair, third))

    def place(blk, slot):
        return jnp.where(slot == me, partner(blk), nband + blk * groups + slot)

    def piece(ref, c):
        return ref.at[pl.ds(c * part * ng, part * ng)]

    def share(blk, lane, slot, src, target, c):
        dst = store.at[nband + blk * groups + slot]
        return remote(piece(src, c), piece(dst, c), ssem.at[blk, lane, c], rsem.at[blk, slot, c], (band, target))

    def along(block, sems, device, c, src=None):
        dst = store.at[block]
        src = dst if src is None else src
        return remote(piece(src, c), piece(dst, c), sems.at[block, c], gsem.at[block, c], (device, me))

    def came(block, c):
        along(block, ysem, pair, c).wait_recv()

    lane = lax.broadcasted_iota(jnp.int32, (1, 128), 1)

    def moved(value, shift, low, high, under):
        out = pltpu.roll(value, shift % 128, 1) if shift % 128 else value
        return jnp.where(jnp.logical_and(lane >= low, lane < high), out, under)

    def gather_in(read, want, blank):
        for y0 in range(8):
            chunks = [None, None, None]
            for h in range(2):
                for b in range(bands):
                    for target, start, stop, base in ((h, 0, 128, 0), (2, 128, bands * ng, 64 * h)):
                        first, final = max(start, b * ng), min(stop, b * ng + ng)
                        if first >= final:
                            continue
                        source = y0 * ng + first - b * ng
                        place_at = first - start + base
                        while first < final:
                            q, off = source // 128, source % 128
                            size = min(final - first, 128 - off)
                            under = chunks[target]
                            under = blank if under is None else under
                            chunks[target] = moved(read(b, h, q), place_at - off, place_at, place_at + size, under)
                            first, source, place_at = first + size, source + size, place_at + size
            for j, value in enumerate(chunks):
                want(j, y0, value)

    def scatter_out(read, write, blank):
        for h in range(2):
            chunks = [blank] * 3
            for y0 in range(8):
                value = read(y0)
                source, at, left = h * ng, y0 * ng, ng
                while left > 0:
                    q, off = at // 128, at % 128
                    size = min(left, 128 - off)
                    chunks[q] = moved(value, off - source, off, off + size, chunks[q])
                    source, at, left = source + size, at + size, left - size
            for q in range(3):
                write(h, q, chunks[q])

    group = flat // 8

    def packed(h, q):
        return pl.ds(q + 3 * group * h, group, stride=3)

    def spaced(y0):
        return pl.ds(y0, group, stride=8)

    def greet(device):
        pl.semaphore_signal(barrier, inc=1, device_id=device, device_id_type=mesh_id)

    barrier = pltpu.get_barrier_semaphore()
    for device in ((band, sib), (band, cross), (band, far), (pair, me)):
        greet(device)

    @pl.when(has_up)
    def _():
        greet((up, me))

    @pl.when(has_down)
    def _():
        greet((down, me))

    @pl.when(ends)
    def _():
        greet((wrap, me))

    count = 4 + has_up.astype(jnp.int32) + has_down.astype(jnp.int32) + ends.astype(jnp.int32)
    def own_copies(c, act):
        def go(copy):
            copy.start() if act == "go" else copy.wait_send()

        go(share(0, 1, me, own_ref, cross, c))
        go(share(0, 0, me, own_ref, sib, c))
        go(along(band, ysem, pair, c, own_ref))

        @pl.when(has_up)
        def _():
            go(along(band, usem, up, c, own_ref))

        @pl.when(has_down)
        def _():
            go(along(band, dsem, down, c, own_ref))

    def wrap_copies(act):
        @pl.when(ends)
        def _():
            for c in range(2):
                copy = along(band, wsem, wrap, c, own_ref)
                copy.start() if act == "go" else copy.wait_send()

    def put_own(j, y0, value):
        ebuf[0, j, spaced(y0), :] = value

    gather_in(lambda b, h, q: nat_ref[b, packed(h, q), :], put_own, jnp.zeros((group, 128), jnp.float32))
    own_ref[...] = jnp.concatenate([ebuf[0, j] for j in range(3)], axis=1)
    pl.semaphore_wait(barrier, count)
    for c in range(2):
        own_copies(c, "go")
    wrap_copies("go")
    local = pltpu.make_async_copy(own_ref, store.at[band], lsem)
    local.start()

    def arrived(blk, slot, c):
        share(blk, 0, slot, own_ref, sib, c).wait_recv()

    def relay(blk, c):
        arrived(blk, cross, c)
        share(blk, 2, cross, store.at[nband + blk * groups + cross], sib, c).start()

    def spread(blk, c):
        came(partner(blk), c)
        share(blk, 1, me, store.at[partner(blk)], cross, c).start()
        share(blk, 0, me, store.at[partner(blk)], sib, c).start()

    def skipped(block):
        return jnp.logical_or(
            jnp.logical_and(pair == 0, block == nband - 1), jnp.logical_and(pair == nband - 1, block == 0)
        )

    def line(d, c, near, act):
        def pass_on(block, exists, on, sems, device):
            @pl.when(exists)
            def _():
                if act == "go":
                    came(block, c)

                def one(copy):
                    copy.start() if act == "go" else copy.wait_send()

                @pl.when(jnp.logical_not(skipped(block)))
                def _():
                    one(along(block, ysem, pair, c))

                @pl.when(on)
                def _():
                    one(along(block, sems, device, c))

        upward = (side == 1) == near
        pass_on(band - 2 * d, jnp.logical_and(upward, pos - d >= 0), has_up, usem, up)
        pass_on(
            band + 2 * d, jnp.logical_and(jnp.logical_not(upward), pos + d <= length - 1), has_down, dsem, down
        )

    def serve(blk, c):
        @pl.when(blk < 2)
        def _():
            spread(blk + 1, c)

        line(blk + 1, c, True, "go")

    def ztrans(v):
        hi, lo = split(v)
        parts = []
        for h in range(2):
            a, b = (jnp.concatenate([t[:, 128 * h:128 * h + 128], t[:, 256:]], axis=1) for t in (hi, lo))
            parts.append(mm(a, zt_ref[h, 0]) + mm(b, zt_ref[h, 0]) + mm(a, zt_ref[h, 1]))
        return jnp.concatenate([parts[0][:, :128], parts[1][:, :128], parts[0][:, 128:] + parts[1][:, 128:]], axis=1)

    def ytrans(v):
        hi, lo = split(v)
        return mm(ty_ref[...], jnp.concatenate([hi, lo, hi], axis=0))

    def amplitude(v):
        hi, lo = split(v)
        parts = []
        for h in range(2):
            a, b = (jnp.concatenate([t[:, 128 * h:128 * h + 128], t[:, 256:]], axis=1) for t in (hi, lo))
            parts.append(mm(a, sel[h]) + mm(b, sel[h]))
        return jnp.concatenate([parts[0][:, :128], parts[1][:, :128], parts[0][:, 128:] + parts[1][:, 128:]], axis=1)

    for n in (4, 2, 3):
        loads[n].wait()
    for h in range(2):
        mark = (me + 1).astype(jnp.float32)
        sel[h] = jnp.where(cp_ref[h].astype(jnp.float32) == mark, 1.0, 0.0).astype(jnp.bfloat16)

    def transform(blk, slots, c):
        rows = pl.ds(c * part * ng, part * ng)

        @pl.when(blk == 0)
        def _():
            own = jnp.concatenate([store[place(0, slot), rows] for slot in slots], axis=0)
            out = amplitude(own).reshape(len(slots), part * ng, width)
            for n, slot in enumerate(slots):
                amp[slot, rows] = out[n]

        p = jnp.concatenate([amp[slot, rows] * store[place(blk, slot), rows] for slot in slots], axis=0)
        q = ztrans(p).reshape(len(slots), part, ng, width)
        for n, slot in enumerate(slots):
            for r in range(part):
                work[slot, c * part + r] = ytrans(q[n, r])

    def near(blk, c):
        arrived(blk, sib, c)

        @pl.when(jnp.logical_and(blk > 0, c == 1))
        def _():
            relay(blk, 0)

        transform(blk, (me, sib), c)

    def other(blk, i):
        c = i // 2

        @pl.when(jnp.logical_and(blk == 0, i == 0))
        def _():
            serve(blk, 0)
            relay(blk, 0)

        @pl.when(i == 1)
        def _():
            serve(blk, 1)
            relay(blk, 1)

        @pl.when(i % 2 == 1)
        def _():
            arrived(blk, far, c)

        @pl.when(jnp.logical_and(blk > 0, i == 2))
        def _():
            line(blk, 1, False, "go")

        transform(blk, (jnp.where(i % 2 == 0, cross, far),), c)

    def conv(vals, kern):
        spec = rfft(vals)
        out = []
        for k, (re, im) in enumerate(spec):
            kv = kern(k)
            out.append((re * kv, None if im is None else im * kv))
        return irfft(out, ng)

    def xconv(t):
        order = [(g, h, r) for g in range(4) for h in range(2) for r in range(planes)]
        for i in range(2):
            rows = pl.ds(pl.multiple_of(t * 16 + 8 * i, 8), 8)
            res = conv([work[g, r, rows, h * 128:h * 128 + 128] for g, h, r in order],
                       lambda k: k1_ref[k, rows, :])
            for (g, h, r), v in zip(order, res):
                work[g, r, rows, h * 128:h * 128 + 128] = v
        ra = pl.ds(pl.multiple_of(t * 16, 8), 8)
        rb = pl.ds(pl.multiple_of(t * 16 + 8, 8), 8)
        left = lax.broadcasted_iota(jnp.int32, (8, 128), 1) < 64

        def half(g, h, r):
            u, w = work[g, r, ra, 256:384], work[g, r, rb, 256:384]
            if h == 0:
                return jnp.where(left, u, pltpu.roll(w, 64, 1))
            return jnp.where(left, pltpu.roll(u, 64, 1), w)

        rk = pl.ds(pl.multiple_of(t * 8, 8), 8)
        res = dict(zip(order, conv([half(*o) for o in order], lambda k: k2_ref[k, rk, :])))
        for g in range(4):
            for r in range(planes):
                a, b = res[(g, 0, r)], res[(g, 1, r)]
                work[g, r, ra, 256:384] = jnp.where(left, a, pltpu.roll(b, 64, 1))
                work[g, r, rb, 256:384] = jnp.where(left, pltpu.roll(a, 64, 1), b)

    def push(slot):
        return remote(vec.at[slot], recv.at[me], osem.at[slot], orsem.at[me], (band, slot))

    def inverse(blk, s):
        slot = ((chip + 1 - s // 2) % 2) * 2 + (core + s % 2 + s // 2) % 2
        q = jnp.concatenate([ytrans(work[slot, r]) for r in range(planes)], axis=0)
        w = ztrans(q) * store[place(blk, slot)]

        @pl.when(jnp.logical_and(blk < 2, s == 2))
        def _():
            serve(blk + 1, 0)
            line(blk + 1, 0, False, "go")

        @pl.when(blk == 0)
        def _():
            acc[slot] = w

        @pl.when(blk == 1)
        def _():
            acc[slot] += w

        @pl.when(blk == 2)
        def _():
            hi, lo = split(acc[slot] + w)
            tmp[...] = -(mm(hi, s_ref[...]) + mm(lo, s_ref[...]))

            def put_vec(h, q, value):
                vec[slot, packed(h, q), :] = value

            scatter_out(lambda y0: tmp[spaced(y0), :], put_vec, jnp.zeros((group, 128), jnp.float32))

            @pl.when(s < 3)
            def _():
                push(slot).start()

    def block(blk, _):
        @pl.when(blk == 0)
        def _():
            local.wait()

        def fwd_near(c, _):
            near(blk, c)
            return 0

        def fwd_other(i, _):
            other(blk, i)
            return 0

        def mid(t, _):
            xconv(t)
            return 0

        def inv(s, _):
            inverse(blk, s)
            return 0

        lax.fori_loop(0, 2, fwd_near, 0)
        lax.fori_loop(0, 4, fwd_other, 0)

        @pl.when(blk == 0)
        def _():
            for n in (0, 1, 5, 6):
                loads[n].wait()

        lax.fori_loop(0, ng // 16, mid, 0)
        lax.fori_loop(0, 4, inv, 0)
        return 0

    lax.fori_loop(0, 3, block, 0)

    def later(d, _):
        for c in range(2):
            line(d, c, False, "go")
            line(d + 1, c, True, "go")
        return 0

    lax.fori_loop(3, length, later, 0)

    def emit(src, slot):
        return pltpu.make_async_copy(src.at[slot], o_ref.at[slot], esem.at[slot])

    def spread_out(src, slot, n):
        def put(j, y0, value):
            ebuf[n, j, spaced(y0), :] = value

        gather_in(lambda b, h, q: src[slot, packed(h, q), :], put, jnp.zeros((group, 128), jnp.float32))

    def columns(block, slots):
        parts = [[jnp.zeros((8, 128), jnp.float32) for _ in range(3)] for _ in slots]
        for r in range(flat // 8):
            for j in range(3):
                phi = store[block, pl.ds(8 * r, 8), pl.ds(128 * j, 128)]
                for n, p in enumerate(parts):
                    p[j] = p[j] + phi * ebuf[n, j, pl.ds(8 * r, 8)]
        for slot, p in zip(slots, parts):
            rows_buf[block, slot] = jnp.concatenate(p, axis=1)

    def ready(block):
        near_by = jnp.logical_or(block == pair, block == third)
        return jnp.logical_or(near_by, block % 2 == side)

    def early(block, _):
        @pl.when(ready(block))
        def _():
            columns(block, (me, sib))

        return 0

    def late(block, _):
        @pl.when(jnp.logical_not(ready(block)))
        def _():
            for c in range(2):
                came(block, c)
            columns(block, (me, sib))

        return 0

    def rest(block, _):
        columns(block, (cross, far))
        return 0

    def settle(slot):
        remote(vec.at[slot], recv.at[slot], osem.at[slot], orsem.at[slot], (band, slot)).wait()
        emit(recv, slot).start()

    emit(vec, me).start()
    spread_out(vec, me, 0)
    settle(sib)
    spread_out(recv, sib, 1)
    lax.fori_loop(0, nband, early, 0)
    lax.fori_loop(0, nband, late, 0)
    settle(cross)
    spread_out(recv, cross, 0)
    settle(far)
    spread_out(recv, far, 1)
    lax.fori_loop(0, nband, rest, 0)

    lanes = jnp.sum(rows_buf[...], axis=2).reshape(groups * nband, width)
    left_over = lanes
    terms = jnp.zeros((groups * nband, hot_ref.shape[-1]), jnp.float32)
    for _ in range(3):
        hi = left_over.astype(jnp.bfloat16)
        terms += mm(hi, hot_ref[...])
        left_over = left_over - hi.astype(jnp.float32)
    mine[...] = (terms / ncell).reshape(groups, nband, terms.shape[-1])

    def give(slot):
        return remote(mine.at[slot], marg.at[me], msem.at[slot], mrsem.at[me], (band, slot))

    for slot in (cross, far, sib):
        give(slot).start()
    for slot in range(groups):
        emit(recv, slot).wait()
    wrap_copies("end")
    for c in range(2):
        own_copies(c, "end")

    def finish(i, _):
        blk, c = 1 + i // 2, i % 2
        for lane, target in ((0, sib), (1, cross)):
            share(blk, lane, me, own_ref, target, c).wait_send()
        return 0

    def finish_relay(i, _):
        share(i // 2, 2, me, own_ref, sib, i % 2).wait_send()
        return 0

    def finish_line(i, _):
        line(1 + i // 2, i % 2, True, "end")
        line(1 + i // 2, i % 2, False, "end")
        return 0

    lax.fori_loop(0, 4, finish, 0)
    lax.fori_loop(0, 6, finish_relay, 0)
    lax.fori_loop(0, 2 * (length - 1), finish_line, 0)
    total = mine[me]
    for slot in (sib, cross, far):
        remote(mine.at[slot], marg.at[slot], msem.at[slot], mrsem.at[slot], (band, slot)).wait()
        total += marg[slot]
    m_ref[...] = total


def lane_tables(ng, bands):
    w = bands * ng
    half, bz = [], []
    for lo, hi in ((0, 128), (128, w)):
        for h in range(2):
            half.append(np.full(hi - lo, h))
            bz.append(np.arange(lo, hi))
    half, bz = np.concatenate(half), np.concatenate(bz)
    return half, bz // ng, bz % ng


def tiles(table, half):
    out = []
    for h in range(2):
        pick = np.concatenate([np.arange(128 * h, 128 * h + 128), np.arange(256, len(half))])
        live = half[pick] == h
        out.append(np.where(live[:, None] & live[None, :], table[pick][:, pick], 0.0))
    return np.stack(out)


def solve(nat, ng, groups, nband):
    bands = nat.shape[0]
    width = 2 * bands * ng
    flat = nat.shape[1] * nat.shape[2] // (2 * ng)
    half, bnd, zed = lane_tables(ng, bands)
    ht = hartley(ng)
    th, tl = split_const(ht)
    same = (half[:, None] == half[None, :])
    zmat = np.where(same & (bnd[:, None] == bnd[None, :]), ht[zed[:, None], zed[None, :]], 0.0)
    zt = np.stack(split_const(tiles(zmat, half)), axis=1)
    ty = np.concatenate([th, th, tl], axis=1)
    cp = tiles(np.where(same & (zed[:, None] == zed[None, :]), bnd[:, None] + 1.0, 0.0), half)
    s = np.zeros((width, 128), np.float32)
    s[np.arange(width), half * ng + zed] = 1.0
    hot = np.zeros((width, 128), np.float32)
    hot[np.arange(width), bnd] = 1.0
    kv = kernel_values(ng).astype(np.float32) / np.float32(ng**3)
    kb = np.tile(kv, (1, 1, bands))
    k1 = kb[:, :, :128]
    rest = kb[:, :, 128:].reshape(kb.shape[0], ng // 16, 2, 8, 64)
    k2 = np.concatenate([rest[:, :, 0], rest[:, :, 1]], axis=-1).reshape(kb.shape[0], ng // 2, 128)
    b16 = jnp.bfloat16
    consts = [k1, k2, zt, ty, cp.astype(b16), s.astype(b16), hot.astype(b16)]
    full = (groups, flat, width)
    slim = (groups,) + nat.shape[1:]
    f32, dma = jnp.float32, pltpu.SemaphoreType.DMA
    return pl.pallas_call(
        functools.partial(solve_kernel, ng, ng**3),
        out_shape=(
            jax.ShapeDtypeStruct(slim, f32), jax.ShapeDtypeStruct((nband, 128), f32)
        ),
        in_specs=[pl.BlockSpec(memory_space=pltpu.VMEM)] + [pl.BlockSpec(memory_space=pl.ANY)] * len(consts),
        out_specs=(pl.BlockSpec(memory_space=pl.ANY), pl.BlockSpec(memory_space=pltpu.VMEM)),
        scratch_shapes=[
            *[pltpu.VMEM(c.shape, c.dtype) for c in consts],
            pltpu.VMEM(full[1:], f32), pltpu.VMEM((nband + 3 * groups,) + full[1:], f32),
            pltpu.VMEM(full, f32), pltpu.VMEM(full, f32), pltpu.VMEM((groups, flat // ng, ng, width), f32),
            pltpu.VMEM(slim, f32), pltpu.VMEM(slim, f32),
            pltpu.VMEM((2, 256, 256), b16), pltpu.VMEM((nband, groups, 8, width), f32),
            pltpu.VMEM((groups, nband, 128), f32), pltpu.VMEM((groups, nband, 128), f32),
            dma((3, groups, 2)), dma((3, 3, 2)), dma((nband, 2)), dma((nband, 2)), dma((nband, 2)), dma((nband, 2)),
            dma((nband, 2)),
            dma((groups,)), dma((groups,)), dma((groups,)), dma((groups,)), dma(()), dma((len(consts),)), dma((groups,)),
            pltpu.VMEM((flat, 128), f32), pltpu.VMEM((2, 3, flat, 128), f32),
        ],
        compiler_params=pltpu.CompilerParams(
            vmem_limit_bytes=60 * 1024 * 1024, collective_id=0, has_side_effects=True
        ),
        cost_estimate=pl.CostEstimate(flops=10**11, bytes_accessed=10**7, transcendentals=0),
        name="solve",
    )(nat, *[jnp.asarray(c) for c in consts])


def on_device(orbitals):
    groups, nband = lax.axis_size("grid"), lax.axis_size("band")
    bands, local = orbitals.shape
    ncell = local * groups
    ng = round(ncell ** (1 / 3))
    out, marg = solve(orbitals.reshape(bands, local // 128, 128), ng, groups, nband)
    vectors = out.reshape(bands, local)
    margin = marg[:, :bands].reshape(nband // groups, groups, bands).transpose(0, 2, 1).reshape(nband, groups)
    return (vectors, margin)


def solution(mesh):
    return jax.shard_map(
        on_device,
        mesh=mesh,
        in_specs=(P("band", "grid"),),
        out_specs=(P("band", "grid"), P("grid", "band")),
        check_vma=False,
    )
```

```python
import functools

import jax
import jax.numpy as jnp
import numpy as np
from jax import lax
from jax.experimental import pallas as pl
from jax.experimental.pallas import tpu as pltpu
from jax.sharding import PartitionSpec as P


def kernel_values(ng):
    freqs = ((np.arange(ng) + ng // 2) % ng - ng // 2).astype(np.float32)
    sq = freqs[: ng // 2 + 1, None, None] ** 2 + freqs[None, :, None] ** 2 + freqs[None, None, :] ** 2
    safe = np.where(sq > 0, sq, np.float32(1.0))
    return np.where(sq > 0, 40.0 * (1.0 - np.exp(-sq / 16.0)) / safe, 0.0)


def hartley(ng):
    k = np.arange(ng)
    ang = (k[:, None] * k[None, :] % ng) * (2.0 * np.pi / ng)
    return np.cos(ang) + np.sin(ang)


def split_const(table):
    table = np.asarray(table, np.float32)
    hi = table.astype(jnp.bfloat16)
    lo = (table - hi.astype(np.float32)).astype(jnp.bfloat16)
    return hi, lo


def rfft(xs):
    n = len(xs)
    if n == 3:
        s = xs[1] + xs[2]
        d = xs[1] - xs[2]
        return [(xs[0] + s, None), (xs[0] - 0.5 * s, d * (-np.sqrt(3.0) / 2))]
    even, odd = rfft(xs[0::2]), rfft(xs[1::2])
    half = n // 2
    out = [None] * (half + 1)
    for k in range(half // 2 + 1):
        er, ei = even[k]
        orr, oi = odd[k]
        if k == 0:
            out[0] = (er + orr, None)
            out[half] = (er - orr, None)
            continue
        c, s = np.cos(2 * np.pi * k / n), -np.sin(2 * np.pi * k / n)
        if 2 * k == half:
            out[k] = (er, -orr)
            continue
        tr, ti = cmul(orr, oi, c, s)
        out[k] = (er + tr, addo(ei, ti))
        out[half - k] = (er - tr, subo(ti, ei))
    return out


def addo(a, b):
    return b if a is None else a + b


def subo(a, b):
    return a if b is None else a - b


def cmul(r, i, c, s):
    if i is None:
        return r * c, r * s
    if abs(abs(c) - abs(s)) < 1e-9:
        if s < 0 < c:
            return (r + i) * c, (i - r) * c
        return (r - i) * c, (r + i) * c
    return r * c - i * s, r * s + i * c


def irfft(spec, n):
    if n == 3:
        dc, (r, i) = spec[0][0], spec[1]
        base = dc - r
        t = i * np.sqrt(3.0)
        return [dc + 2.0 * r, base - t, base + t]
    half = n // 2
    even, odd = [None] * (half // 2 + 1), [None] * (half // 2 + 1)
    for k in range(half // 2 + 1):
        yr, yi = spec[k]
        if k == 0:
            hr = spec[half][0]
            even[0] = (yr + hr, None)
            odd[0] = (yr - hr, None)
            continue
        if 2 * k == half:
            even[k] = (yr + yr, None)
            odd[k] = (-(yi + yi), None)
            continue
        zr, zi = spec[half - k]
        er, ei = yr + zr, yi - zi
        dr, di = yr - zr, yi + zi
        c, s = np.cos(2 * np.pi * k / n), np.sin(2 * np.pi * k / n)
        even[k] = (er, ei)
        odd[k] = cmul(dr, di, c, s)
    ev, od = irfft(even, half), irfft(odd, half)
    out = [None] * n
    out[0::2], out[1::2] = ev, od
    return out


def split(v):
    hi = v.astype(jnp.bfloat16)
    lo = (v - hi.astype(jnp.float32)).astype(jnp.bfloat16)
    return hi, lo


def mm(a, b):
    return jnp.dot(a, b, preferred_element_type=jnp.float32)


def solve_kernel(ng, ncell, in_ref, *refs):
    tables, refs = refs[:7], refs[7:]
    (o_ref, m_ref, nat_ref, k1_ref, k2_ref, zt_ref, ty_ref, cp_ref, s_ref, hot_ref, own_ref, store, amp, acc, work, vec, recv, sel,
     rows_buf, mine, marg, rsem, ssem, gsem, ysem, usem, dsem, wsem, osem, orsem, msem, mrsem, lsem, csem, esem, isem, tmp, ebuf) = refs
    inputs = [pltpu.make_async_copy(in_ref.at[:, b], nat_ref.at[b], isem.at[b]) for b in range(in_ref.shape[1])]
    for copy in inputs:
        copy.start()
    kept = (k1_ref, k2_ref, zt_ref, ty_ref, cp_ref, s_ref, hot_ref)
    loads = [pltpu.make_async_copy(src, dst, csem.at[n]) for n, (src, dst) in enumerate(zip(tables, kept))]
    for n in (4, 2, 3, 0, 1, 5, 6):
        loads[n].start()
    bands = in_ref.shape[1]
    flat, width = own_ref.shape
    planes = flat // ng
    groups = vec.shape[0]
    me = lax.axis_index("grid")
    band, nband = lax.axis_index("band"), lax.axis_size("band")
    chip, core = me // 2, me % 2
    sib = chip * 2 + (1 - core)
    cross = (1 - chip) * 2 + core
    far = (1 - chip) * 2 + (1 - core)
    length = nband // 2
    side, pos = band % 2, band // 2
    pair = band + 1 - 2 * side
    third = (band + nband - 1 + 2 * side) % nband
    first, last = band == 0, band == nband - 1
    ends = jnp.logical_or(first, last)
    wrap = jnp.where(first, nband - 1, 0)
    has_up, has_down = pos < length - 1, pos > 0
    up, down = jnp.where(has_up, band + 2, band), jnp.where(has_down, band - 2, band)
    mesh_id = pl.DeviceIdType.MESH
    part = planes // 2

    def remote(src, dst, send, recv_sem, device):
        return pltpu.make_async_remote_copy(
            src_ref=src, dst_ref=dst, send_sem=send, recv_sem=recv_sem,
            device_id=device, device_id_type=mesh_id,
        )

    def partner(blk):
        return jnp.where(blk == 0, band, jnp.where(blk == 1, pair, third))

    def place(blk, slot):
        return jnp.where(slot == me, partner(blk), nband + blk * groups + slot)

    def piece(ref, c):
        return ref.at[pl.ds(c * part * ng, part * ng)]

    def share(blk, lane, slot, src, target, c):
        dst = store.at[nband + blk * groups + slot]
        return remote(piece(src, c), piece(dst, c), ssem.at[blk, lane, c], rsem.at[blk, slot, c], (band, target))

    def along(block, sems, device, c, src=None):
        dst = store.at[block]
        src = dst if src is None else src
        return remote(piece(src, c), piece(dst, c), sems.at[block, c], gsem.at[block, c], (device, me))

    def came(block, c):
        along(block, ysem, pair, c).wait_recv()

    lane = lax.broadcasted_iota(jnp.int32, (1, 128), 1)

    def moved(value, shift, low, high, under):
        out = pltpu.roll(value, shift % 128, 1) if shift % 128 else value
        return jnp.where(jnp.logical_and(lane >= low, lane < high), out, under)

    def gather_in(read, want, blank):
        for y0 in range(8):
            chunks = [None, None, None]
            for h in range(2):
                for b in range(bands):
                    for target, start, stop, base in ((h, 0, 128, 0), (2, 128, bands * ng, 64 * h)):
                        first, final = max(start, b * ng), min(stop, b * ng + ng)
                        if first >= final:
                            continue
                        source = y0 * ng + first - b * ng
                        place_at = first - start + base
                        while first < final:
                            q, off = source // 128, source % 128
                            size = min(final - first, 128 - off)
                            under = chunks[target]
                            under = blank if under is None else under
                            chunks[target] = moved(read(b, h, q), place_at - off, place_at, place_at + size, under)
                            first, source, place_at = first + size, source + size, place_at + size
            for j, value in enumerate(chunks):
                want(j, y0, value)

    def scatter_out(read, write, blank):
        for h in range(2):
            chunks = [blank] * 3
            for y0 in range(8):
                value = read(y0)
                source, at, left = h * ng, y0 * ng, ng
                while left > 0:
                    q, off = at // 128, at % 128
                    size = min(left, 128 - off)
                    chunks[q] = moved(value, off - source, off, off + size, chunks[q])
                    source, at, left = source + size, at + size, left - size
            for q in range(3):
                write(h, q, chunks[q])

    group = flat // 8

    def packed(h, q):
        return pl.ds(q + 3 * group * h, group, stride=3)

    def spaced(y0):
        return pl.ds(y0, group, stride=8)

    def greet(device):
        pl.semaphore_signal(barrier, inc=1, device_id=device, device_id_type=mesh_id)

    barrier = pltpu.get_barrier_semaphore()
    for device in ((band, sib), (band, cross), (band, far), (pair, me)):
        greet(device)

    @pl.when(has_up)
    def _():
        greet((up, me))

    @pl.when(has_down)
    def _():
        greet((down, me))

    @pl.when(ends)
    def _():
        greet((wrap, me))

    count = 4 + has_up.astype(jnp.int32) + has_down.astype(jnp.int32) + ends.astype(jnp.int32)
    def own_copies(c, act):
        def go(copy):
            copy.start() if act == "go" else copy.wait_send()

        go(share(0, 1, me, own_ref, cross, c))
        go(share(0, 0, me, own_ref, sib, c))
        go(along(band, ysem, pair, c, own_ref))

        @pl.when(has_up)
        def _():
            go(along(band, usem, up, c, own_ref))

        @pl.when(has_down)
        def _():
            go(along(band, dsem, down, c, own_ref))

    def wrap_copies(act):
        @pl.when(ends)
        def _():
            for c in range(2):
                copy = along(band, wsem, wrap, c, own_ref)
                copy.start() if act == "go" else copy.wait_send()

    def put_own(j, y0, value):
        ebuf[0, j, spaced(y0), :] = value

    for copy in inputs:
        copy.wait()
    gather_in(lambda b, h, q: nat_ref[b, packed(h, q), :], put_own, jnp.zeros((group, 128), jnp.float32))
    own_ref[...] = jnp.concatenate([ebuf[0, j] for j in range(3)], axis=1)
    pl.semaphore_wait(barrier, count)
    for c in range(2):
        own_copies(c, "go")
    wrap_copies("go")
    local = pltpu.make_async_copy(own_ref, store.at[band], lsem)
    local.start()

    def arrived(blk, slot, c):
        share(blk, 0, slot, own_ref, sib, c).wait_recv()

    def relay(blk, c):
        arrived(blk, cross, c)
        share(blk, 2, cross, store.at[nband + blk * groups + cross], sib, c).start()

    def spread(blk, c):
        came(partner(blk), c)
        share(blk, 1, me, store.at[partner(blk)], cross, c).start()
        share(blk, 0, me, store.at[partner(blk)], sib, c).start()

    def skipped(block):
        return jnp.logical_or(
            jnp.logical_and(pair == 0, block == nband - 1), jnp.logical_and(pair == nband - 1, block == 0)
        )

    def line(d, c, near, act):
        def pass_on(block, exists, on, sems, device):
            @pl.when(exists)
            def _():
                if act == "go":
                    came(block, c)

                def one(copy):
                    copy.start() if act == "go" else copy.wait_send()

                @pl.when(jnp.logical_not(skipped(block)))
                def _():
                    one(along(block, ysem, pair, c))

                @pl.when(on)
                def _():
                    one(along(block, sems, device, c))

        upward = (side == 1) == near
        pass_on(band - 2 * d, jnp.logical_and(upward, pos - d >= 0), has_up, usem, up)
        pass_on(
            band + 2 * d, jnp.logical_and(jnp.logical_not(upward), pos + d <= length - 1), has_down, dsem, down
        )

    def serve(blk, c):
        @pl.when(blk < 2)
        def _():
            spread(blk + 1, c)

        line(blk + 1, c, True, "go")

    def ztrans(v):
        hi, lo = split(v)
        parts = []
        for h in range(2):
            a, b = (jnp.concatenate([t[:, 128 * h:128 * h + 128], t[:, 256:]], axis=1) for t in (hi, lo))
            parts.append(mm(a, zt_ref[h, 0]) + mm(b, zt_ref[h, 0]) + mm(a, zt_ref[h, 1]))
        return jnp.concatenate([parts[0][:, :128], parts[1][:, :128], parts[0][:, 128:] + parts[1][:, 128:]], axis=1)

    def ytrans(v):
        hi, lo = split(v)
        return mm(ty_ref[...], jnp.concatenate([hi, lo, hi], axis=0))

    def amplitude(v):
        hi, lo = split(v)
        parts = []
        for h in range(2):
            a, b = (jnp.concatenate([t[:, 128 * h:128 * h + 128], t[:, 256:]], axis=1) for t in (hi, lo))
            parts.append(mm(a, sel[h]) + mm(b, sel[h]))
        return jnp.concatenate([parts[0][:, :128], parts[1][:, :128], parts[0][:, 128:] + parts[1][:, 128:]], axis=1)

    for n in (4, 2, 3):
        loads[n].wait()
    for h in range(2):
        mark = (me + 1).astype(jnp.float32)
        sel[h] = jnp.where(cp_ref[h].astype(jnp.float32) == mark, 1.0, 0.0).astype(jnp.bfloat16)

    def transform(blk, slots, c):
        rows = pl.ds(c * part * ng, part * ng)

        @pl.when(blk == 0)
        def _():
            own = jnp.concatenate([store[place(0, slot), rows] for slot in slots], axis=0)
            out = amplitude(own).reshape(len(slots), part * ng, width)
            for n, slot in enumerate(slots):
                amp[slot, rows] = out[n]

        p = jnp.concatenate([amp[slot, rows] * store[place(blk, slot), rows] for slot in slots], axis=0)
        q = ztrans(p).reshape(len(slots), part, ng, width)
        for n, slot in enumerate(slots):
            for r in range(part):
                work[slot, c * part + r] = ytrans(q[n, r])

    def near(blk, c):
        arrived(blk, sib, c)

        @pl.when(jnp.logical_and(blk > 0, c == 1))
        def _():
            relay(blk, 0)

        transform(blk, (me, sib), c)

    def other(blk, i):
        c = i // 2

        @pl.when(jnp.logical_and(blk == 0, i == 0))
        def _():
            serve(blk, 0)
            relay(blk, 0)

        @pl.when(i == 1)
        def _():
            serve(blk, 1)
            relay(blk, 1)

        @pl.when(i % 2 == 1)
        def _():
            arrived(blk, far, c)

        @pl.when(jnp.logical_and(blk > 0, i == 2))
        def _():
            line(blk, 1, False, "go")

        transform(blk, (jnp.where(i % 2 == 0, cross, far),), c)

    def conv(vals, kern):
        spec = rfft(vals)
        out = []
        for k, (re, im) in enumerate(spec):
            kv = kern(k)
            out.append((re * kv, None if im is None else im * kv))
        return irfft(out, ng)

    def xconv(t):
        order = [(g, h, r) for g in range(4) for h in range(2) for r in range(planes)]
        for i in range(2):
            rows = pl.ds(pl.multiple_of(t * 16 + 8 * i, 8), 8)
            res = conv([work[g, r, rows, h * 128:h * 128 + 128] for g, h, r in order],
                       lambda k: k1_ref[k, rows, :])
            for (g, h, r), v in zip(order, res):
                work[g, r, rows, h * 128:h * 128 + 128] = v
        ra = pl.ds(pl.multiple_of(t * 16, 8), 8)
        rb = pl.ds(pl.multiple_of(t * 16 + 8, 8), 8)
        left = lax.broadcasted_iota(jnp.int32, (8, 128), 1) < 64

        def half(g, h, r):
            u, w = work[g, r, ra, 256:384], work[g, r, rb, 256:384]
            if h == 0:
                return jnp.where(left, u, pltpu.roll(w, 64, 1))
            return jnp.where(left, pltpu.roll(u, 64, 1), w)

        rk = pl.ds(pl.multiple_of(t * 8, 8), 8)
        res = dict(zip(order, conv([half(*o) for o in order], lambda k: k2_ref[k, rk, :])))
        for g in range(4):
            for r in range(planes):
                a, b = res[(g, 0, r)], res[(g, 1, r)]
                work[g, r, ra, 256:384] = jnp.where(left, a, pltpu.roll(b, 64, 1))
                work[g, r, rb, 256:384] = jnp.where(left, pltpu.roll(a, 64, 1), b)

    def push(slot):
        return remote(vec.at[slot], recv.at[me], osem.at[slot], orsem.at[me], (band, slot))

    def inverse(blk, s):
        slot = ((chip + 1 - s // 2) % 2) * 2 + (core + s % 2 + s // 2) % 2
        q = jnp.concatenate([ytrans(work[slot, r]) for r in range(planes)], axis=0)
        w = ztrans(q) * store[place(blk, slot)]

        @pl.when(jnp.logical_and(blk < 2, s == 2))
        def _():
            serve(blk + 1, 0)
            line(blk + 1, 0, False, "go")

        @pl.when(blk == 0)
        def _():
            acc[slot] = w

        @pl.when(blk == 1)
        def _():
            acc[slot] += w

        @pl.when(blk == 2)
        def _():
            hi, lo = split(acc[slot] + w)
            tmp[...] = -(mm(hi, s_ref[...]) + mm(lo, s_ref[...]))

            def put_vec(h, q, value):
                vec[slot, packed(h, q), :] = value

            scatter_out(lambda y0: tmp[spaced(y0), :], put_vec, jnp.zeros((group, 128), jnp.float32))

            @pl.when(s < 3)
            def _():
                push(slot).start()

    def block(blk, _):
        @pl.when(blk == 0)
        def _():
            local.wait()

        def fwd_near(c, _):
            near(blk, c)
            return 0

        def fwd_other(i, _):
            other(blk, i)
            return 0

        def mid(t, _):
            xconv(t)
            return 0

        def inv(s, _):
            inverse(blk, s)
            return 0

        lax.fori_loop(0, 2, fwd_near, 0)
        lax.fori_loop(0, 4, fwd_other, 0)

        @pl.when(blk == 0)
        def _():
            for n in (0, 1, 5, 6):
                loads[n].wait()

        lax.fori_loop(0, ng // 16, mid, 0)
        lax.fori_loop(0, 4, inv, 0)
        return 0

    lax.fori_loop(0, 3, block, 0)

    def later(d, _):
        for c in range(2):
            line(d, c, False, "go")
            line(d + 1, c, True, "go")
        return 0

    lax.fori_loop(3, length, later, 0)

    def emit(src, slot):
        return pltpu.make_async_copy(src.at[slot], o_ref.at[:, slot], esem.at[slot])

    def spread_out(src, slot, n):
        def put(j, y0, value):
            ebuf[n, j, spaced(y0), :] = value

        values = {(h, q): src[slot, packed(h, q), :] for h in range(2) for q in range(3)}
        gather_in(lambda b, h, q: values[h, q], put, jnp.zeros((group, 128), jnp.float32))

    def columns(block, slots):
        parts = [[jnp.zeros((8, 128), jnp.float32) for _ in range(3)] for _ in slots]
        for r in range(flat // 8):
            for j in range(3):
                phi = store[block, pl.ds(8 * r, 8), pl.ds(128 * j, 128)]
                for n, p in enumerate(parts):
                    p[j] = p[j] + phi * ebuf[n, j, pl.ds(8 * r, 8)]
        for slot, p in zip(slots, parts):
            rows_buf[slot, block] = jnp.concatenate(p, axis=1)

    def ready(block):
        near_by = jnp.logical_or(block == pair, block == third)
        return jnp.logical_or(near_by, block % 2 == side)

    def early(block, _):
        @pl.when(ready(block))
        def _():
            columns(block, (me, sib))

        return 0

    def late(block, _):
        @pl.when(jnp.logical_not(ready(block)))
        def _():
            for c in range(2):
                came(block, c)
            columns(block, (me, sib))

        return 0

    def rest(block, _):
        columns(block, (cross, far))
        return 0

    def settle(slot):
        remote(vec.at[slot], recv.at[slot], osem.at[slot], orsem.at[slot], (band, slot)).wait()
        emit(recv, slot).start()

    emit(vec, me).start()
    spread_out(vec, me, 0)
    settle(sib)
    spread_out(recv, sib, 1)
    lax.fori_loop(0, nband, early, 0)
    lax.fori_loop(0, nband, late, 0)
    settle(cross)
    spread_out(recv, cross, 0)
    settle(far)
    spread_out(recv, far, 1)
    lax.fori_loop(0, nband, rest, 0)

    lanes = jnp.sum(rows_buf[...], axis=2).reshape(groups * nband, width)
    left_over = lanes
    terms = jnp.zeros((groups * nband, hot_ref.shape[-1]), jnp.float32)
    for _ in range(3):
        hi = left_over.astype(jnp.bfloat16)
        terms += mm(hi, hot_ref[...])
        left_over = left_over - hi.astype(jnp.float32)
    terms = (terms / ncell).reshape(groups, nband, terms.shape[-1])
    each = nband // groups
    for slot in range(groups):
        total = jnp.zeros((groups, terms.shape[-1]), jnp.float32)
        for n in range(each):
            value = terms[:, slot * each + n]
            total += pltpu.roll(value, bands * n, 1) if n else value
        mine[slot] = total

    def give(slot):
        return remote(mine.at[slot], marg.at[me], msem.at[slot], mrsem.at[me], (band, slot))

    for slot in (cross, far, sib):
        give(slot).start()
    for slot in range(groups):
        emit(recv, slot).wait()
    wrap_copies("end")
    for c in range(2):
        own_copies(c, "end")

    def finish(i, _):
        blk, c = 1 + i // 2, i % 2
        for lane, target in ((0, sib), (1, cross)):
            share(blk, lane, me, own_ref, target, c).wait_send()
        return 0

    def finish_relay(i, _):
        share(i // 2, 2, me, own_ref, sib, i % 2).wait_send()
        return 0

    def finish_line(i, _):
        line(1 + i // 2, i % 2, True, "end")
        line(1 + i // 2, i % 2, False, "end")
        return 0

    lax.fori_loop(0, 4, finish, 0)
    lax.fori_loop(0, 6, finish_relay, 0)
    lax.fori_loop(0, 2 * (length - 1), finish_line, 0)
    total = mine[me]
    for slot in (sib, cross, far):
        remote(mine.at[slot], marg.at[slot], msem.at[slot], mrsem.at[slot], (band, slot)).wait()
        total += marg[slot]
    m_ref[...] = total[:, :nband]


def lane_tables(ng, bands):
    w = bands * ng
    half, bz = [], []
    for lo, hi in ((0, 128), (128, w)):
        for h in range(2):
            half.append(np.full(hi - lo, h))
            bz.append(np.arange(lo, hi))
    half, bz = np.concatenate(half), np.concatenate(bz)
    return half, bz // ng, bz % ng


def tiles(table, half):
    out = []
    for h in range(2):
        pick = np.concatenate([np.arange(128 * h, 128 * h + 128), np.arange(256, len(half))])
        live = half[pick] == h
        out.append(np.where(live[:, None] & live[None, :], table[pick][:, pick], 0.0))
    return np.stack(out)


def solve(nat, ng, groups, nband):
    bands = nat.shape[1]
    width = 2 * bands * ng
    flat = nat.shape[0] * nat.shape[2] // (2 * ng)
    half, bnd, zed = lane_tables(ng, bands)
    ht = hartley(ng)
    th, tl = split_const(ht)
    same = (half[:, None] == half[None, :])
    zmat = np.where(same & (bnd[:, None] == bnd[None, :]), ht[zed[:, None], zed[None, :]], 0.0)
    zt = np.stack(split_const(tiles(zmat, half)), axis=1)
    ty = np.concatenate([th, th, tl], axis=1)
    cp = tiles(np.where(same & (zed[:, None] == zed[None, :]), bnd[:, None] + 1.0, 0.0), half)
    s = np.zeros((width, 128), np.float32)
    s[np.arange(width), half * ng + zed] = 1.0
    hot = np.zeros((width, 128), np.float32)
    hot[np.arange(width), bnd] = 1.0
    kv = kernel_values(ng).astype(np.float32) / np.float32(ng**3)
    kb = np.tile(kv, (1, 1, bands))
    k1 = kb[:, :, :128]
    rest = kb[:, :, 128:].reshape(kb.shape[0], ng // 16, 2, 8, 64)
    k2 = np.concatenate([rest[:, :, 0], rest[:, :, 1]], axis=-1).reshape(kb.shape[0], ng // 2, 128)
    b16 = jnp.bfloat16
    consts = [k1, k2, zt, ty, cp.astype(b16), s.astype(b16), hot.astype(b16)]
    full = (groups, flat, width)
    slim = (groups, nat.shape[0], nat.shape[2])
    f32, dma = jnp.float32, pltpu.SemaphoreType.DMA
    return pl.pallas_call(
        functools.partial(solve_kernel, ng, ng**3),
        out_shape=(
            jax.ShapeDtypeStruct(nat.shape, f32), jax.ShapeDtypeStruct((groups, nband), f32)
        ),
        in_specs=[pl.BlockSpec(memory_space=pl.ANY)] * (1 + len(consts)),
        out_specs=(pl.BlockSpec(memory_space=pl.ANY), pl.BlockSpec(memory_space=pltpu.VMEM)),
        scratch_shapes=[
            pltpu.VMEM((bands,) + slim[1:], f32), *[pltpu.VMEM(c.shape, c.dtype) for c in consts],
            pltpu.VMEM(full[1:], f32), pltpu.VMEM((nband + 3 * groups,) + full[1:], f32),
            pltpu.VMEM(full, f32), pltpu.VMEM(full, f32), pltpu.VMEM((groups, flat // ng, ng, width), f32),
            pltpu.VMEM(slim, f32), pltpu.VMEM(slim, f32),
            pltpu.VMEM((2, 256, 256), b16), pltpu.VMEM((groups, nband, 8, width), f32),
            pltpu.VMEM((groups, groups, 128), f32), pltpu.VMEM((groups, groups, 128), f32),
            dma((3, groups, 2)), dma((3, 3, 2)), dma((nband, 2)), dma((nband, 2)), dma((nband, 2)), dma((nband, 2)),
            dma((nband, 2)),
            dma((groups,)), dma((groups,)), dma((groups,)), dma((groups,)), dma(()), dma((len(consts),)), dma((groups,)), dma((bands,)),
            pltpu.VMEM((flat, 128), f32), pltpu.VMEM((2, 3, flat, 128), f32),
        ],
        compiler_params=pltpu.CompilerParams(
            vmem_limit_bytes=60 * 1024 * 1024, collective_id=0, has_side_effects=True
        ),
        cost_estimate=pl.CostEstimate(flops=10**11, bytes_accessed=10**7, transcendentals=0),
        name="solve",
    )(nat, *[jnp.asarray(c) for c in consts])


def on_device(orbitals):
    groups, nband = lax.axis_size("grid"), lax.axis_size("band")
    bands, local = orbitals.shape
    ncell = local * groups
    ng = round(ncell ** (1 / 3))
    nat = orbitals.reshape(bands, local // 128, 128).transpose(1, 0, 2)
    out, marg = solve(nat, ng, groups, nband)
    vectors = out.transpose(1, 0, 2).reshape(bands, local)
    margin = marg.T
    return (vectors, margin)


def solution(mesh):
    return jax.shard_map(
        on_device,
        mesh=mesh,
        in_specs=(P("band", "grid"),),
        out_specs=(P("band", "grid"), P("grid", "band")),
        check_vma=False,
    )
```

```python
import functools

import jax
import jax.numpy as jnp
import numpy as np
from jax import lax
from jax.experimental import pallas as pl
from jax.experimental.pallas import tpu as pltpu
from jax.sharding import PartitionSpec as P


def kernel_values(ng):
    freqs = ((np.arange(ng) + ng // 2) % ng - ng // 2).astype(np.float32)
    sq = freqs[: ng // 2 + 1, None, None] ** 2 + freqs[None, :, None] ** 2 + freqs[None, None, :] ** 2
    safe = np.where(sq > 0, sq, np.float32(1.0))
    return np.where(sq > 0, 40.0 * (1.0 - np.exp(-sq / 16.0)) / safe, 0.0)


def hartley(ng):
    k = np.arange(ng)
    ang = (k[:, None] * k[None, :] % ng) * (2.0 * np.pi / ng)
    return np.cos(ang) + np.sin(ang)


def split_const(table):
    table = np.asarray(table, np.float32)
    hi = table.astype(jnp.bfloat16)
    lo = (table - hi.astype(np.float32)).astype(jnp.bfloat16)
    return hi, lo


def rfft(xs):
    n = len(xs)
    if n == 3:
        s = xs[1] + xs[2]
        d = xs[1] - xs[2]
        return [(xs[0] + s, None), (xs[0] - 0.5 * s, d * (-np.sqrt(3.0) / 2))]
    even, odd = rfft(xs[0::2]), rfft(xs[1::2])
    half = n // 2
    out = [None] * (half + 1)
    for k in range(half // 2 + 1):
        er, ei = even[k]
        orr, oi = odd[k]
        if k == 0:
            out[0] = (er + orr, None)
            out[half] = (er - orr, None)
            continue
        c, s = np.cos(2 * np.pi * k / n), -np.sin(2 * np.pi * k / n)
        if 2 * k == half:
            out[k] = (er, -orr)
            continue
        tr, ti = cmul(orr, oi, c, s)
        out[k] = (er + tr, addo(ei, ti))
        out[half - k] = (er - tr, subo(ti, ei))
    return out


def addo(a, b):
    return b if a is None else a + b


def subo(a, b):
    return a if b is None else a - b


def cmul(r, i, c, s):
    if i is None:
        return r * c, r * s
    if abs(abs(c) - abs(s)) < 1e-9:
        if s < 0 < c:
            return (r + i) * c, (i - r) * c
        return (r - i) * c, (r + i) * c
    return r * c - i * s, r * s + i * c


def irfft(spec, n):
    if n == 3:
        dc, (r, i) = spec[0][0], spec[1]
        base = dc - r
        t = i * np.sqrt(3.0)
        return [dc + 2.0 * r, base - t, base + t]
    half = n // 2
    even, odd = [None] * (half // 2 + 1), [None] * (half // 2 + 1)
    for k in range(half // 2 + 1):
        yr, yi = spec[k]
        if k == 0:
            hr = spec[half][0]
            even[0] = (yr + hr, None)
            odd[0] = (yr - hr, None)
            continue
        if 2 * k == half:
            even[k] = (yr + yr, None)
            odd[k] = (-(yi + yi), None)
            continue
        zr, zi = spec[half - k]
        er, ei = yr + zr, yi - zi
        dr, di = yr - zr, yi + zi
        c, s = np.cos(2 * np.pi * k / n), np.sin(2 * np.pi * k / n)
        even[k] = (er, ei)
        odd[k] = cmul(dr, di, c, s)
    ev, od = irfft(even, half), irfft(odd, half)
    out = [None] * n
    out[0::2], out[1::2] = ev, od
    return out


def split(v):
    hi = v.astype(jnp.bfloat16)
    lo = (v - hi.astype(jnp.float32)).astype(jnp.bfloat16)
    return hi, lo


def mm(a, b):
    return jnp.dot(a, b, preferred_element_type=jnp.float32)


def in_copies(in_ref, nat_ref, sems, c):
    size = nat_ref.shape[3]
    return [
        pltpu.make_async_copy(in_ref.at[pl.ds((2 * h + c) * size, size), b], nat_ref.at[h, c, b], sems.at[h, c, b])
        for h in range(2)
        for b in range(in_ref.shape[1])
    ]


def solve_kernel(ng, ncell, in_ref, *refs):
    (k_hbm, t_hbm, o_ref, m_ref, nat_ref, k_ref, t_ref, own_ref, store, amp, acc, work, vec, recv, sel, rows_buf, mine, marg,
     rsem, ssem, gsem, ysem, usem, dsem, wsem, osem, orsem, msem, mrsem, lsem, csem, esem, isem, tmp, ebuf) = refs
    for copy in in_copies(in_ref, nat_ref, isem, 0) + in_copies(in_ref, nat_ref, isem, 1):
        copy.start()
    load_t = pltpu.make_async_copy(t_hbm, t_ref, csem.at[0])
    load_k = pltpu.make_async_copy(k_hbm, k_ref, csem.at[1])
    load_t.start()
    load_k.start()
    bands = in_ref.shape[1]
    flat, width = own_ref.shape
    planes = flat // ng
    groups = vec.shape[0]
    me = lax.axis_index("grid")
    band, nband = lax.axis_index("band"), lax.axis_size("band")
    chip, core = me // 2, me % 2
    sib = chip * 2 + (1 - core)
    cross = (1 - chip) * 2 + core
    far = (1 - chip) * 2 + (1 - core)
    length = nband // 2
    side, pos = band % 2, band // 2
    pair = band + 1 - 2 * side
    third = (band + nband - 1 + 2 * side) % nband
    first, last = band == 0, band == nband - 1
    ends = jnp.logical_or(first, last)
    wrap = jnp.where(first, nband - 1, 0)
    has_up, has_down = pos < length - 1, pos > 0
    up, down = jnp.where(has_up, band + 2, band), jnp.where(has_down, band - 2, band)
    mesh_id = pl.DeviceIdType.MESH
    part = planes // 2
    zrow, crow = 256, 1024
    srow = crow + 512
    yrow = srow + width

    def remote(src, dst, send, recv_sem, device):
        return pltpu.make_async_remote_copy(
            src_ref=src, dst_ref=dst, send_sem=send, recv_sem=recv_sem,
            device_id=device, device_id_type=mesh_id,
        )

    def partner(blk):
        return jnp.where(blk == 0, band, jnp.where(blk == 1, pair, third))

    def place(blk, slot):
        return jnp.where(slot == me, partner(blk), nband + blk * groups + slot)

    def piece(ref, c):
        return ref.at[pl.ds(c * part * ng, part * ng)]

    def share(blk, lane, slot, src, target, c):
        dst = store.at[nband + blk * groups + slot]
        return remote(piece(src, c), piece(dst, c), ssem.at[blk, lane, c], rsem.at[blk, slot, c], (band, target))

    def along(block, sems, device, c, src=None):
        dst = store.at[block]
        src = dst if src is None else src
        return remote(piece(src, c), piece(dst, c), sems.at[block, c], gsem.at[block, c], (device, me))

    def came(block, c):
        along(block, ysem, pair, c).wait_recv()

    lane = lax.broadcasted_iota(jnp.int32, (1, 128), 1)

    def moved(value, shift, low, high, under):
        out = pltpu.roll(value, shift % 128, 1) if shift % 128 else value
        return jnp.where(jnp.logical_and(lane >= low, lane < high), out, under)

    def gather_in(read, want, blank):
        for y0 in range(8):
            chunks = [None, None, None]
            for h in range(2):
                for b in range(bands):
                    for target, start, stop, base in ((h, 0, 128, 0), (2, 128, bands * ng, 64 * h)):
                        first, final = max(start, b * ng), min(stop, b * ng + ng)
                        if first >= final:
                            continue
                        source = y0 * ng + first - b * ng
                        place_at = first - start + base
                        while first < final:
                            q, off = source // 128, source % 128
                            size = min(final - first, 128 - off)
                            under = chunks[target]
                            under = blank if under is None else under
                            chunks[target] = moved(read(b, h, q), place_at - off, place_at, place_at + size, under)
                            first, source, place_at = first + size, source + size, place_at + size
            for j, value in enumerate(chunks):
                want(j, y0, value)

    def scatter_out(read, write, blank):
        for h in range(2):
            chunks = [blank] * 3
            for y0 in range(8):
                value = read(y0)
                source, at, left = h * ng, y0 * ng, ng
                while left > 0:
                    q, off = at // 128, at % 128
                    size = min(left, 128 - off)
                    chunks[q] = moved(value, off - source, off, off + size, chunks[q])
                    source, at, left = source + size, at + size, left - size
            for q in range(3):
                write(h, q, chunks[q])

    group = flat // 8

    def packed(h, q):
        return pl.ds(q + 3 * group * h, group, stride=3)

    def spaced(y0):
        return pl.ds(y0, group, stride=8)

    def greet(device):
        pl.semaphore_signal(barrier, inc=1, device_id=device, device_id_type=mesh_id)

    barrier = pltpu.get_barrier_semaphore()
    for device in ((band, sib), (band, cross), (band, far), (pair, me)):
        greet(device)

    @pl.when(has_up)
    def _():
        greet((up, me))

    @pl.when(has_down)
    def _():
        greet((down, me))

    @pl.when(ends)
    def _():
        greet((wrap, me))

    count = 4 + has_up.astype(jnp.int32) + has_down.astype(jnp.int32) + ends.astype(jnp.int32)
    def own_copies(c, act):
        def go(copy):
            copy.start() if act == "go" else copy.wait_send()

        go(share(0, 1, me, own_ref, cross, c))
        go(share(0, 0, me, own_ref, sib, c))
        go(along(band, ysem, pair, c, own_ref))

        @pl.when(has_up)
        def _():
            go(along(band, usem, up, c, own_ref))

        @pl.when(has_down)
        def _():
            go(along(band, dsem, down, c, own_ref))

    def wrap_copies(act):
        @pl.when(ends)
        def _():
            for c in range(2):
                copy = along(band, wsem, wrap, c, own_ref)
                copy.start() if act == "go" else copy.wait_send()

    few = group // 2
    for c in range(2):
        for copy in in_copies(in_ref, nat_ref, isem, c):
            copy.wait()

        def put_own(j, y0, value):
            ebuf[0, j, pl.ds(c * part * ng + y0, few, stride=8), :] = value

        gather_in(
            lambda b, h, q: nat_ref[h, c, b, pl.ds(q, few, stride=3), :], put_own, jnp.zeros((few, 128), jnp.float32)
        )
        half_rows = pl.ds(c * part * ng, part * ng)
        own_ref[half_rows, :] = jnp.concatenate([ebuf[0, j, half_rows, :] for j in range(3)], axis=1)
        if c == 0:
            pl.semaphore_wait(barrier, count)
        own_copies(c, "go")
    wrap_copies("go")
    local = pltpu.make_async_copy(own_ref, store.at[band], lsem)
    local.start()

    def arrived(blk, slot, c):
        share(blk, 0, slot, own_ref, sib, c).wait_recv()

    def relay(blk, c):
        arrived(blk, cross, c)
        share(blk, 2, cross, store.at[nband + blk * groups + cross], sib, c).start()

    def spread(blk, c):
        came(partner(blk), c)
        share(blk, 1, me, store.at[partner(blk)], cross, c).start()
        share(blk, 0, me, store.at[partner(blk)], sib, c).start()

    def skipped(block):
        return jnp.logical_or(
            jnp.logical_and(pair == 0, block == nband - 1), jnp.logical_and(pair == nband - 1, block == 0)
        )

    def line(d, c, near, act):
        def pass_on(block, exists, on, sems, device):
            @pl.when(exists)
            def _():
                if act == "go":
                    came(block, c)

                def one(copy):
                    copy.start() if act == "go" else copy.wait_send()

                @pl.when(jnp.logical_not(skipped(block)))
                def _():
                    one(along(block, ysem, pair, c))

                @pl.when(on)
                def _():
                    one(along(block, sems, device, c))

        upward = (side == 1) == near
        pass_on(band - 2 * d, jnp.logical_and(upward, pos - d >= 0), has_up, usem, up)
        pass_on(
            band + 2 * d, jnp.logical_and(jnp.logical_not(upward), pos + d <= length - 1), has_down, dsem, down
        )

    def serve(blk, c):
        @pl.when(blk < 2)
        def _():
            spread(blk + 1, c)

        line(blk + 1, c, True, "go")

    def ztrans(v):
        hi, lo = split(v)
        parts = []
        for h in range(2):
            a, b = (jnp.concatenate([t[:, 128 * h:128 * h + 128], t[:, 256:]], axis=1) for t in (hi, lo))
            high, low = (t_ref[pl.ds((2 * h + n) * zrow, zrow), :] for n in range(2))
            parts.append(mm(a, high) + mm(b, high) + mm(a, low))
        return jnp.concatenate([parts[0][:, :128], parts[1][:, :128], parts[0][:, 128:] + parts[1][:, 128:]], axis=1)

    def ytrans(v):
        hi, lo = split(v)
        return mm(t_ref[pl.ds(yrow, ng), pl.ds(0, 3 * ng)], jnp.concatenate([hi, lo, hi], axis=0))

    def amplitude(v):
        hi, lo = split(v)
        parts = []
        for h in range(2):
            a, b = (jnp.concatenate([t[:, 128 * h:128 * h + 128], t[:, 256:]], axis=1) for t in (hi, lo))
            parts.append(mm(a, sel[h]) + mm(b, sel[h]))
        return jnp.concatenate([parts[0][:, :128], parts[1][:, :128], parts[0][:, 128:] + parts[1][:, 128:]], axis=1)

    load_t.wait()
    for h in range(2):
        mark = (me + 1).astype(jnp.float32)
        sel[h] = jnp.where(t_ref[pl.ds(crow + zrow * h, zrow), :].astype(jnp.float32) == mark, 1.0, 0.0).astype(jnp.bfloat16)

    def transform(blk, slots, c):
        rows = pl.ds(c * part * ng, part * ng)

        @pl.when(blk == 0)
        def _():
            own = jnp.concatenate([store[place(0, slot), rows] for slot in slots], axis=0)
            out = amplitude(own).reshape(len(slots), part * ng, width)
            for n, slot in enumerate(slots):
                amp[slot, rows] = out[n]

        p = jnp.concatenate([amp[slot, rows] * store[place(blk, slot), rows] for slot in slots], axis=0)
        q = ztrans(p).reshape(len(slots), part, ng, width)
        for n, slot in enumerate(slots):
            for r in range(part):
                work[slot, c * part + r] = ytrans(q[n, r])

    def near(blk, c):
        arrived(blk, sib, c)

        @pl.when(jnp.logical_and(blk > 0, c == 1))
        def _():
            relay(blk, 0)

        transform(blk, (me, sib), c)

    def other(blk, i):
        c = i // 2

        @pl.when(jnp.logical_and(blk == 0, i == 0))
        def _():
            serve(blk, 0)
            relay(blk, 0)

        @pl.when(i == 1)
        def _():
            serve(blk, 1)
            relay(blk, 1)

        @pl.when(i % 2 == 1)
        def _():
            arrived(blk, far, c)

        @pl.when(jnp.logical_and(blk > 0, i == 2))
        def _():
            line(blk, 1, False, "go")

        transform(blk, (jnp.where(i % 2 == 0, cross, far),), c)

    def conv(vals, kern):
        spec = rfft(vals)
        out = []
        for k, (re, im) in enumerate(spec):
            kv = kern(k)
            out.append((re * kv, None if im is None else im * kv))
        return irfft(out, ng)

    def xconv(t):
        order = [(g, h, r) for g in range(4) for h in range(2) for r in range(planes)]
        for i in range(2):
            rows = pl.ds(pl.multiple_of(t * 16 + 8 * i, 8), 8)
            res = conv([work[g, r, rows, h * 128:h * 128 + 128] for g, h, r in order],
                       lambda k: k_ref[k, rows, :])
            for (g, h, r), v in zip(order, res):
                work[g, r, rows, h * 128:h * 128 + 128] = v
        ra = pl.ds(pl.multiple_of(t * 16, 8), 8)
        rb = pl.ds(pl.multiple_of(t * 16 + 8, 8), 8)
        left = lax.broadcasted_iota(jnp.int32, (8, 128), 1) < 64

        def half(g, h, r):
            u, w = work[g, r, ra, 256:384], work[g, r, rb, 256:384]
            if h == 0:
                return jnp.where(left, u, pltpu.roll(w, 64, 1))
            return jnp.where(left, pltpu.roll(u, 64, 1), w)

        rk = pl.ds(pl.multiple_of(ng + t * 8, 8), 8)
        res = dict(zip(order, conv([half(*o) for o in order], lambda k: k_ref[k, rk, :])))
        for g in range(4):
            for r in range(planes):
                a, b = res[(g, 0, r)], res[(g, 1, r)]
                work[g, r, ra, 256:384] = jnp.where(left, a, pltpu.roll(b, 64, 1))
                work[g, r, rb, 256:384] = jnp.where(left, pltpu.roll(a, 64, 1), b)

    def push(slot):
        return remote(vec.at[slot], recv.at[me], osem.at[slot], orsem.at[me], (band, slot))

    def inverse(blk, s):
        slot = ((chip + 1 - s // 2) % 2) * 2 + (core + s % 2 + s // 2) % 2
        q = jnp.concatenate([ytrans(work[slot, r]) for r in range(planes)], axis=0)
        w = ztrans(q) * store[place(blk, slot)]

        @pl.when(jnp.logical_and(blk < 2, s == 2))
        def _():
            serve(blk + 1, 0)
            line(blk + 1, 0, False, "go")

        @pl.when(blk == 0)
        def _():
            acc[slot] = w

        @pl.when(blk == 1)
        def _():
            acc[slot] += w

        @pl.when(blk == 2)
        def _():
            hi, lo = split(acc[slot] + w)
            s_tab = t_ref[pl.ds(srow, width), pl.ds(0, 128)]
            tmp[...] = -(mm(hi, s_tab) + mm(lo, s_tab))

            def put_vec(h, q, value):
                vec[slot, packed(h, q), :] = value

            scatter_out(lambda y0: tmp[spaced(y0), :], put_vec, jnp.zeros((group, 128), jnp.float32))

            @pl.when(s < 3)
            def _():
                push(slot).start()

    def block(blk, _):
        @pl.when(blk == 0)
        def _():
            local.wait()

        def fwd_near(c, _):
            near(blk, c)
            return 0

        def fwd_other(i, _):
            other(blk, i)
            return 0

        def mid(t, _):
            xconv(t)
            return 0

        def inv(s, _):
            inverse(blk, s)
            return 0

        lax.fori_loop(0, 2, fwd_near, 0)
        lax.fori_loop(0, 4, fwd_other, 0)

        @pl.when(blk == 0)
        def _():
            load_k.wait()

        lax.fori_loop(0, ng // 16, mid, 0)
        lax.fori_loop(0, 4, inv, 0)
        return 0

    lax.fori_loop(0, 3, block, 0)

    def later(d, _):
        for c in range(2):
            line(d, c, False, "go")
            line(d + 1, c, True, "go")
        return 0

    lax.fori_loop(3, length, later, 0)

    def emit(src, slot):
        return pltpu.make_async_copy(src.at[slot], o_ref.at[:, slot], esem.at[slot])

    def spread_out(src, slot, n):
        def put(j, y0, value):
            ebuf[n, j, spaced(y0), :] = value

        values = {(h, q): src[slot, packed(h, q), :] for h in range(2) for q in range(3)}
        gather_in(lambda b, h, q: values[h, q], put, jnp.zeros((group, 128), jnp.float32))

    def columns(block, slots):
        parts = [[jnp.zeros((8, 128), jnp.float32) for _ in range(3)] for _ in slots]
        for r in range(flat // 8):
            for j in range(3):
                phi = store[block, pl.ds(8 * r, 8), pl.ds(128 * j, 128)]
                for n, p in enumerate(parts):
                    p[j] = p[j] + phi * ebuf[n, j, pl.ds(8 * r, 8)]
        for slot, p in zip(slots, parts):
            rows_buf[slot, block] = jnp.concatenate(p, axis=1)

    def ready(block):
        near_by = jnp.logical_or(block == pair, block == third)
        return jnp.logical_or(near_by, block % 2 == side)

    def early(block, _):
        @pl.when(ready(block))
        def _():
            columns(block, (me, sib))

        return 0

    def late(block, _):
        @pl.when(jnp.logical_not(ready(block)))
        def _():
            for c in range(2):
                came(block, c)
            columns(block, (me, sib))

        return 0

    def rest(block, _):
        columns(block, (cross, far))
        return 0

    def settle(slot):
        remote(vec.at[slot], recv.at[slot], osem.at[slot], orsem.at[slot], (band, slot)).wait()
        emit(recv, slot).start()

    emit(vec, me).start()
    spread_out(vec, me, 0)
    settle(sib)
    spread_out(recv, sib, 1)
    lax.fori_loop(0, nband, early, 0)
    lax.fori_loop(0, nband, late, 0)
    settle(cross)
    spread_out(recv, cross, 0)
    settle(far)
    spread_out(recv, far, 1)
    lax.fori_loop(0, nband, rest, 0)

    lanes = jnp.sum(rows_buf[...], axis=2).reshape(groups * nband, width)
    left_over = lanes
    terms = jnp.zeros((groups * nband, 128), jnp.float32)
    for _ in range(3):
        hi = left_over.astype(jnp.bfloat16)
        terms += mm(hi, t_ref[pl.ds(srow, width), pl.ds(128, 128)])
        left_over = left_over - hi.astype(jnp.float32)
    terms = (terms / ncell).reshape(groups, nband, terms.shape[-1])
    each = nband // groups
    for slot in range(groups):
        total = jnp.zeros((groups, terms.shape[-1]), jnp.float32)
        for n in range(each):
            value = terms[:, slot * each + n]
            total += pltpu.roll(value, bands * n, 1) if n else value
        mine[slot] = total

    def give(slot):
        return remote(mine.at[slot], marg.at[me], msem.at[slot], mrsem.at[me], (band, slot))

    for slot in (cross, far, sib):
        give(slot).start()
    for slot in range(groups):
        emit(recv, slot).wait()
    wrap_copies("end")
    for c in range(2):
        own_copies(c, "end")

    def finish(i, _):
        blk, c = 1 + i // 2, i % 2
        for lane, target in ((0, sib), (1, cross)):
            share(blk, lane, me, own_ref, target, c).wait_send()
        return 0

    def finish_relay(i, _):
        share(i // 2, 2, me, own_ref, sib, i % 2).wait_send()
        return 0

    def finish_line(i, _):
        line(1 + i // 2, i % 2, True, "end")
        line(1 + i // 2, i % 2, False, "end")
        return 0

    lax.fori_loop(0, 4, finish, 0)
    lax.fori_loop(0, 6, finish_relay, 0)
    lax.fori_loop(0, 2 * (length - 1), finish_line, 0)
    total = mine[me]
    for slot in (sib, cross, far):
        remote(mine.at[slot], marg.at[slot], msem.at[slot], mrsem.at[slot], (band, slot)).wait()
        total += marg[slot]
    m_ref[...] = total[:, :nband]


def lane_tables(ng, bands):
    w = bands * ng
    half, bz = [], []
    for lo, hi in ((0, 128), (128, w)):
        for h in range(2):
            half.append(np.full(hi - lo, h))
            bz.append(np.arange(lo, hi))
    half, bz = np.concatenate(half), np.concatenate(bz)
    return half, bz // ng, bz % ng


def tiles(table, half):
    out = []
    for h in range(2):
        pick = np.concatenate([np.arange(128 * h, 128 * h + 128), np.arange(256, len(half))])
        live = half[pick] == h
        out.append(np.where(live[:, None] & live[None, :], table[pick][:, pick], 0.0))
    return np.stack(out)


def solve(nat, ng, groups, nband):
    bands = nat.shape[1]
    width = 2 * bands * ng
    flat = nat.shape[0] * nat.shape[2] // (2 * ng)
    half, bnd, zed = lane_tables(ng, bands)
    ht = hartley(ng)
    th, tl = split_const(ht)
    same = (half[:, None] == half[None, :])
    zmat = np.where(same & (bnd[:, None] == bnd[None, :]), ht[zed[:, None], zed[None, :]], 0.0)
    zt = np.stack(split_const(tiles(zmat, half)), axis=1)
    ty = np.concatenate([th, th, tl], axis=1)
    cp = tiles(np.where(same & (zed[:, None] == zed[None, :]), bnd[:, None] + 1.0, 0.0), half)
    s = np.zeros((width, 128), np.float32)
    s[np.arange(width), half * ng + zed] = 1.0
    hot = np.zeros((width, 128), np.float32)
    hot[np.arange(width), bnd] = 1.0
    kv = kernel_values(ng).astype(np.float32) / np.float32(ng**3)
    kb = np.tile(kv, (1, 1, bands))
    k1 = kb[:, :, :128]
    rest = kb[:, :, 128:].reshape(kb.shape[0], ng // 16, 2, 8, 64)
    k2 = np.concatenate([rest[:, :, 0], rest[:, :, 1]], axis=-1).reshape(kb.shape[0], ng // 2, 128)
    b16 = jnp.bfloat16
    tyw = np.zeros((ng, 256), b16)
    tyw[:, : 3 * ng] = ty
    tab = [zt.reshape(-1, 256), cp.astype(b16).reshape(-1, 256), np.concatenate([s, hot], axis=1).astype(b16), tyw]
    consts = [np.concatenate([k1, k2], axis=1), np.concatenate(tab, axis=0)]
    full = (groups, flat, width)
    slim = (groups, nat.shape[0], nat.shape[2])
    f32, dma = jnp.float32, pltpu.SemaphoreType.DMA
    return pl.pallas_call(
        functools.partial(solve_kernel, ng, ng**3),
        out_shape=(
            jax.ShapeDtypeStruct(nat.shape, f32), jax.ShapeDtypeStruct((groups, nband), f32)
        ),
        in_specs=[pl.BlockSpec(memory_space=pl.ANY)] * (1 + len(consts)),
        out_specs=(pl.BlockSpec(memory_space=pl.ANY), pl.BlockSpec(memory_space=pltpu.VMEM)),
        scratch_shapes=[
            pltpu.VMEM((2, 2, bands, slim[1] // 4, 128), f32), *[pltpu.VMEM(c.shape, c.dtype) for c in consts],
            pltpu.VMEM(full[1:], f32), pltpu.VMEM((nband + 3 * groups,) + full[1:], f32),
            pltpu.VMEM(full, f32), pltpu.VMEM(full, f32), pltpu.VMEM((groups, flat // ng, ng, width), f32),
            pltpu.VMEM(slim, f32), pltpu.VMEM(slim, f32),
            pltpu.VMEM((2, 256, 256), b16), pltpu.VMEM((groups, nband, 8, width), f32),
            pltpu.VMEM((groups, groups, 128), f32), pltpu.VMEM((groups, groups, 128), f32),
            dma((3, groups, 2)), dma((3, 3, 2)), dma((nband, 2)), dma((nband, 2)), dma((nband, 2)), dma((nband, 2)),
            dma((nband, 2)),
            dma((groups,)), dma((groups,)), dma((groups,)), dma((groups,)), dma(()), dma((len(consts),)), dma((groups,)), dma((2, 2, bands)),
            pltpu.VMEM((flat, 128), f32), pltpu.VMEM((2, 3, flat, 128), f32),
        ],
        compiler_params=pltpu.CompilerParams(
            vmem_limit_bytes=55_800_000, collective_id=0, has_side_effects=True
        ),
        cost_estimate=pl.CostEstimate(flops=10**11, bytes_accessed=10**7, transcendentals=0),
        name="solve",
    )(nat, *[jnp.asarray(c) for c in consts])


def on_device(orbitals):
    groups, nband = lax.axis_size("grid"), lax.axis_size("band")
    bands, local = orbitals.shape
    ncell = local * groups
    ng = round(ncell ** (1 / 3))
    nat = orbitals.reshape(bands, local // 128, 128).transpose(1, 0, 2)
    out, marg = solve(nat, ng, groups, nband)
    vectors = out.transpose(1, 0, 2).reshape(bands, local)
    margin = marg.T
    return (vectors, margin)


def solution(mesh):
    return jax.shard_map(
        on_device,
        mesh=mesh,
        in_specs=(P("band", "grid"),),
        out_specs=(P("band", "grid"), P("grid", "band")),
        check_vma=False,
    )
```

```python
import functools

import jax
import jax.numpy as jnp
import numpy as np
from jax import lax
from jax.experimental import pallas as pl
from jax.experimental.pallas import tpu as pltpu
from jax.sharding import PartitionSpec as P


def kernel_values(ng):
    freqs = ((np.arange(ng) + ng // 2) % ng - ng // 2).astype(np.float32)
    sq = freqs[: ng // 2 + 1, None, None] ** 2 + freqs[None, :, None] ** 2 + freqs[None, None, :] ** 2
    safe = np.where(sq > 0, sq, np.float32(1.0))
    return np.where(sq > 0, 40.0 * (1.0 - np.exp(-sq / 16.0)) / safe, 0.0)


def hartley(ng):
    k = np.arange(ng)
    ang = (k[:, None] * k[None, :] % ng) * (2.0 * np.pi / ng)
    return np.cos(ang) + np.sin(ang)


def split_const(table):
    table = np.asarray(table, np.float32)
    hi = table.astype(jnp.bfloat16)
    lo = (table - hi.astype(np.float32)).astype(jnp.bfloat16)
    return hi, lo


def rfft(xs):
    n = len(xs)
    if n == 3:
        s = xs[1] + xs[2]
        d = xs[1] - xs[2]
        return [(xs[0] + s, None), (xs[0] - 0.5 * s, d * (-np.sqrt(3.0) / 2))]
    even, odd = rfft(xs[0::2]), rfft(xs[1::2])
    half = n // 2
    out = [None] * (half + 1)
    for k in range(half // 2 + 1):
        er, ei = even[k]
        orr, oi = odd[k]
        if k == 0:
            out[0] = (er + orr, None)
            out[half] = (er - orr, None)
            continue
        c, s = np.cos(2 * np.pi * k / n), -np.sin(2 * np.pi * k / n)
        if 2 * k == half:
            out[k] = (er, -orr)
            continue
        tr, ti = cmul(orr, oi, c, s)
        out[k] = (er + tr, addo(ei, ti))
        out[half - k] = (er - tr, subo(ti, ei))
    return out


def addo(a, b):
    return b if a is None else a + b


def subo(a, b):
    return a if b is None else a - b


def cmul(r, i, c, s):
    if i is None:
        return r * c, r * s
    if abs(abs(c) - abs(s)) < 1e-9:
        if s < 0 < c:
            return (r + i) * c, (i - r) * c
        return (r - i) * c, (r + i) * c
    return r * c - i * s, r * s + i * c


def irfft(spec, n):
    if n == 3:
        dc, (r, i) = spec[0][0], spec[1]
        base = dc - r
        t = i * np.sqrt(3.0)
        return [dc + 2.0 * r, base - t, base + t]
    half = n // 2
    even, odd = [None] * (half // 2 + 1), [None] * (half // 2 + 1)
    for k in range(half // 2 + 1):
        yr, yi = spec[k]
        if k == 0:
            hr = spec[half][0]
            even[0] = (yr + hr, None)
            odd[0] = (yr - hr, None)
            continue
        if 2 * k == half:
            even[k] = (yr + yr, None)
            odd[k] = (-(yi + yi), None)
            continue
        zr, zi = spec[half - k]
        er, ei = yr + zr, yi - zi
        dr, di = yr - zr, yi + zi
        c, s = np.cos(2 * np.pi * k / n), np.sin(2 * np.pi * k / n)
        even[k] = (er, ei)
        odd[k] = cmul(dr, di, c, s)
    ev, od = irfft(even, half), irfft(odd, half)
    out = [None] * n
    out[0::2], out[1::2] = ev, od
    return out


def split(v):
    hi = v.astype(jnp.bfloat16)
    lo = (v - hi.astype(jnp.float32)).astype(jnp.bfloat16)
    return hi, lo


def mm(a, b):
    return jnp.dot(a, b, preferred_element_type=jnp.float32)


def in_copies(in_ref, nat_ref, sems, c):
    size = nat_ref.shape[3]
    return [
        pltpu.make_async_copy(in_ref.at[pl.ds((2 * h + c) * size, size), b], nat_ref.at[c, h, b], sems.at[c])
        for h in range(2)
        for b in range(in_ref.shape[1])
    ]


def solve_kernel(ng, ncell, in_ref, *refs):
    (k_hbm, t_hbm, o_ref, m_ref, nat_ref, k_ref, t_ref, own_ref, store, amp, acc, work, vec, recv, sel, rows_buf, mine, marg,
     rsem, ssem, gsem, ysem, zsem, dsem, wsem, osem, orsem, msem, mrsem, lsem, csem, esem, isem, tmp, ebuf) = refs
    for copy in in_copies(in_ref, nat_ref, isem, 0) + in_copies(in_ref, nat_ref, isem, 1):
        copy.start()
    load_t = pltpu.make_async_copy(t_hbm, t_ref, csem.at[0])
    load_k = pltpu.make_async_copy(k_hbm, k_ref, csem.at[1])
    load_t.start()
    load_k.start()
    bands = in_ref.shape[1]
    flat, width = own_ref.shape
    planes = flat // ng
    groups = vec.shape[0]
    me = lax.axis_index("grid")
    band, nband = lax.axis_index("band"), lax.axis_size("band")
    chip, core = me // 2, me % 2
    sib = chip * 2 + (1 - core)
    cross = (1 - chip) * 2 + core
    far = (1 - chip) * 2 + (1 - core)
    length = nband // 2
    side, pos = band % 2, band // 2
    pair = band + 1 - 2 * side
    third = (band + nband - 1 + 2 * side) % nband
    first, last = band == 0, band == nband - 1
    ends = jnp.logical_or(first, last)
    wrap = jnp.where(first, nband - 1, 0)
    has_up, has_down = pos < length - 1, pos > 0
    up, down = jnp.where(has_up, band + 2, band), jnp.where(has_down, band - 2, band)
    mesh_id = pl.DeviceIdType.MESH
    part = planes // 2
    zrow, crow = 256, 1024
    srow = crow + 512
    yrow = srow + width

    def remote(src, dst, send, recv_sem, device):
        return pltpu.make_async_remote_copy(
            src_ref=src, dst_ref=dst, send_sem=send, recv_sem=recv_sem,
            device_id=device, device_id_type=mesh_id,
        )

    def partner(blk):
        return jnp.where(blk == 0, band, jnp.where(blk == 1, pair, third))

    def place(blk, slot):
        return jnp.where(slot == me, partner(blk), nband + blk * groups + slot)

    def piece(ref, c):
        return ref.at[pl.ds(c * part * ng, part * ng)]

    def skip(slot, at):
        return slot - (slot > at).astype(jnp.int32)

    def share(blk, lane, slot, src, target, c):
        dst = store.at[nband + blk * groups + slot]
        return remote(piece(src, c), piece(dst, c), ssem.at[lane], rsem.at[blk, skip(slot, target), c], (band, target))

    def along(block, sem, device, c, src=None):
        dst = store.at[block]
        src = dst if src is None else src
        return remote(piece(src, c), piece(dst, c), sem, gsem.at[block, c], (device, me))

    def came(block, c):
        along(block, wsem, pair, c).wait_recv()

    lane = lax.broadcasted_iota(jnp.int32, (1, 128), 1)

    def moved(value, shift, low, high, under):
        out = pltpu.roll(value, shift % 128, 1) if shift % 128 else value
        return jnp.where(jnp.logical_and(lane >= low, lane < high), out, under)

    def gather_in(read, want, blank):
        for y0 in range(8):
            chunks = [None, None, None]
            for h in range(2):
                for b in range(bands):
                    for target, start, stop, base in ((h, 0, 128, 0), (2, 128, bands * ng, 64 * h)):
                        first, final = max(start, b * ng), min(stop, b * ng + ng)
                        if first >= final:
                            continue
                        source = y0 * ng + first - b * ng
                        place_at = first - start + base
                        while first < final:
                            q, off = source // 128, source % 128
                            size = min(final - first, 128 - off)
                            under = chunks[target]
                            under = blank if under is None else under
                            chunks[target] = moved(read(b, h, q), place_at - off, place_at, place_at + size, under)
                            first, source, place_at = first + size, source + size, place_at + size
            for j, value in enumerate(chunks):
                want(j, y0, value)

    def scatter_out(read, write, blank):
        for h in range(2):
            chunks = [blank] * 3
            for y0 in range(8):
                value = read(y0)
                source, at, left = h * ng, y0 * ng, ng
                while left > 0:
                    q, off = at // 128, at % 128
                    size = min(left, 128 - off)
                    chunks[q] = moved(value, off - source, off, off + size, chunks[q])
                    source, at, left = source + size, at + size, left - size
            for q in range(3):
                write(h, q, chunks[q])

    group = flat // 8

    def packed(h, q):
        return pl.ds(q + 3 * group * h, group, stride=3)

    def spaced(y0):
        return pl.ds(y0, group, stride=8)

    def greet(device):
        pl.semaphore_signal(barrier, inc=1, device_id=device, device_id_type=mesh_id)

    barrier = pltpu.get_barrier_semaphore()
    for device in ((band, sib), (band, cross), (band, far), (pair, me)):
        greet(device)

    @pl.when(has_up)
    def _():
        greet((up, me))

    @pl.when(has_down)
    def _():
        greet((down, me))

    @pl.when(ends)
    def _():
        greet((wrap, me))

    count = 4 + has_up.astype(jnp.int32) + has_down.astype(jnp.int32) + ends.astype(jnp.int32)
    def own_copies(c):
        share(0, 1, me, own_ref, cross, c).start()
        share(0, 0, me, own_ref, sib, c).start()
        along(band, ysem.at[pos, c], pair, c, own_ref).start()

        @pl.when(has_up)
        def _():
            along(band, zsem.at[pos, c], up, c, own_ref).start()

        @pl.when(has_down)
        def _():
            along(band, dsem, down, c, own_ref).start()

    few = group // 2
    for c in range(2):
        pltpu.make_async_copy(nat_ref.at[c], nat_ref.at[c], isem.at[c]).wait()

        def put_own(j, y0, value):
            ebuf[0, j, pl.ds(c * part * ng + y0, few, stride=8), :] = value

        gather_in(
            lambda b, h, q: nat_ref[c, h, b, pl.ds(q, few, stride=3), :], put_own, jnp.zeros((few, 128), jnp.float32)
        )
        half_rows = pl.ds(c * part * ng, part * ng)
        own_ref[half_rows, :] = jnp.concatenate([ebuf[0, j, half_rows, :] for j in range(3)], axis=1)
        if c == 0:
            pl.semaphore_wait(barrier, count)
        own_copies(c)

    @pl.when(ends)
    def _():
        for c in range(2):
            along(band, wsem, wrap, c, own_ref).start()

    local = pltpu.make_async_copy(own_ref, store.at[band], lsem)
    local.start()

    def arrived(blk, slot, c):
        dst = piece(store.at[nband + blk * groups + slot], c)
        remote(dst, dst, ssem.at[0], rsem.at[blk, skip(slot, me), c], (band, sib)).wait_recv()

    def relay(blk, c):
        arrived(blk, cross, c)
        share(blk, 2, cross, store.at[nband + blk * groups + cross], sib, c).start()

    def spread(blk, c):
        came(partner(blk), c)
        share(blk, 1, me, store.at[partner(blk)], cross, c).start()
        share(blk, 0, me, store.at[partner(blk)], sib, c).start()

    def skipped(block):
        return jnp.logical_or(
            jnp.logical_and(pair == 0, block == nband - 1), jnp.logical_and(pair == nband - 1, block == 0)
        )

    def line(d, c, near, act):
        def pass_on(block, exists, on, device):
            @pl.when(exists)
            def _():
                if act == "go":
                    came(block, c)

                def one(copy):
                    copy.start() if act == "go" else copy.wait_send()

                @pl.when(jnp.logical_not(skipped(block)))
                def _():
                    one(along(block, ysem.at[block // 2, c], pair, c))

                @pl.when(on)
                def _():
                    one(along(block, zsem.at[block // 2, c], device, c))

        upward = (side == 1) == near
        pass_on(band - 2 * d, jnp.logical_and(upward, pos - d >= 0), has_up, up)
        pass_on(
            band + 2 * d, jnp.logical_and(jnp.logical_not(upward), pos + d <= length - 1), has_down, down
        )

    def serve(blk, c):
        @pl.when(blk < 2)
        def _():
            spread(blk + 1, c)

        line(blk + 1, c, True, "go")

    def ztrans(v):
        hi, lo = split(v)
        parts = []
        for h in range(2):
            a, b = (jnp.concatenate([t[:, 128 * h:128 * h + 128], t[:, 256:]], axis=1) for t in (hi, lo))
            high, low = (t_ref[pl.ds((2 * h + n) * zrow, zrow), :] for n in range(2))
            parts.append(mm(a, high) + mm(b, high) + mm(a, low))
        return jnp.concatenate([parts[0][:, :128], parts[1][:, :128], parts[0][:, 128:] + parts[1][:, 128:]], axis=1)

    def ytrans(v):
        hi, lo = split(v)
        return mm(t_ref[pl.ds(yrow, ng), pl.ds(0, 3 * ng)], jnp.concatenate([hi, lo, hi], axis=0))

    def amplitude(v):
        hi, lo = split(v)
        parts = []
        for h in range(2):
            a, b = (jnp.concatenate([t[:, 128 * h:128 * h + 128], t[:, 256:]], axis=1) for t in (hi, lo))
            parts.append(mm(a, sel[h]) + mm(b, sel[h]))
        return jnp.concatenate([parts[0][:, :128], parts[1][:, :128], parts[0][:, 128:] + parts[1][:, 128:]], axis=1)

    load_t.wait()
    for h in range(2):
        mark = (me + 1).astype(jnp.float32)
        sel[h] = jnp.where(t_ref[pl.ds(crow + zrow * h, zrow), :].astype(jnp.float32) == mark, 1.0, 0.0).astype(jnp.bfloat16)

    def transform(blk, slots, c):
        rows = pl.ds(c * part * ng, part * ng)

        @pl.when(blk == 0)
        def _():
            own = jnp.concatenate([store[place(0, slot), rows] for slot in slots], axis=0)
            out = amplitude(own).reshape(len(slots), part * ng, width)
            for n, slot in enumerate(slots):
                amp[slot, rows] = out[n]

        p = jnp.concatenate([amp[slot, rows] * store[place(blk, slot), rows] for slot in slots], axis=0)
        q = ztrans(p).reshape(len(slots), part, ng, width)
        for n, slot in enumerate(slots):
            for r in range(part):
                work[slot, c * part + r] = ytrans(q[n, r])

    def near(blk, c):
        arrived(blk, sib, c)

        @pl.when(jnp.logical_and(blk > 0, c == 1))
        def _():
            relay(blk, 0)

        transform(blk, (me, sib), c)

    def other(blk, i):
        c = i // 2

        @pl.when(jnp.logical_and(blk == 0, i == 0))
        def _():
            serve(blk, 0)
            relay(blk, 0)

        @pl.when(i == 1)
        def _():
            serve(blk, 1)
            relay(blk, 1)

        @pl.when(i % 2 == 1)
        def _():
            arrived(blk, far, c)

        @pl.when(jnp.logical_and(blk > 0, i == 2))
        def _():
            line(blk, 1, False, "go")

        transform(blk, (jnp.where(i % 2 == 0, cross, far),), c)

    def conv(vals, kern):
        spec = rfft(vals)
        out = []
        for k, (re, im) in enumerate(spec):
            kv = kern(k)
            out.append((re * kv, None if im is None else im * kv))
        return irfft(out, ng)

    def xconv(t):
        order = [(g, h, r) for g in range(4) for h in range(2) for r in range(planes)]
        for i in range(2):
            rows = pl.ds(pl.multiple_of(t * 16 + 8 * i, 8), 8)
            res = conv([work[g, r, rows, h * 128:h * 128 + 128] for g, h, r in order],
                       lambda k: k_ref[k, rows, :])
            for (g, h, r), v in zip(order, res):
                work[g, r, rows, h * 128:h * 128 + 128] = v
        ra = pl.ds(pl.multiple_of(t * 16, 8), 8)
        rb = pl.ds(pl.multiple_of(t * 16 + 8, 8), 8)
        left = lax.broadcasted_iota(jnp.int32, (8, 128), 1) < 64

        def half(g, h, r):
            u, w = work[g, r, ra, 256:384], work[g, r, rb, 256:384]
            if h == 0:
                return jnp.where(left, u, pltpu.roll(w, 64, 1))
            return jnp.where(left, pltpu.roll(u, 64, 1), w)

        rk = pl.ds(pl.multiple_of(ng + t * 8, 8), 8)
        res = dict(zip(order, conv([half(*o) for o in order], lambda k: k_ref[k, rk, :])))
        for g in range(4):
            for r in range(planes):
                a, b = res[(g, 0, r)], res[(g, 1, r)]
                work[g, r, ra, 256:384] = jnp.where(left, a, pltpu.roll(b, 64, 1))
                work[g, r, rb, 256:384] = jnp.where(left, pltpu.roll(a, 64, 1), b)

    def push(slot):
        return remote(vec.at[slot], recv.at[me], osem, orsem.at[me], (band, slot))

    def inverse(blk, s):
        slot = ((chip + 1 - s // 2) % 2) * 2 + (core + s % 2 + s // 2) % 2
        q = jnp.concatenate([ytrans(work[slot, r]) for r in range(planes)], axis=0)
        w = ztrans(q) * store[place(blk, slot)]

        @pl.when(jnp.logical_and(blk < 2, s == 2))
        def _():
            serve(blk + 1, 0)
            line(blk + 1, 0, False, "go")

        @pl.when(blk == 0)
        def _():
            acc[slot] = w

        @pl.when(blk == 1)
        def _():
            acc[slot] += w

        @pl.when(blk == 2)
        def _():
            hi, lo = split(acc[slot] + w)
            s_tab = t_ref[pl.ds(srow, width), pl.ds(0, 128)]
            tmp[...] = -(mm(hi, s_tab) + mm(lo, s_tab))

            def put_vec(h, q, value):
                vec[slot, packed(h, q), :] = value

            scatter_out(lambda y0: tmp[spaced(y0), :], put_vec, jnp.zeros((group, 128), jnp.float32))

            @pl.when(s < 3)
            def _():
                push(slot).start()

    def block(blk, _):
        @pl.when(blk == 0)
        def _():
            local.wait()

        def fwd_near(c, _):
            near(blk, c)
            return 0

        def fwd_other(i, _):
            other(blk, i)
            return 0

        def mid(t, _):
            xconv(t)
            return 0

        def inv(s, _):
            inverse(blk, s)
            return 0

        lax.fori_loop(0, 2, fwd_near, 0)
        lax.fori_loop(0, 4, fwd_other, 0)

        @pl.when(blk == 0)
        def _():
            load_k.wait()

        lax.fori_loop(0, ng // 16, mid, 0)
        lax.fori_loop(0, 4, inv, 0)
        return 0

    lax.fori_loop(0, 3, block, 0)

    def later(d, _):
        for c in range(2):
            line(d, c, False, "go")
            line(d + 1, c, True, "go")
        return 0

    lax.fori_loop(3, length, later, 0)

    def emit(src, slot):
        return pltpu.make_async_copy(src.at[slot], o_ref.at[:, slot], esem)

    def spread_out(src, slot, n):
        def put(j, y0, value):
            ebuf[n, j, spaced(y0), :] = value

        values = {(h, q): src[slot, packed(h, q), :] for h in range(2) for q in range(3)}
        gather_in(lambda b, h, q: values[h, q], put, jnp.zeros((group, 128), jnp.float32))

    order = (me, sib, cross, far)

    def columns(block, slots):
        where = [next(n for n, s in enumerate(order) if s is slot) for slot in slots]
        parts = [[jnp.zeros((8, 128), jnp.float32) for _ in range(3)] for _ in slots]
        for r in range(flat // 8):
            for j in range(3):
                phi = store[block, pl.ds(8 * r, 8), pl.ds(128 * j, 128)]
                for n, p in zip(where, parts):
                    p[j] = p[j] + phi * ebuf[n, j, pl.ds(8 * r, 8)]
        for slot, p in zip(slots, parts):
            rows_buf[slot, block] = jnp.concatenate(p, axis=1)

    def ready(block):
        near_by = jnp.logical_or(block == pair, block == third)
        return jnp.logical_or(near_by, block % 2 == side)

    def early(slots):
        def body(block, _):
            @pl.when(ready(block))
            def _():
                columns(block, slots)

            return 0

        return body

    def late(block, _):
        @pl.when(jnp.logical_not(ready(block)))
        def _():
            for c in range(2):
                came(block, c)
            columns(block, (me, sib, cross))

        return 0

    def settle(slot):
        remote(vec.at[slot], recv.at[slot], osem, orsem.at[slot], (band, slot)).wait_recv()
        emit(recv, slot).start()

    emit(vec, me).start()
    spread_out(vec, me, 0)
    settle(sib)
    spread_out(recv, sib, 1)
    lax.fori_loop(0, nband, early((me, sib)), 0)
    settle(cross)
    spread_out(recv, cross, 2)
    lax.fori_loop(0, nband, early((cross,)), 0)
    lax.fori_loop(0, nband, late, 0)
    settle(far)
    spread_out(recv, far, 3)

    def last(block, _):
        columns(block, (far,))
        return 0

    lax.fori_loop(0, nband, last, 0)
    lanes = jnp.sum(rows_buf[...], axis=2).reshape(groups * nband, width)
    left_over = lanes
    terms = jnp.zeros((groups * nband, 128), jnp.float32)
    for _ in range(3):
        hi = left_over.astype(jnp.bfloat16)
        terms += mm(hi, t_ref[pl.ds(srow, width), pl.ds(128, 128)])
        left_over = left_over - hi.astype(jnp.float32)
    terms = (terms / ncell).reshape(groups, nband, terms.shape[-1])
    each = nband // groups
    for slot in range(groups):
        total = jnp.zeros((groups, terms.shape[-1]), jnp.float32)
        for n in range(each):
            value = terms[:, slot * each + n]
            total += pltpu.roll(value, bands * n, 1) if n else value
        mine[slot] = total

    def give(slot):
        return remote(mine.at[slot], marg.at[me], msem, mrsem.at[me], (band, slot))

    for slot in (cross, far, sib):
        give(slot).start()
    pltpu.make_async_copy(o_ref, o_ref, esem).wait()
    others = pl.ds(0, groups - 1)
    remote(vec.at[others], recv.at[others], osem, orsem.at[me], (band, sib)).wait_send()
    remote(mine.at[others], marg.at[others], msem, mrsem.at[me], (band, sib)).wait_send()
    three = store.at[pl.ds(0, 3)]
    for n in range(3):
        remote(three, three, ssem.at[n], gsem.at[0, 0], (band, sib)).wait_send()
    whole = store.at[band]

    @pl.when(ends)
    def _():
        remote(whole, whole, wsem, gsem.at[0, 0], (wrap, me)).wait_send()

    @pl.when(has_down)
    def _():
        remote(whole, whole, dsem, gsem.at[0, 0], (down, me)).wait_send()

    for c in range(2):
        along(band, ysem.at[pos, c], pair, c).wait_send()

        @pl.when(has_up)
        def _():
            along(band, zsem.at[pos, c], up, c).wait_send()

    def finish_line(i, _):
        line(1 + i // 2, i % 2, True, "end")
        line(1 + i // 2, i % 2, False, "end")
        return 0

    lax.fori_loop(0, 2 * (length - 1), finish_line, 0)
    total = mine[me]
    for slot in (sib, cross, far):
        remote(mine.at[slot], marg.at[slot], msem, mrsem.at[slot], (band, slot)).wait_recv()
        total += marg[slot]
    m_ref[...] = total[:, :nband]


def lane_tables(ng, bands):
    w = bands * ng
    half, bz = [], []
    for lo, hi in ((0, 128), (128, w)):
        for h in range(2):
            half.append(np.full(hi - lo, h))
            bz.append(np.arange(lo, hi))
    half, bz = np.concatenate(half), np.concatenate(bz)
    return half, bz // ng, bz % ng


def tiles(table, half):
    out = []
    for h in range(2):
        pick = np.concatenate([np.arange(128 * h, 128 * h + 128), np.arange(256, len(half))])
        live = half[pick] == h
        out.append(np.where(live[:, None] & live[None, :], table[pick][:, pick], 0.0))
    return np.stack(out)


def solve(nat, ng, groups, nband):
    bands = nat.shape[1]
    width = 2 * bands * ng
    flat = nat.shape[0] * nat.shape[2] // (2 * ng)
    half, bnd, zed = lane_tables(ng, bands)
    ht = hartley(ng)
    th, tl = split_const(ht)
    same = (half[:, None] == half[None, :])
    zmat = np.where(same & (bnd[:, None] == bnd[None, :]), ht[zed[:, None], zed[None, :]], 0.0)
    zt = np.stack(split_const(tiles(zmat, half)), axis=1)
    ty = np.concatenate([th, th, tl], axis=1)
    cp = tiles(np.where(same & (zed[:, None] == zed[None, :]), bnd[:, None] + 1.0, 0.0), half)
    s = np.zeros((width, 128), np.float32)
    s[np.arange(width), half * ng + zed] = 1.0
    hot = np.zeros((width, 128), np.float32)
    hot[np.arange(width), bnd] = 1.0
    kv = kernel_values(ng).astype(np.float32) / np.float32(ng**3)
    kb = np.tile(kv, (1, 1, bands))
    k1 = kb[:, :, :128]
    rest = kb[:, :, 128:].reshape(kb.shape[0], ng // 16, 2, 8, 64)
    k2 = np.concatenate([rest[:, :, 0], rest[:, :, 1]], axis=-1).reshape(kb.shape[0], ng // 2, 128)
    b16 = jnp.bfloat16
    tyw = np.zeros((ng, 256), b16)
    tyw[:, : 3 * ng] = ty
    tab = [zt.reshape(-1, 256), cp.astype(b16).reshape(-1, 256), np.concatenate([s, hot], axis=1).astype(b16), tyw]
    consts = [np.concatenate([k1, k2], axis=1), np.concatenate(tab, axis=0)]
    full = (groups, flat, width)
    slim = (groups, nat.shape[0], nat.shape[2])
    f32, dma = jnp.float32, pltpu.SemaphoreType.DMA
    return pl.pallas_call(
        functools.partial(solve_kernel, ng, ng**3),
        out_shape=(
            jax.ShapeDtypeStruct(nat.shape, f32), jax.ShapeDtypeStruct((groups, nband), f32)
        ),
        in_specs=[pl.BlockSpec(memory_space=pl.ANY)] * (1 + len(consts)),
        out_specs=(pl.BlockSpec(memory_space=pl.ANY), pl.BlockSpec(memory_space=pltpu.VMEM)),
        scratch_shapes=[
            pltpu.VMEM((2, 2, bands, slim[1] // 4, 128), f32), *[pltpu.VMEM(c.shape, c.dtype) for c in consts],
            pltpu.VMEM(full[1:], f32), pltpu.VMEM((nband + 3 * groups,) + full[1:], f32),
            pltpu.VMEM(full, f32), pltpu.VMEM(full, f32), pltpu.VMEM((groups, flat // ng, ng, width), f32),
            pltpu.VMEM(slim, f32), pltpu.VMEM(slim, f32),
            pltpu.VMEM((2, 256, 256), b16), pltpu.VMEM((groups, nband, 8, width), f32),
            pltpu.VMEM((groups, groups, 128), f32), pltpu.VMEM((groups, groups, 128), f32),
            dma((3, groups - 1, 2)), dma((3,)), dma((nband, 2)), dma((nband // 2, 2)), dma((nband // 2, 2)), dma(()), dma(()),
            dma(()), dma((groups,)), dma(()), dma((groups,)), dma(()), dma((2,)), dma(()), dma((2,)),
            pltpu.VMEM((flat, 128), f32), pltpu.VMEM((groups, 3, flat, 128), f32),
        ],
        compiler_params=pltpu.CompilerParams(
            vmem_limit_bytes=55_800_000, collective_id=0, has_side_effects=True
        ),
        cost_estimate=pl.CostEstimate(flops=10**11, bytes_accessed=10**7, transcendentals=0),
        name="solve",
    )(nat, *[jnp.asarray(c) for c in consts])


def on_device(orbitals):
    groups, nband = lax.axis_size("grid"), lax.axis_size("band")
    bands, local = orbitals.shape
    ncell = local * groups
    ng = round(ncell ** (1 / 3))
    nat = orbitals.reshape(bands, local // 128, 128).transpose(1, 0, 2)
    out, marg = solve(nat, ng, groups, nband)
    vectors = out.transpose(1, 0, 2).reshape(bands, local)
    margin = marg.T
    return (vectors, margin)


def solution(mesh):
    return jax.shard_map(
        on_device,
        mesh=mesh,
        in_specs=(P("band", "grid"),),
        out_specs=(P("band", "grid"), P("grid", "band")),
        check_vma=False,
    )
```

```python
import functools

import jax
import jax.numpy as jnp
import numpy as np
from jax import lax
from jax.experimental import pallas as pl
from jax.experimental.pallas import tpu as pltpu
from jax.sharding import PartitionSpec as P


def kernel_values(ng):
    freqs = ((np.arange(ng) + ng // 2) % ng - ng // 2).astype(np.float32)
    sq = freqs[: ng // 2 + 1, None, None] ** 2 + freqs[None, :, None] ** 2 + freqs[None, None, :] ** 2
    safe = np.where(sq > 0, sq, np.float32(1.0))
    return np.where(sq > 0, 40.0 * (1.0 - np.exp(-sq / 16.0)) / safe, 0.0)


def hartley(ng):
    k = np.arange(ng)
    ang = (k[:, None] * k[None, :] % ng) * (2.0 * np.pi / ng)
    return np.cos(ang) + np.sin(ang)


def split_const(table):
    table = np.asarray(table, np.float32)
    hi = table.astype(jnp.bfloat16)
    lo = (table - hi.astype(np.float32)).astype(jnp.bfloat16)
    return hi, lo


def rfft(xs):
    n = len(xs)
    if n == 1:
        return [(xs[0], None)]
    even, odd = rfft(xs[0::2]), rfft(xs[1::2])
    half = n // 2
    out = [None] * (half + 1)
    for k in range(half // 2 + 1):
        er, ei = even[k]
        orr, oi = odd[k]
        if k == 0:
            out[0] = (er + orr, None)
            out[half] = (er - orr, None)
            continue
        c, s = np.cos(2 * np.pi * k / n), -np.sin(2 * np.pi * k / n)
        if 2 * k == half:
            out[k] = (er, -orr)
            continue
        tr, ti = cmul(orr, oi, c, s)
        out[k] = (er + tr, addo(ei, ti))
        out[half - k] = (er - tr, subo(ti, ei))
    return out


def addo(a, b):
    return b if a is None else a + b


def subo(a, b):
    return a if b is None else a - b


def cmul(r, i, c, s):
    if i is None:
        return r * c, r * s
    if abs(abs(c) - abs(s)) < 1e-9:
        if s < 0 < c:
            return (r + i) * c, (i - r) * c
        return (r - i) * c, (r + i) * c
    return r * c - i * s, r * s + i * c


def irfft(spec, n):
    if n == 1:
        return [spec[0][0]]
    half = n // 2
    even, odd = [None] * (half // 2 + 1), [None] * (half // 2 + 1)
    for k in range(half // 2 + 1):
        yr, yi = spec[k]
        if k == 0:
            hr = spec[half][0]
            even[0] = (yr + hr, None)
            odd[0] = (yr - hr, None)
            continue
        if 2 * k == half:
            even[k] = (yr + yr, None)
            odd[k] = (-(yi + yi), None)
            continue
        zr, zi = spec[half - k]
        er, ei = yr + zr, yi - zi
        dr, di = yr - zr, yi + zi
        c, s = np.cos(2 * np.pi * k / n), np.sin(2 * np.pi * k / n)
        even[k] = (er, ei)
        odd[k] = cmul(dr, di, c, s)
    ev, od = irfft(even, half), irfft(odd, half)
    out = [None] * n
    out[0::2], out[1::2] = ev, od
    return out


def cfft(xs, sign):
    n = len(xs)
    if n == 1:
        return xs
    even, odd = cfft(xs[0::2], sign), cfft(xs[1::2], sign)
    half = n // 2
    out = [None] * n
    for k in range(half):
        (er, ei), (r, i) = even[k], odd[k]
        if 4 * k == n:
            out[k] = (er + i, ei - r) if sign < 0 else (er - i, ei + r)
            out[k + half] = (er - i, ei + r) if sign < 0 else (er + i, ei - r)
            continue
        if k == 0:
            tr, ti = r, i
        else:
            tr, ti = turn(r, i, np.cos(2 * np.pi * k / n), sign * np.sin(2 * np.pi * k / n))
        out[k] = (er + tr, ei + ti)
        out[k + half] = (er - tr, ei - ti)
    return out


def turn(r, i, c, s):
    if abs(abs(c) - abs(s)) > 1e-9:
        return r * c - i * s, r * s + i * c
    if c * s > 0:
        return (r - i) * c, (r + i) * c
    return (r + i) * c, (i - r) * c


def split(v):
    hi = v.astype(jnp.bfloat16)
    lo = (v - hi.astype(jnp.float32)).astype(jnp.bfloat16)
    return hi, lo


def mm(a, b):
    return jnp.dot(a, b, preferred_element_type=jnp.float32)


def in_copies(in_ref, nat_ref, sems, c):
    size = nat_ref.shape[3]
    return [
        pltpu.make_async_copy(in_ref.at[pl.ds((2 * h + c) * size, size), b], nat_ref.at[c, h, b], sems.at[c])
        for h in range(2)
        for b in range(in_ref.shape[1])
    ]


def solve_kernel(ng, ncell, in_ref, *refs):
    (k_hbm, t_hbm, o_ref, m_ref, nat_ref, k_ref, t_ref, own_ref, store, amp, acc, work, vec, recv, sel, rows_buf, mine, marg,
     rsem, ssem, gsem, ysem, zsem, dsem, wsem, osem, orsem, msem, mrsem, lsem, csem, esem, isem, tmp, ebuf) = refs
    for copy in in_copies(in_ref, nat_ref, isem, 0) + in_copies(in_ref, nat_ref, isem, 1):
        copy.start()
    load_t = pltpu.make_async_copy(t_hbm, t_ref, csem.at[0])
    load_k = pltpu.make_async_copy(k_hbm, k_ref, csem.at[1])
    load_t.start()
    load_k.start()
    bands = in_ref.shape[1]
    flat, width = own_ref.shape
    planes = flat // ng
    groups = vec.shape[0]
    me = lax.axis_index("grid")
    band, nband = lax.axis_index("band"), lax.axis_size("band")
    chip, core = me // 2, me % 2
    sib = chip * 2 + (1 - core)
    cross = (1 - chip) * 2 + core
    far = (1 - chip) * 2 + (1 - core)
    length = nband // 2
    side, pos = band % 2, band // 2
    pair = band + 1 - 2 * side
    third = (band + nband - 1 + 2 * side) % nband
    first, last = band == 0, band == nband - 1
    ends = jnp.logical_or(first, last)
    wrap = jnp.where(first, nband - 1, 0)
    has_up, has_down = pos < length - 1, pos > 0
    up, down = jnp.where(has_up, band + 2, band), jnp.where(has_down, band - 2, band)
    mesh_id = pl.DeviceIdType.MESH
    part = planes // 2
    zrow, crow = 256, 1024
    srow = crow + 512
    yrow = srow + width

    def remote(src, dst, send, recv_sem, device):
        return pltpu.make_async_remote_copy(
            src_ref=src, dst_ref=dst, send_sem=send, recv_sem=recv_sem,
            device_id=device, device_id_type=mesh_id,
        )

    def partner(blk):
        return jnp.where(blk == 0, band, jnp.where(blk == 1, pair, third))

    def place(blk, slot):
        return jnp.where(slot == me, partner(blk), nband + blk * groups + slot)

    def piece(ref, c):
        return ref.at[pl.ds(c * part * ng, part * ng)]

    def skip(slot, at):
        return slot - (slot > at).astype(jnp.int32)

    def share(blk, lane, slot, src, target, c):
        dst = store.at[nband + blk * groups + slot]
        return remote(piece(src, c), piece(dst, c), ssem.at[lane], rsem.at[blk, skip(slot, target), c], (band, target))

    def along(block, sem, device, c, src=None):
        dst = store.at[block]
        src = dst if src is None else src
        return remote(piece(src, c), piece(dst, c), sem, gsem.at[block, c], (device, me))

    def came(block, c):
        along(block, wsem, pair, c).wait_recv()

    lane = lax.broadcasted_iota(jnp.int32, (1, 128), 1)

    def moved(value, shift, low, high, under):
        out = pltpu.roll(value, shift % 128, 1) if shift % 128 else value
        return jnp.where(jnp.logical_and(lane >= low, lane < high), out, under)

    def gather_in(read, want, blank):
        for y0 in range(8):
            chunks = [None, None, None]
            for h in range(2):
                for b in range(bands):
                    for target, start, stop, base in ((h, 0, 128, 0), (2, 128, bands * ng, 64 * h)):
                        first, final = max(start, b * ng), min(stop, b * ng + ng)
                        if first >= final:
                            continue
                        source = y0 * ng + first - b * ng
                        place_at = first - start + base
                        while first < final:
                            q, off = source // 128, source % 128
                            size = min(final - first, 128 - off)
                            under = chunks[target]
                            under = blank if under is None else under
                            chunks[target] = moved(read(b, h, q), place_at - off, place_at, place_at + size, under)
                            first, source, place_at = first + size, source + size, place_at + size
            for j, value in enumerate(chunks):
                want(j, y0, value)

    def scatter_out(read, write, blank):
        for h in range(2):
            chunks = [blank] * 3
            for y0 in range(8):
                value = read(y0)
                source, at, left = h * ng, y0 * ng, ng
                while left > 0:
                    q, off = at // 128, at % 128
                    size = min(left, 128 - off)
                    chunks[q] = moved(value, off - source, off, off + size, chunks[q])
                    source, at, left = source + size, at + size, left - size
            for q in range(3):
                write(h, q, chunks[q])

    group = flat // 8

    def packed(h, q):
        return pl.ds(q + 3 * group * h, group, stride=3)

    def spaced(y0):
        return pl.ds(y0, group, stride=8)

    def greet(device):
        pl.semaphore_signal(barrier, inc=1, device_id=device, device_id_type=mesh_id)

    barrier = pltpu.get_barrier_semaphore()
    for device in ((band, sib), (band, cross), (band, far), (pair, me)):
        greet(device)

    @pl.when(has_up)
    def _():
        greet((up, me))

    @pl.when(has_down)
    def _():
        greet((down, me))

    @pl.when(ends)
    def _():
        greet((wrap, me))

    count = 4 + has_up.astype(jnp.int32) + has_down.astype(jnp.int32) + ends.astype(jnp.int32)
    def own_copies(c):
        share(0, 1, me, own_ref, cross, c).start()
        share(0, 0, me, own_ref, sib, c).start()
        along(band, ysem.at[pos, c], pair, c, own_ref).start()

        @pl.when(has_up)
        def _():
            along(band, zsem.at[pos, c], up, c, own_ref).start()

        @pl.when(has_down)
        def _():
            along(band, dsem, down, c, own_ref).start()

    few = group // 2
    for c in range(2):
        pltpu.make_async_copy(nat_ref.at[c], nat_ref.at[c], isem.at[c]).wait()

        def put_own(j, y0, value):
            ebuf[0, j, pl.ds(c * part * ng + y0, few, stride=8), :] = value

        gather_in(
            lambda b, h, q: nat_ref[c, h, b, pl.ds(q, few, stride=3), :], put_own, jnp.zeros((few, 128), jnp.float32)
        )
        half_rows = pl.ds(c * part * ng, part * ng)
        own_ref[half_rows, :] = jnp.concatenate([ebuf[0, j, half_rows, :] for j in range(3)], axis=1)
        if c == 0:
            pl.semaphore_wait(barrier, count)
        own_copies(c)

    @pl.when(ends)
    def _():
        for c in range(2):
            along(band, wsem, wrap, c, own_ref).start()

    local = pltpu.make_async_copy(own_ref, store.at[band], lsem)
    local.start()

    def arrived(blk, slot, c):
        dst = piece(store.at[nband + blk * groups + slot], c)
        remote(dst, dst, ssem.at[0], rsem.at[blk, skip(slot, me), c], (band, sib)).wait_recv()

    def relay(blk, c):
        arrived(blk, cross, c)
        share(blk, 2, cross, store.at[nband + blk * groups + cross], sib, c).start()

    def spread(blk, c):
        came(partner(blk), c)
        share(blk, 1, me, store.at[partner(blk)], cross, c).start()
        share(blk, 0, me, store.at[partner(blk)], sib, c).start()

    def skipped(block):
        return jnp.logical_or(
            jnp.logical_and(pair == 0, block == nband - 1), jnp.logical_and(pair == nband - 1, block == 0)
        )

    def line(d, c, near, act):
        def pass_on(block, exists, on, device):
            @pl.when(exists)
            def _():
                if act == "go":
                    came(block, c)

                def one(copy):
                    copy.start() if act == "go" else copy.wait_send()

                @pl.when(jnp.logical_not(skipped(block)))
                def _():
                    one(along(block, ysem.at[block // 2, c], pair, c))

                @pl.when(on)
                def _():
                    one(along(block, zsem.at[block // 2, c], device, c))

        upward = (side == 1) == near
        pass_on(band - 2 * d, jnp.logical_and(upward, pos - d >= 0), has_up, up)
        pass_on(
            band + 2 * d, jnp.logical_and(jnp.logical_not(upward), pos + d <= length - 1), has_down, down
        )

    def serve(blk, c):
        @pl.when(blk < 2)
        def _():
            spread(blk + 1, c)

        line(blk + 1, c, True, "go")

    def ztrans(v):
        hi, lo = split(v)
        parts = []
        for h in range(2):
            a, b = (jnp.concatenate([t[:, 128 * h:128 * h + 128], t[:, 256:]], axis=1) for t in (hi, lo))
            high, low = (t_ref[pl.ds((2 * h + n) * zrow, zrow), :] for n in range(2))
            parts.append(mm(a, high) + mm(b, high) + mm(a, low))
        return jnp.concatenate([parts[0][:, :128], parts[1][:, :128], parts[0][:, 128:] + parts[1][:, 128:]], axis=1)

    def ytrans(v):
        hi, lo = split(v)
        return mm(t_ref[pl.ds(yrow, ng), pl.ds(0, 3 * ng)], jnp.concatenate([hi, lo, hi], axis=0))

    def amplitude(v):
        hi, lo = split(v)
        parts = []
        for h in range(2):
            a, b = (jnp.concatenate([t[:, 128 * h:128 * h + 128], t[:, 256:]], axis=1) for t in (hi, lo))
            parts.append(mm(a, sel[h]) + mm(b, sel[h]))
        return jnp.concatenate([parts[0][:, :128], parts[1][:, :128], parts[0][:, 128:] + parts[1][:, 128:]], axis=1)

    load_t.wait()
    for h in range(2):
        mark = (me + 1).astype(jnp.float32)
        sel[h] = jnp.where(t_ref[pl.ds(crow + zrow * h, zrow), :].astype(jnp.float32) == mark, 1.0, 0.0).astype(jnp.bfloat16)

    def transform(blk, slots, c):
        rows = pl.ds(c * part * ng, part * ng)

        @pl.when(blk == 0)
        def _():
            own = jnp.concatenate([store[place(0, slot), rows] for slot in slots], axis=0)
            out = amplitude(own).reshape(len(slots), part * ng, width)
            for n, slot in enumerate(slots):
                amp[slot, rows] = out[n]

        p = jnp.concatenate([amp[slot, rows] * store[place(blk, slot), rows] for slot in slots], axis=0)
        q = ztrans(p).reshape(len(slots), part, ng, width)
        for n, slot in enumerate(slots):
            for r in range(part):
                work[slot, c * part + r] = ytrans(q[n, r])

    def near(blk, c):
        arrived(blk, sib, c)

        @pl.when(jnp.logical_and(blk > 0, c == 1))
        def _():
            relay(blk, 0)

        transform(blk, (me, sib), c)

    def other(blk, i):
        c = i // 2

        @pl.when(jnp.logical_and(blk == 0, i == 0))
        def _():
            serve(blk, 0)
            relay(blk, 0)

        @pl.when(i == 1)
        def _():
            serve(blk, 1)
            relay(blk, 1)

        @pl.when(i % 2 == 1)
        def _():
            arrived(blk, far, c)

        @pl.when(jnp.logical_and(blk > 0, i == 2))
        def _():
            line(blk, 1, False, "go")

        transform(blk, (jnp.where(i % 2 == 0, cross, far),), c)

    def conv(vals, kern):
        n = len(vals)
        m = n // 3
        freq = {(k % 3, k % m): min(k, n - k) for k in range(n)}
        real, pairs = [], []
        for j in range(m):
            a, b, c = (vals[(m * i + 3 * j) % n] for i in range(3))
            s = b + c
            real.append(a + s)
            pairs.append((a - 0.5 * s, (c - b) * (np.sqrt(3.0) / 2)))
        spec = []
        for k, (re, im) in enumerate(rfft(real)):
            kv = kern(freq[0, k])
            spec.append((re * kv, None if im is None else im * kv))
        real = irfft(spec, m)
        spec = []
        for k, (re, im) in enumerate(cfft(pairs, -1)):
            kv = kern(freq[1, k])
            spec.append((re * kv, im * kv))
        pairs = cfft(spec, 1)
        out = [None] * n
        for j in range(m):
            u, (re, im) = real[j], pairs[j]
            base, t = u - re, im * np.sqrt(3.0)
            out[3 * j % n] = u + (re + re)
            out[(m + 3 * j) % n] = base - t
            out[(2 * m + 3 * j) % n] = base + t
        return out

    def xconv(t):
        order = [(g, h, r) for g in range(4) for h in range(2) for r in range(planes)]
        for i in range(2):
            rows = pl.ds(pl.multiple_of(t * 16 + 8 * i, 8), 8)
            res = conv([work[g, r, rows, h * 128:h * 128 + 128] for g, h, r in order],
                       lambda k: k_ref[k, rows, :])
            for (g, h, r), v in zip(order, res):
                work[g, r, rows, h * 128:h * 128 + 128] = v
        ra = pl.ds(pl.multiple_of(t * 16, 8), 8)
        rb = pl.ds(pl.multiple_of(t * 16 + 8, 8), 8)
        left = lax.broadcasted_iota(jnp.int32, (8, 128), 1) < 64

        def half(g, h, r):
            u, w = work[g, r, ra, 256:384], work[g, r, rb, 256:384]
            if h == 0:
                return jnp.where(left, u, pltpu.roll(w, 64, 1))
            return jnp.where(left, pltpu.roll(u, 64, 1), w)

        rk = pl.ds(pl.multiple_of(ng + t * 8, 8), 8)
        res = dict(zip(order, conv([half(*o) for o in order], lambda k: k_ref[k, rk, :])))
        for g in range(4):
            for r in range(planes):
                a, b = res[(g, 0, r)], res[(g, 1, r)]
                work[g, r, ra, 256:384] = jnp.where(left, a, pltpu.roll(b, 64, 1))
                work[g, r, rb, 256:384] = jnp.where(left, pltpu.roll(a, 64, 1), b)

    def push(slot):
        return remote(vec.at[slot], recv.at[me], osem, orsem.at[me], (band, slot))

    def inverse(blk, s):
        slot = ((chip + 1 - s // 2) % 2) * 2 + (core + s % 2 + s // 2) % 2
        q = jnp.concatenate([ytrans(work[slot, r]) for r in range(planes)], axis=0)
        w = ztrans(q) * store[place(blk, slot)]

        @pl.when(jnp.logical_and(blk < 2, s == 2))
        def _():
            serve(blk + 1, 0)
            line(blk + 1, 0, False, "go")

        @pl.when(blk == 0)
        def _():
            acc[slot] = w

        @pl.when(blk == 1)
        def _():
            acc[slot] += w

        @pl.when(blk == 2)
        def _():
            hi, lo = split(acc[slot] + w)
            s_tab = t_ref[pl.ds(srow, width), pl.ds(0, 128)]
            tmp[...] = -(mm(hi, s_tab) + mm(lo, s_tab))

            def put_vec(h, q, value):
                vec[slot, packed(h, q), :] = value

            scatter_out(lambda y0: tmp[spaced(y0), :], put_vec, jnp.zeros((group, 128), jnp.float32))

            @pl.when(s < 3)
            def _():
                push(slot).start()

    def block(blk, _):
        @pl.when(blk == 0)
        def _():
            local.wait()

        def fwd_near(c, _):
            near(blk, c)
            return 0

        def fwd_other(i, _):
            other(blk, i)
            return 0

        def mid(t, _):
            xconv(t)
            return 0

        def inv(s, _):
            inverse(blk, s)
            return 0

        lax.fori_loop(0, 2, fwd_near, 0)
        lax.fori_loop(0, 4, fwd_other, 0)

        @pl.when(blk == 0)
        def _():
            load_k.wait()

        lax.fori_loop(0, ng // 16, mid, 0, unroll=True)
        lax.fori_loop(0, 4, inv, 0)
        return 0

    lax.fori_loop(0, 3, block, 0)

    def later(d, _):
        for c in range(2):
            line(d, c, False, "go")
            line(d + 1, c, True, "go")
        return 0

    lax.fori_loop(3, length, later, 0)

    def emit(src, slot):
        return pltpu.make_async_copy(src.at[slot], o_ref.at[:, slot], esem)

    def spread_out(src, slot, n):
        def put(j, y0, value):
            ebuf[n, j, spaced(y0), :] = value

        values = {(h, q): src[slot, packed(h, q), :] for h in range(2) for q in range(3)}
        gather_in(lambda b, h, q: values[h, q], put, jnp.zeros((group, 128), jnp.float32))

    order = (me, sib, cross, far)

    def columns(block, slots):
        where = [next(n for n, s in enumerate(order) if s is slot) for slot in slots]
        parts = [[jnp.zeros((8, 128), jnp.float32) for _ in range(3)] for _ in slots]
        for r in range(flat // 8):
            for j in range(3):
                phi = store[block, pl.ds(8 * r, 8), pl.ds(128 * j, 128)]
                for n, p in zip(where, parts):
                    p[j] = p[j] + phi * ebuf[n, j, pl.ds(8 * r, 8)]
        for slot, p in zip(slots, parts):
            rows_buf[slot, block] = jnp.concatenate(p, axis=1)

    def ready(block):
        near_by = jnp.logical_or(block == pair, block == third)
        return jnp.logical_or(near_by, block % 2 == side)

    def early(slots):
        def body(block, _):
            @pl.when(ready(block))
            def _():
                columns(block, slots)

            return 0

        return body

    def late(block, _):
        @pl.when(jnp.logical_not(ready(block)))
        def _():
            for c in range(2):
                came(block, c)
            columns(block, (me, sib, cross, far))

        return 0

    def settle(slot):
        remote(vec.at[slot], recv.at[slot], osem, orsem.at[slot], (band, slot)).wait_recv()
        emit(recv, slot).start()

    emit(vec, me).start()
    spread_out(vec, me, 0)
    settle(sib)
    spread_out(recv, sib, 1)
    lax.fori_loop(0, nband, early((me, sib)), 0)
    settle(cross)
    spread_out(recv, cross, 2)
    lax.fori_loop(0, nband, early((cross,)), 0)
    settle(far)
    spread_out(recv, far, 3)
    lax.fori_loop(0, nband, early((far,)), 0)
    lax.fori_loop(0, nband, late, 0)

    lanes = jnp.sum(rows_buf[...], axis=2).reshape(groups * nband, width)
    left_over = lanes
    terms = jnp.zeros((groups * nband, 128), jnp.float32)
    for _ in range(3):
        hi = left_over.astype(jnp.bfloat16)
        terms += mm(hi, t_ref[pl.ds(srow, width), pl.ds(128, 128)])
        left_over = left_over - hi.astype(jnp.float32)
    terms = (terms / ncell).reshape(groups, nband, terms.shape[-1])
    each = nband // groups
    for slot in range(groups):
        total = jnp.zeros((groups, terms.shape[-1]), jnp.float32)
        for n in range(each):
            value = terms[:, slot * each + n]
            total += pltpu.roll(value, bands * n, 1) if n else value
        mine[slot] = total

    def give(slot):
        return remote(mine.at[slot], marg.at[me], msem, mrsem.at[me], (band, slot))

    for slot in (cross, far, sib):
        give(slot).start()
    pltpu.make_async_copy(o_ref, o_ref, esem).wait()
    others = pl.ds(0, groups - 1)
    remote(vec.at[others], recv.at[others], osem, orsem.at[me], (band, sib)).wait_send()
    remote(mine.at[others], marg.at[others], msem, mrsem.at[me], (band, sib)).wait_send()
    three = store.at[pl.ds(0, 3)]
    for n in range(3):
        remote(three, three, ssem.at[n], gsem.at[0, 0], (band, sib)).wait_send()
    whole = store.at[band]

    @pl.when(ends)
    def _():
        remote(whole, whole, wsem, gsem.at[0, 0], (wrap, me)).wait_send()

    @pl.when(has_down)
    def _():
        remote(whole, whole, dsem, gsem.at[0, 0], (down, me)).wait_send()

    for c in range(2):
        along(band, ysem.at[pos, c], pair, c).wait_send()

        @pl.when(has_up)
        def _():
            along(band, zsem.at[pos, c], up, c).wait_send()

    def finish_line(i, _):
        line(1 + i // 2, i % 2, True, "end")
        line(1 + i // 2, i % 2, False, "end")
        return 0

    lax.fori_loop(0, 2 * (length - 1), finish_line, 0)
    total = mine[me]
    for slot in (sib, cross, far):
        remote(mine.at[slot], marg.at[slot], msem, mrsem.at[slot], (band, slot)).wait_recv()
        total += marg[slot]
    m_ref[...] = total[:, :nband]


def lane_tables(ng, bands):
    w = bands * ng
    half, bz = [], []
    for lo, hi in ((0, 128), (128, w)):
        for h in range(2):
            half.append(np.full(hi - lo, h))
            bz.append(np.arange(lo, hi))
    half, bz = np.concatenate(half), np.concatenate(bz)
    return half, bz // ng, bz % ng


def tiles(table, half):
    out = []
    for h in range(2):
        pick = np.concatenate([np.arange(128 * h, 128 * h + 128), np.arange(256, len(half))])
        live = half[pick] == h
        out.append(np.where(live[:, None] & live[None, :], table[pick][:, pick], 0.0))
    return np.stack(out)


def solve(nat, ng, groups, nband):
    bands = nat.shape[1]
    width = 2 * bands * ng
    flat = nat.shape[0] * nat.shape[2] // (2 * ng)
    half, bnd, zed = lane_tables(ng, bands)
    ht = hartley(ng)
    th, tl = split_const(ht)
    same = (half[:, None] == half[None, :])
    zmat = np.where(same & (bnd[:, None] == bnd[None, :]), ht[zed[:, None], zed[None, :]], 0.0)
    zt = np.stack(split_const(tiles(zmat, half)), axis=1)
    ty = np.concatenate([th, th, tl], axis=1)
    cp = tiles(np.where(same & (zed[:, None] == zed[None, :]), bnd[:, None] + 1.0, 0.0), half)
    s = np.zeros((width, 128), np.float32)
    s[np.arange(width), half * ng + zed] = 1.0
    hot = np.zeros((width, 128), np.float32)
    hot[np.arange(width), bnd] = 1.0
    kv = kernel_values(ng).astype(np.float32) / np.float32(ng**3)
    kb = np.tile(kv, (1, 1, bands))
    k1 = kb[:, :, :128]
    rest = kb[:, :, 128:].reshape(kb.shape[0], ng // 16, 2, 8, 64)
    k2 = np.concatenate([rest[:, :, 0], rest[:, :, 1]], axis=-1).reshape(kb.shape[0], ng // 2, 128)
    b16 = jnp.bfloat16
    tyw = np.zeros((ng, 256), b16)
    tyw[:, : 3 * ng] = ty
    tab = [zt.reshape(-1, 256), cp.astype(b16).reshape(-1, 256), np.concatenate([s, hot], axis=1).astype(b16), tyw]
    consts = [np.concatenate([k1, k2], axis=1), np.concatenate(tab, axis=0)]
    full = (groups, flat, width)
    slim = (groups, nat.shape[0], nat.shape[2])
    f32, dma = jnp.float32, pltpu.SemaphoreType.DMA
    return pl.pallas_call(
        functools.partial(solve_kernel, ng, ng**3),
        out_shape=(
            jax.ShapeDtypeStruct(nat.shape, f32), jax.ShapeDtypeStruct((groups, nband), f32)
        ),
        in_specs=[pl.BlockSpec(memory_space=pl.ANY)] * (1 + len(consts)),
        out_specs=(pl.BlockSpec(memory_space=pl.ANY), pl.BlockSpec(memory_space=pltpu.VMEM)),
        scratch_shapes=[
            pltpu.VMEM((2, 2, bands, slim[1] // 4, 128), f32), *[pltpu.VMEM(c.shape, c.dtype) for c in consts],
            pltpu.VMEM(full[1:], f32), pltpu.VMEM((nband + 3 * groups,) + full[1:], f32),
            pltpu.VMEM(full, f32), pltpu.VMEM(full, f32), pltpu.VMEM((groups, flat // ng, ng, width), f32),
            pltpu.VMEM(slim, f32), pltpu.VMEM(slim, f32),
            pltpu.VMEM((2, 256, 256), b16), pltpu.VMEM((groups, nband, 8, width), f32),
            pltpu.VMEM((groups, groups, 128), f32), pltpu.VMEM((groups, groups, 128), f32),
            dma((3, groups - 1, 2)), dma((3,)), dma((nband, 2)), dma((nband // 2, 2)), dma((nband // 2, 2)), dma(()), dma(()),
            dma(()), dma((groups,)), dma(()), dma((groups,)), dma(()), dma((2,)), dma(()), dma((2,)),
            pltpu.VMEM((flat, 128), f32), pltpu.VMEM((groups, 3, flat, 128), f32),
        ],
        compiler_params=pltpu.CompilerParams(
            vmem_limit_bytes=55_800_000, collective_id=0, has_side_effects=True
        ),
        cost_estimate=pl.CostEstimate(flops=10**11, bytes_accessed=10**7, transcendentals=0),
        name="solve",
    )(nat, *[jnp.asarray(c) for c in consts])


def on_device(orbitals):
    groups, nband = lax.axis_size("grid"), lax.axis_size("band")
    bands, local = orbitals.shape
    ncell = local * groups
    ng = round(ncell ** (1 / 3))
    nat = orbitals.reshape(bands, local // 128, 128).transpose(1, 0, 2)
    out, marg = solve(nat, ng, groups, nband)
    vectors = out.transpose(1, 0, 2).reshape(bands, local)
    margin = marg.T
    return (vectors, margin)


def solution(mesh):
    return jax.shard_map(
        on_device,
        mesh=mesh,
        in_specs=(P("band", "grid"),),
        out_specs=(P("band", "grid"), P("grid", "band")),
        check_vma=False,
    )
```

```python
import functools

import jax
import jax.numpy as jnp
import numpy as np
from jax import lax
from jax.experimental import pallas as pl
from jax.experimental.pallas import tpu as pltpu
from jax.sharding import PartitionSpec as P


def kernel_values(ng):
    freqs = ((np.arange(ng) + ng // 2) % ng - ng // 2).astype(np.float32)
    sq = freqs[: ng // 2 + 1, None, None] ** 2 + freqs[None, :, None] ** 2 + freqs[None, None, :] ** 2
    safe = np.where(sq > 0, sq, np.float32(1.0))
    return np.where(sq > 0, 40.0 * (1.0 - np.exp(-sq / 16.0)) / safe, 0.0)


def hartley(ng):
    k = np.arange(ng)
    ang = (k[:, None] * k[None, :] % ng) * (2.0 * np.pi / ng)
    return np.cos(ang) + np.sin(ang)


def split_const(table):
    table = np.asarray(table, np.float32)
    hi = table.astype(jnp.bfloat16)
    lo = (table - hi.astype(np.float32)).astype(jnp.bfloat16)
    return hi, lo


def rfft(xs):
    n = len(xs)
    if n == 1:
        return [(xs[0], None)]
    even, odd = rfft(xs[0::2]), rfft(xs[1::2])
    half = n // 2
    out = [None] * (half + 1)
    for k in range(half // 2 + 1):
        er, ei = even[k]
        orr, oi = odd[k]
        if k == 0:
            out[0] = (er + orr, None)
            out[half] = (er - orr, None)
            continue
        c, s = np.cos(2 * np.pi * k / n), -np.sin(2 * np.pi * k / n)
        if 2 * k == half:
            out[k] = (er, -orr)
            continue
        tr, ti = cmul(orr, oi, c, s)
        out[k] = (er + tr, addo(ei, ti))
        out[half - k] = (er - tr, subo(ti, ei))
    return out


def addo(a, b):
    return b if a is None else a + b


def subo(a, b):
    return a if b is None else a - b


def cmul(r, i, c, s):
    if i is None:
        return r * c, r * s
    if abs(abs(c) - abs(s)) < 1e-9:
        if s < 0 < c:
            return (r + i) * c, (i - r) * c
        return (r - i) * c, (r + i) * c
    return r * c - i * s, r * s + i * c


def irfft(spec, n):
    if n == 1:
        return [spec[0][0]]
    half = n // 2
    even, odd = [None] * (half // 2 + 1), [None] * (half // 2 + 1)
    for k in range(half // 2 + 1):
        yr, yi = spec[k]
        if k == 0:
            hr = spec[half][0]
            even[0] = (yr + hr, None)
            odd[0] = (yr - hr, None)
            continue
        if 2 * k == half:
            even[k] = (yr + yr, None)
            odd[k] = (-(yi + yi), None)
            continue
        zr, zi = spec[half - k]
        er, ei = yr + zr, yi - zi
        dr, di = yr - zr, yi + zi
        c, s = np.cos(2 * np.pi * k / n), np.sin(2 * np.pi * k / n)
        even[k] = (er, ei)
        odd[k] = cmul(dr, di, c, s)
    ev, od = irfft(even, half), irfft(odd, half)
    out = [None] * n
    out[0::2], out[1::2] = ev, od
    return out


def cfft(xs, sign):
    n = len(xs)
    if n == 1:
        return xs
    even, odd = cfft(xs[0::2], sign), cfft(xs[1::2], sign)
    half = n // 2
    out = [None] * n
    for k in range(half):
        (er, ei), (r, i) = even[k], odd[k]
        if 4 * k == n:
            out[k] = (er + i, ei - r) if sign < 0 else (er - i, ei + r)
            out[k + half] = (er - i, ei + r) if sign < 0 else (er + i, ei - r)
            continue
        if k == 0:
            tr, ti = r, i
        else:
            tr, ti = turn(r, i, np.cos(2 * np.pi * k / n), sign * np.sin(2 * np.pi * k / n))
        out[k] = (er + tr, ei + ti)
        out[k + half] = (er - tr, ei - ti)
    return out


def turn(r, i, c, s):
    if abs(abs(c) - abs(s)) > 1e-9:
        return r * c - i * s, r * s + i * c
    if c * s > 0:
        return (r - i) * c, (r + i) * c
    return (r + i) * c, (i - r) * c


def split(v):
    hi = v.astype(jnp.bfloat16)
    lo = (v - hi.astype(jnp.float32)).astype(jnp.bfloat16)
    return hi, lo


def mm(a, b):
    return jnp.dot(a, b, preferred_element_type=jnp.float32)


def in_copies(in_ref, nat_ref, sems, c):
    size = nat_ref.shape[3]
    return [
        pltpu.make_async_copy(in_ref.at[pl.ds((2 * h + c) * size, size), b], nat_ref.at[c, h, b], sems.at[c])
        for h in range(2)
        for b in range(in_ref.shape[1])
    ]


def solve_kernel(ng, ncell, in_ref, *refs):
    (k_hbm, t_hbm, o_ref, m_ref, nat_ref, k_ref, t_ref, own_ref, store, amp, acc, work, vec, recv, sel, rows_buf, mine, marg,
     rsem, ssem, gsem, ysem, zsem, dsem, wsem, osem, orsem, msem, mrsem, lsem, csem, esem, isem, tmp, ebuf) = refs
    for copy in in_copies(in_ref, nat_ref, isem, 0) + in_copies(in_ref, nat_ref, isem, 1):
        copy.start()
    load_t = pltpu.make_async_copy(t_hbm, t_ref, csem.at[0])
    load_k = pltpu.make_async_copy(k_hbm, k_ref, csem.at[1])
    load_t.start()
    load_k.start()
    bands = in_ref.shape[1]
    flat, width = own_ref.shape
    planes = flat // ng
    groups = vec.shape[0]
    me = lax.axis_index("grid")
    band, nband = lax.axis_index("band"), lax.axis_size("band")
    chip, core = me // 2, me % 2
    sib = chip * 2 + (1 - core)
    cross = (1 - chip) * 2 + core
    far = (1 - chip) * 2 + (1 - core)
    length = nband // 2
    side, pos = band % 2, band // 2
    pair = band + 1 - 2 * side
    third = (band + nband - 1 + 2 * side) % nband
    first, last = band == 0, band == nband - 1
    ends = jnp.logical_or(first, last)
    wrap = jnp.where(first, nband - 1, 0)
    has_up, has_down = pos < length - 1, pos > 0
    up, down = jnp.where(has_up, band + 2, band), jnp.where(has_down, band - 2, band)
    mesh_id = pl.DeviceIdType.MESH
    part = planes // 2
    zrow, crow = 256, 1024
    srow = crow + 512
    yrow = srow + width

    def remote(src, dst, send, recv_sem, device):
        return pltpu.make_async_remote_copy(
            src_ref=src, dst_ref=dst, send_sem=send, recv_sem=recv_sem,
            device_id=device, device_id_type=mesh_id,
        )

    def partner(blk):
        return jnp.where(blk == 0, band, jnp.where(blk == 1, pair, third))

    def place(blk, slot):
        return jnp.where(slot == me, partner(blk), nband + blk * groups + slot)

    def piece(ref, c):
        return ref.at[pl.ds(c * part * ng, part * ng)]

    def skip(slot, at):
        return slot - (slot > at).astype(jnp.int32)

    def share(blk, lane, slot, src, target, c):
        dst = store.at[nband + blk * groups + slot]
        return remote(piece(src, c), piece(dst, c), ssem.at[lane], rsem.at[blk, skip(slot, target), c], (band, target))

    def along(block, sem, device, c, src=None):
        dst = store.at[block]
        src = dst if src is None else src
        return remote(piece(src, c), piece(dst, c), sem, gsem.at[block, c], (device, me))

    def came(block, c):
        along(block, wsem, pair, c).wait_recv()

    lane = lax.broadcasted_iota(jnp.int32, (1, 128), 1)

    def moved(value, shift, low, high, under):
        out = pltpu.roll(value, shift % 128, 1) if shift % 128 else value
        return jnp.where(jnp.logical_and(lane >= low, lane < high), out, under)

    def gather_in(read, want, blank):
        for y0 in range(8):
            chunks = [None, None, None]
            for h in range(2):
                for b in range(bands):
                    for target, start, stop, base in ((h, 0, 128, 0), (2, 128, bands * ng, 64 * h)):
                        first, final = max(start, b * ng), min(stop, b * ng + ng)
                        if first >= final:
                            continue
                        source = y0 * ng + first - b * ng
                        place_at = first - start + base
                        while first < final:
                            q, off = source // 128, source % 128
                            size = min(final - first, 128 - off)
                            under = chunks[target]
                            under = blank if under is None else under
                            chunks[target] = moved(read(b, h, q), place_at - off, place_at, place_at + size, under)
                            first, source, place_at = first + size, source + size, place_at + size
            for j, value in enumerate(chunks):
                want(j, y0, value)

    def scatter_out(read, write, blank):
        for h in range(2):
            chunks = [blank] * 3
            for y0 in range(8):
                value = read(y0)
                source, at, left = h * ng, y0 * ng, ng
                while left > 0:
                    q, off = at // 128, at % 128
                    size = min(left, 128 - off)
                    chunks[q] = moved(value, off - source, off, off + size, chunks[q])
                    source, at, left = source + size, at + size, left - size
            for q in range(3):
                write(h, q, chunks[q])

    group = flat // 8

    def packed(h, q):
        return pl.ds(q + 3 * group * h, group, stride=3)

    def spaced(y0):
        return pl.ds(y0, group, stride=8)

    def greet(device):
        pl.semaphore_signal(barrier, inc=1, device_id=device, device_id_type=mesh_id)

    barrier = pltpu.get_barrier_semaphore()
    for device in ((band, sib), (band, cross), (band, far), (pair, me)):
        greet(device)

    @pl.when(has_up)
    def _():
        greet((up, me))

    @pl.when(has_down)
    def _():
        greet((down, me))

    @pl.when(ends)
    def _():
        greet((wrap, me))

    count = 4 + has_up.astype(jnp.int32) + has_down.astype(jnp.int32) + ends.astype(jnp.int32)
    def own_copies(c):
        share(0, 1, me, own_ref, cross, c).start()
        share(0, 0, me, own_ref, sib, c).start()
        along(band, ysem.at[pos, c], pair, c, own_ref).start()

        @pl.when(has_up)
        def _():
            along(band, zsem.at[pos, c], up, c, own_ref).start()

        @pl.when(has_down)
        def _():
            along(band, dsem, down, c, own_ref).start()

    few = group // 2
    for c in range(2):
        pltpu.make_async_copy(nat_ref.at[c], nat_ref.at[c], isem.at[c]).wait()

        def put_own(j, y0, value):
            ebuf[0, j, pl.ds(c * part * ng + y0, few, stride=8), :] = value

        gather_in(
            lambda b, h, q: nat_ref[c, h, b, pl.ds(q, few, stride=3), :], put_own, jnp.zeros((few, 128), jnp.float32)
        )
        half_rows = pl.ds(c * part * ng, part * ng)
        own_ref[half_rows, :] = jnp.concatenate([ebuf[0, j, half_rows, :] for j in range(3)], axis=1)
        if c == 0:
            pl.semaphore_wait(barrier, count)
        own_copies(c)

    @pl.when(ends)
    def _():
        for c in range(2):
            along(band, wsem, wrap, c, own_ref).start()

    local = pltpu.make_async_copy(own_ref, store.at[band], lsem)
    local.start()

    def arrived(blk, slot, c):
        dst = piece(store.at[nband + blk * groups + slot], c)
        remote(dst, dst, ssem.at[0], rsem.at[blk, skip(slot, me), c], (band, sib)).wait_recv()

    def relay(blk, c):
        arrived(blk, cross, c)
        share(blk, 2, cross, store.at[nband + blk * groups + cross], sib, c).start()

    def spread(blk, c):
        came(partner(blk), c)
        share(blk, 1, me, store.at[partner(blk)], cross, c).start()
        share(blk, 0, me, store.at[partner(blk)], sib, c).start()

    def skipped(block):
        return jnp.logical_or(
            jnp.logical_and(pair == 0, block == nband - 1), jnp.logical_and(pair == nband - 1, block == 0)
        )

    def line(d, c, near, act):
        def pass_on(block, exists, on, device):
            @pl.when(exists)
            def _():
                if act == "go":
                    came(block, c)

                def one(copy):
                    copy.start() if act == "go" else copy.wait_send()

                @pl.when(jnp.logical_not(skipped(block)))
                def _():
                    one(along(block, ysem.at[block // 2, c], pair, c))

                @pl.when(on)
                def _():
                    one(along(block, zsem.at[block // 2, c], device, c))

        upward = (side == 1) == near
        pass_on(band - 2 * d, jnp.logical_and(upward, pos - d >= 0), has_up, up)
        pass_on(
            band + 2 * d, jnp.logical_and(jnp.logical_not(upward), pos + d <= length - 1), has_down, down
        )

    def serve(blk, c):
        @pl.when(blk < 2)
        def _():
            spread(blk + 1, c)

        line(blk + 1, c, True, "go")

    def ztrans(v):
        hi, lo = split(v)
        parts = []
        for h in range(2):
            a, b = (jnp.concatenate([t[:, 128 * h:128 * h + 128], t[:, 256:]], axis=1) for t in (hi, lo))
            high, low = (t_ref[pl.ds((2 * h + n) * zrow, zrow), :] for n in range(2))
            parts.append(mm(a, high) + mm(b, high) + mm(a, low))
        return jnp.concatenate([parts[0][:, :128], parts[1][:, :128], parts[0][:, 128:] + parts[1][:, 128:]], axis=1)

    def ytrans(v):
        hi, lo = split(v)
        return mm(t_ref[pl.ds(yrow, ng), pl.ds(0, 3 * ng)], jnp.concatenate([hi, lo, hi], axis=0))

    def amplitude(v):
        hi, lo = split(v)
        parts = []
        for h in range(2):
            a, b = (jnp.concatenate([t[:, 128 * h:128 * h + 128], t[:, 256:]], axis=1) for t in (hi, lo))
            parts.append(mm(a, sel[h]) + mm(b, sel[h]))
        return jnp.concatenate([parts[0][:, :128], parts[1][:, :128], parts[0][:, 128:] + parts[1][:, 128:]], axis=1)

    load_t.wait()
    for h in range(2):
        mark = (me + 1).astype(jnp.float32)
        sel[h] = jnp.where(t_ref[pl.ds(crow + zrow * h, zrow), :].astype(jnp.float32) == mark, 1.0, 0.0).astype(jnp.bfloat16)

    def transform(blk, slots, c):
        rows = pl.ds(c * part * ng, part * ng)

        @pl.when(blk == 0)
        def _():
            own = jnp.concatenate([store[place(0, slot), rows] for slot in slots], axis=0)
            out = amplitude(own).reshape(len(slots), part * ng, width)
            for n, slot in enumerate(slots):
                amp[slot, rows] = out[n]

        p = jnp.concatenate([amp[slot, rows] * store[place(blk, slot), rows] for slot in slots], axis=0)
        q = ztrans(p).reshape(len(slots), part, ng, width)
        for n, slot in enumerate(slots):
            for r in range(part):
                work[slot, c * part + r] = ytrans(q[n, r])

    def near(blk, c):
        arrived(blk, sib, c)

        @pl.when(jnp.logical_and(blk > 0, c == 1))
        def _():
            relay(blk, 0)

        transform(blk, (me, sib), c)

    def other(blk, i):
        c = i // 2

        @pl.when(jnp.logical_and(blk == 0, i == 0))
        def _():
            serve(blk, 0)
            relay(blk, 0)

        @pl.when(i == 1)
        def _():
            serve(blk, 1)
            relay(blk, 1)

        @pl.when(i % 2 == 1)
        def _():
            arrived(blk, far, c)

        @pl.when(jnp.logical_and(blk > 0, i == 2))
        def _():
            line(blk, 1, False, "go")

        transform(blk, (jnp.where(i % 2 == 0, cross, far),), c)

    def conv(vals, kern):
        n = len(vals)
        m = n // 3
        freq = {(k % 3, k % m): min(k, n - k) for k in range(n)}
        real, pairs = [], []
        for j in range(m):
            a, b, c = (vals[(m * i + 3 * j) % n] for i in range(3))
            s = b + c
            real.append(a + s)
            pairs.append((a - 0.5 * s, (c - b) * (np.sqrt(3.0) / 2)))
        spec = []
        for k, (re, im) in enumerate(rfft(real)):
            kv = kern(freq[0, k])
            spec.append((re * kv, None if im is None else im * kv))
        real = irfft(spec, m)
        spec = []
        for k, (re, im) in enumerate(cfft(pairs, -1)):
            kv = kern(freq[1, k])
            spec.append((re * kv, im * kv))
        pairs = cfft(spec, 1)
        out = [None] * n
        for j in range(m):
            u, (re, im) = real[j], pairs[j]
            base, t = u - re, im * np.sqrt(3.0)
            out[3 * j % n] = u + (re + re)
            out[(m + 3 * j) % n] = base - t
            out[(2 * m + 3 * j) % n] = base + t
        return out

    def xconv(t):
        order = [(g, h, r) for g in range(4) for h in range(2) for r in range(planes)]
        for i in range(2):
            rows = pl.ds(pl.multiple_of(t * 16 + 8 * i, 8), 8)
            res = conv([work[g, r, rows, h * 128:h * 128 + 128] for g, h, r in order],
                       lambda k: k_ref[k, rows, :])
            for (g, h, r), v in zip(order, res):
                work[g, r, rows, h * 128:h * 128 + 128] = v
        ra = pl.ds(pl.multiple_of(t * 16, 8), 8)
        rb = pl.ds(pl.multiple_of(t * 16 + 8, 8), 8)
        left = lax.broadcasted_iota(jnp.int32, (8, 128), 1) < 64

        def half(g, h, r):
            u, w = work[g, r, ra, 256:384], work[g, r, rb, 256:384]
            if h == 0:
                return jnp.where(left, u, pltpu.roll(w, 64, 1))
            return jnp.where(left, pltpu.roll(u, 64, 1), w)

        rk = pl.ds(pl.multiple_of(ng + t * 8, 8), 8)
        res = dict(zip(order, conv([half(*o) for o in order], lambda k: k_ref[k, rk, :])))
        for g in range(4):
            for r in range(planes):
                a, b = res[(g, 0, r)], res[(g, 1, r)]
                work[g, r, ra, 256:384] = jnp.where(left, a, pltpu.roll(b, 64, 1))
                work[g, r, rb, 256:384] = jnp.where(left, pltpu.roll(a, 64, 1), b)

    def push(slot):
        return remote(vec.at[slot], recv.at[me], osem, orsem.at[me], (band, slot))

    def inverse(blk, s):
        slot = ((chip + 1 - s // 2) % 2) * 2 + (core + s % 2 + s // 2) % 2
        q = jnp.concatenate([ytrans(work[slot, r]) for r in range(planes)], axis=0)
        w = ztrans(q) * store[place(blk, slot)]

        @pl.when(jnp.logical_and(blk < 2, s == 2))
        def _():
            serve(blk + 1, 0)
            line(blk + 1, 0, False, "go")

        @pl.when(blk == 0)
        def _():
            acc[slot] = w

        @pl.when(blk == 1)
        def _():
            acc[slot] += w

        @pl.when(blk == 2)
        def _():
            hi, lo = split(acc[slot] + w)
            s_tab = t_ref[pl.ds(srow, width), pl.ds(0, 128)]
            tmp[...] = -(mm(hi, s_tab) + mm(lo, s_tab))

            def put_vec(h, q, value):
                vec[slot, packed(h, q), :] = value

            scatter_out(lambda y0: tmp[spaced(y0), :], put_vec, jnp.zeros((group, 128), jnp.float32))

            @pl.when(s < 3)
            def _():
                push(slot).start()

    def block(blk, _):
        @pl.when(blk == 0)
        def _():
            local.wait()

        def fwd_near(c, _):
            near(blk, c)
            return 0

        def fwd_other(i, _):
            other(blk, i)
            return 0

        def mid(t, _):
            xconv(t)
            return 0

        def inv(s, _):
            inverse(blk, s)
            return 0

        lax.fori_loop(0, 2, fwd_near, 0)
        lax.fori_loop(0, 4, fwd_other, 0)

        @pl.when(blk == 0)
        def _():
            load_k.wait()

        lax.fori_loop(0, ng // 16, mid, 0, unroll=True)
        lax.fori_loop(0, 4, inv, 0)
        return 0

    lax.fori_loop(0, 3, block, 0)

    def later(d, _):
        for c in range(2):
            line(d, c, False, "go")
            line(d + 1, c, True, "go")
        return 0

    lax.fori_loop(3, length, later, 0)

    def emit(src, slot):
        return pltpu.make_async_copy(src.at[slot], o_ref.at[:, slot], esem)

    def spread_out(src, slot, n):
        def put(j, y0, value):
            ebuf[n, j, spaced(y0), :] = value

        values = {(h, q): src[slot, packed(h, q), :] for h in range(2) for q in range(3)}
        gather_in(lambda b, h, q: values[h, q], put, jnp.zeros((group, 128), jnp.float32))

    order = (me, sib, cross, far)

    def columns(block, slots):
        where = [next(n for n, s in enumerate(order) if s is slot) for slot in slots]
        parts = [[jnp.zeros((8, 128), jnp.float32) for _ in range(3)] for _ in slots]
        for r in range(flat // 8):
            for j in range(3):
                phi = store[block, pl.ds(8 * r, 8), pl.ds(128 * j, 128)]
                for n, p in zip(where, parts):
                    p[j] = p[j] + phi * ebuf[n, j, pl.ds(8 * r, 8)]
        for slot, p in zip(slots, parts):
            rows_buf[slot, block] = jnp.concatenate(p, axis=1)

    def ready(block):
        near_by = jnp.logical_or(block == pair, block == third)
        return jnp.logical_or(near_by, block % 2 == side)

    def early(slots):
        def body(block, _):
            @pl.when(ready(block))
            def _():
                columns(block, slots)

            return 0

        return body

    def late(block, _):
        @pl.when(jnp.logical_not(ready(block)))
        def _():
            for c in range(2):
                came(block, c)
            columns(block, (me, sib, cross, far))

        return 0

    def settle(slot):
        remote(vec.at[slot], recv.at[slot], osem, orsem.at[slot], (band, slot)).wait_recv()
        emit(recv, slot).start()

    emit(vec, me).start()
    spread_out(vec, me, 0)
    settle(sib)
    spread_out(recv, sib, 1)
    lax.fori_loop(0, nband, early((me, sib)), 0)
    settle(cross)
    spread_out(recv, cross, 2)
    lax.fori_loop(0, nband, early((cross,)), 0)
    settle(far)
    spread_out(recv, far, 3)
    lax.fori_loop(0, nband, early((far,)), 0)
    lax.fori_loop(0, nband, late, 0)

    lanes = jnp.sum(rows_buf[...], axis=2).reshape(groups * nband, width)
    left_over = lanes
    terms = jnp.zeros((groups * nband, 128), jnp.float32)
    for _ in range(3):
        hi = left_over.astype(jnp.bfloat16)
        terms += mm(hi, t_ref[pl.ds(srow, width), pl.ds(128, 128)])
        left_over = left_over - hi.astype(jnp.float32)
    terms = (terms / ncell).reshape(groups, nband, terms.shape[-1])
    each = nband // groups
    for slot in range(groups):
        total = jnp.zeros((groups, terms.shape[-1]), jnp.float32)
        for n in range(each):
            value = terms[:, slot * each + n]
            total += pltpu.roll(value, bands * n, 1) if n else value
        mine[slot] = total

    def give(slot):
        return remote(mine.at[slot], marg.at[me], msem, mrsem.at[me], (band, slot))

    for slot in (cross, far, sib):
        give(slot).start()
    pltpu.make_async_copy(o_ref, o_ref, esem).wait()
    others = pl.ds(0, groups - 1)
    remote(vec.at[others], recv.at[others], osem, orsem.at[me], (band, sib)).wait_send()
    remote(mine.at[others], marg.at[others], msem, mrsem.at[me], (band, sib)).wait_send()
    three = store.at[pl.ds(0, 3)]
    for n in range(3):
        remote(three, three, ssem.at[n], gsem.at[0, 0], (band, sib)).wait_send()
    whole = store.at[band]

    @pl.when(ends)
    def _():
        remote(whole, whole, wsem, gsem.at[0, 0], (wrap, me)).wait_send()

    @pl.when(has_down)
    def _():
        remote(whole, whole, dsem, gsem.at[0, 0], (down, me)).wait_send()

    for c in range(2):
        along(band, ysem.at[pos, c], pair, c).wait_send()

        @pl.when(has_up)
        def _():
            along(band, zsem.at[pos, c], up, c).wait_send()

    def finish_line(i, _):
        line(1 + i // 2, i % 2, True, "end")
        line(1 + i // 2, i % 2, False, "end")
        return 0

    lax.fori_loop(0, 2 * (length - 1), finish_line, 0)
    total = mine[me]
    for slot in (sib, cross, far):
        remote(mine.at[slot], marg.at[slot], msem, mrsem.at[slot], (band, slot)).wait_recv()
        total += marg[slot]
    m_ref[...] = total[:, :nband]


def lane_tables(ng, bands):
    w = bands * ng
    half, bz = [], []
    for lo, hi in ((0, 128), (128, w)):
        for h in range(2):
            half.append(np.full(hi - lo, h))
            bz.append(np.arange(lo, hi))
    half, bz = np.concatenate(half), np.concatenate(bz)
    return half, bz // ng, bz % ng


def tiles(table, half):
    out = []
    for h in range(2):
        pick = np.concatenate([np.arange(128 * h, 128 * h + 128), np.arange(256, len(half))])
        live = half[pick] == h
        out.append(np.where(live[:, None] & live[None, :], table[pick][:, pick], 0.0))
    return np.stack(out)


def solve(nat, ng, groups, nband):
    bands = nat.shape[1]
    width = 2 * bands * ng
    flat = nat.shape[0] * nat.shape[2] // (2 * ng)
    half, bnd, zed = lane_tables(ng, bands)
    ht = hartley(ng)
    th, tl = split_const(ht)
    same = (half[:, None] == half[None, :])
    zmat = np.where(same & (bnd[:, None] == bnd[None, :]), ht[zed[:, None], zed[None, :]], 0.0)
    zt = np.stack(split_const(tiles(zmat, half)), axis=1)
    ty = np.concatenate([th, th, tl], axis=1)
    cp = tiles(np.where(same & (zed[:, None] == zed[None, :]), bnd[:, None] + 1.0, 0.0), half)
    s = np.zeros((width, 128), np.float32)
    s[np.arange(width), half * ng + zed] = 1.0
    hot = np.zeros((width, 128), np.float32)
    hot[np.arange(width), bnd] = 1.0
    kv = kernel_values(ng).astype(np.float32) / np.float32(ng**3)
    kb = np.tile(kv, (1, 1, bands))
    k1 = kb[:, :, :128]
    rest = kb[:, :, 128:].reshape(kb.shape[0], ng // 16, 2, 8, 64)
    k2 = np.concatenate([rest[:, :, 0], rest[:, :, 1]], axis=-1).reshape(kb.shape[0], ng // 2, 128)
    b16 = jnp.bfloat16
    tyw = np.zeros((ng, 256), b16)
    tyw[:, : 3 * ng] = ty
    tab = [zt.reshape(-1, 256), cp.astype(b16).reshape(-1, 256), np.concatenate([s, hot], axis=1).astype(b16), tyw]
    consts = [np.concatenate([k1, k2], axis=1), np.concatenate(tab, axis=0)]
    full = (groups, flat, width)
    slim = (groups, nat.shape[0], nat.shape[2])
    f32, dma = jnp.float32, pltpu.SemaphoreType.DMA
    return pl.pallas_call(
        functools.partial(solve_kernel, ng, ng**3),
        out_shape=(
            jax.ShapeDtypeStruct(nat.shape, f32), jax.ShapeDtypeStruct((groups, nband), f32)
        ),
        in_specs=[pl.BlockSpec(memory_space=pl.ANY)] * (1 + len(consts)),
        out_specs=(pl.BlockSpec(memory_space=pl.ANY), pl.BlockSpec(memory_space=pltpu.VMEM)),
        scratch_shapes=[
            pltpu.VMEM((2, 2, bands, slim[1] // 4, 128), f32), *[pltpu.VMEM(c.shape, c.dtype) for c in consts],
            pltpu.VMEM(full[1:], f32), pltpu.VMEM((nband + 3 * groups,) + full[1:], f32),
            pltpu.VMEM(full, f32), pltpu.VMEM(full, f32), pltpu.VMEM((groups, flat // ng, ng, width), f32),
            pltpu.VMEM(slim, f32), pltpu.VMEM(slim, f32),
            pltpu.VMEM((2, 256, 256), b16), pltpu.VMEM((groups, nband, 8, width), f32),
            pltpu.VMEM((groups, groups, 128), f32), pltpu.VMEM((groups, groups, 128), f32),
            dma((3, groups - 1, 2)), dma((3,)), dma((nband, 2)), dma((nband // 2, 2)), dma((nband // 2, 2)), dma(()), dma(()),
            dma(()), dma((groups,)), dma(()), dma((groups,)), dma(()), dma((2,)), dma(()), dma((2,)),
            pltpu.VMEM((flat, 128), f32), pltpu.VMEM((groups, 3, flat, 128), f32),
        ],
        compiler_params=pltpu.CompilerParams(
            vmem_limit_bytes=55_800_000, collective_id=0, has_side_effects=True
        ),
        cost_estimate=pl.CostEstimate(flops=10**11, bytes_accessed=10**7, transcendentals=0),
        name="solve",
    )(nat, *[jnp.asarray(c) for c in consts])


def leave_kernel(a_ref, b_ref, c_ref, d_ref, sems):
    copies = [pltpu.make_async_copy(a_ref, c_ref, sems.at[0]), pltpu.make_async_copy(b_ref, d_ref, sems.at[1])]
    for copy in copies:
        copy.start()
    for copy in copies:
        copy.wait()


def leave(a, b):
    anywhere = pl.BlockSpec(memory_space=pl.ANY)
    return pl.pallas_call(
        leave_kernel,
        out_shape=(jax.ShapeDtypeStruct(a.shape, a.dtype), jax.ShapeDtypeStruct(b.shape, b.dtype)),
        in_specs=[pl.BlockSpec(memory_space=pltpu.VMEM)] * 2,
        out_specs=(anywhere, anywhere),
        scratch_shapes=[pltpu.SemaphoreType.DMA((2,))],
        compiler_params=pltpu.CompilerParams(vmem_limit_bytes=1 << 20),
        name="leave",
    )(a, b)


def on_device(orbitals):
    groups, nband = lax.axis_size("grid"), lax.axis_size("band")
    bands, local = orbitals.shape
    ncell = local * groups
    ng = round(ncell ** (1 / 3))
    nat = orbitals.reshape(bands, local // 128, 128).transpose(1, 0, 2)
    out, marg = leave(*solve(nat, ng, groups, nband))
    vectors = out.transpose(1, 0, 2).reshape(bands, local)
    margin = marg.T
    return (vectors, margin)


def solution(mesh):
    return jax.shard_map(
        on_device,
        mesh=mesh,
        in_specs=(P("band", "grid"),),
        out_specs=(P("band", "grid"), P("grid", "band")),
        check_vma=False,
    )
```

```python
import functools

import jax
import jax.numpy as jnp
import numpy as np
from jax import lax
from jax.experimental import pallas as pl
from jax.experimental.pallas import tpu as pltpu
from jax.sharding import PartitionSpec as P


def kernel_values(ng):
    freqs = ((np.arange(ng) + ng // 2) % ng - ng // 2).astype(np.float32)
    sq = freqs[: ng // 2 + 1, None, None] ** 2 + freqs[None, :, None] ** 2 + freqs[None, None, :] ** 2
    safe = np.where(sq > 0, sq, np.float32(1.0))
    return np.where(sq > 0, 40.0 * (1.0 - np.exp(-sq / 16.0)) / safe, 0.0)


def hartley(ng):
    k = np.arange(ng)
    ang = (k[:, None] * k[None, :] % ng) * (2.0 * np.pi / ng)
    return np.cos(ang) + np.sin(ang)


def split_const(table):
    table = np.asarray(table, np.float32)
    hi = table.astype(jnp.bfloat16)
    lo = (table - hi.astype(np.float32)).astype(jnp.bfloat16)
    return hi, lo


def rfft(xs):
    n = len(xs)
    if n == 1:
        return [(xs[0], None)]
    even, odd = rfft(xs[0::2]), rfft(xs[1::2])
    half = n // 2
    out = [None] * (half + 1)
    for k in range(half // 2 + 1):
        er, ei = even[k]
        orr, oi = odd[k]
        if k == 0:
            out[0] = (er + orr, None)
            out[half] = (er - orr, None)
            continue
        c, s = np.cos(2 * np.pi * k / n), -np.sin(2 * np.pi * k / n)
        if 2 * k == half:
            out[k] = (er, -orr)
            continue
        tr, ti = cmul(orr, oi, c, s)
        out[k] = (er + tr, addo(ei, ti))
        out[half - k] = (er - tr, subo(ti, ei))
    return out


def addo(a, b):
    return b if a is None else a + b


def subo(a, b):
    return a if b is None else a - b


def cmul(r, i, c, s):
    if i is None:
        return r * c, r * s
    if abs(abs(c) - abs(s)) < 1e-9:
        if s < 0 < c:
            return (r + i) * c, (i - r) * c
        return (r - i) * c, (r + i) * c
    return r * c - i * s, r * s + i * c


def irfft(spec, n):
    if n == 1:
        return [spec[0][0]]
    half = n // 2
    even, odd = [None] * (half // 2 + 1), [None] * (half // 2 + 1)
    for k in range(half // 2 + 1):
        yr, yi = spec[k]
        if k == 0:
            hr = spec[half][0]
            even[0] = (yr + hr, None)
            odd[0] = (yr - hr, None)
            continue
        if 2 * k == half:
            even[k] = (yr + yr, None)
            odd[k] = (-(yi + yi), None)
            continue
        zr, zi = spec[half - k]
        er, ei = yr + zr, yi - zi
        dr, di = yr - zr, yi + zi
        c, s = np.cos(2 * np.pi * k / n), np.sin(2 * np.pi * k / n)
        even[k] = (er, ei)
        odd[k] = cmul(dr, di, c, s)
    ev, od = irfft(even, half), irfft(odd, half)
    out = [None] * n
    out[0::2], out[1::2] = ev, od
    return out


def cfft(xs, sign):
    n = len(xs)
    if n == 1:
        return xs
    even, odd = cfft(xs[0::2], sign), cfft(xs[1::2], sign)
    half = n // 2
    out = [None] * n
    for k in range(half):
        (er, ei), (r, i) = even[k], odd[k]
        if 4 * k == n:
            out[k] = (er + i, ei - r) if sign < 0 else (er - i, ei + r)
            out[k + half] = (er - i, ei + r) if sign < 0 else (er + i, ei - r)
            continue
        if k == 0:
            tr, ti = r, i
        else:
            tr, ti = turn(r, i, np.cos(2 * np.pi * k / n), sign * np.sin(2 * np.pi * k / n))
        out[k] = (er + tr, ei + ti)
        out[k + half] = (er - tr, ei - ti)
    return out


def turn(r, i, c, s):
    if abs(abs(c) - abs(s)) > 1e-9:
        return r * c - i * s, r * s + i * c
    if c * s > 0:
        return (r - i) * c, (r + i) * c
    return (r + i) * c, (i - r) * c


def split(v):
    hi = v.astype(jnp.bfloat16)
    lo = (v - hi.astype(jnp.float32)).astype(jnp.bfloat16)
    return hi, lo


def mm(a, b):
    return jnp.dot(a, b, preferred_element_type=jnp.float32)


def in_copies(in_ref, nat_ref, sems, c):
    size = nat_ref.shape[3]
    return [
        pltpu.make_async_copy(in_ref.at[pl.ds((2 * h + c) * size, size), b], nat_ref.at[c, h, b], sems.at[c])
        for h in range(2)
        for b in range(in_ref.shape[1])
    ]


def solve_kernel(ng, ncell, in_ref, *refs):
    (k_hbm, t_hbm, o_ref, m_ref, nat_ref, k_ref, t_ref, own_ref, store, amp, acc, work, vec, recv, sel, rows_buf, mine, marg,
     rsem, ssem, gsem, ysem, zsem, dsem, wsem, osem, orsem, msem, mrsem, lsem, csem, esem, isem, tmp, ebuf) = refs
    for copy in in_copies(in_ref, nat_ref, isem, 0) + in_copies(in_ref, nat_ref, isem, 1):
        copy.start()
    load_t = pltpu.make_async_copy(t_hbm, t_ref, csem.at[0])
    load_k = pltpu.make_async_copy(k_hbm, k_ref, csem.at[1])
    load_t.start()
    load_k.start()
    bands = in_ref.shape[1]
    flat, width = own_ref.shape
    planes = flat // ng
    groups = vec.shape[0]
    me = lax.axis_index("grid")
    band, nband = lax.axis_index("band"), lax.axis_size("band")
    chip, core = me // 2, me % 2
    sib = chip * 2 + (1 - core)
    cross = (1 - chip) * 2 + core
    far = (1 - chip) * 2 + (1 - core)
    length = nband // 2
    side, pos = band % 2, band // 2
    pair = band + 1 - 2 * side
    third = (band + nband - 1 + 2 * side) % nband
    first, last = band == 0, band == nband - 1
    ends = jnp.logical_or(first, last)
    wrap = jnp.where(first, nband - 1, 0)
    has_up, has_down = pos < length - 1, pos > 0
    up, down = jnp.where(has_up, band + 2, band), jnp.where(has_down, band - 2, band)
    mesh_id = pl.DeviceIdType.MESH
    part = planes // 2
    zrow, crow = 256, 1024
    srow = crow + 512
    yrow = srow + width

    def remote(src, dst, send, recv_sem, device):
        return pltpu.make_async_remote_copy(
            src_ref=src, dst_ref=dst, send_sem=send, recv_sem=recv_sem,
            device_id=device, device_id_type=mesh_id,
        )

    def partner(blk):
        return jnp.where(blk == 0, band, jnp.where(blk == 1, pair, third))

    def place(blk, slot):
        return jnp.where(slot == me, partner(blk), nband + blk * groups + slot)

    def piece(ref, c):
        return ref.at[pl.ds(c * part * ng, part * ng)]

    def skip(slot, at):
        return slot - (slot > at).astype(jnp.int32)

    def share(blk, lane, slot, src, target, c):
        dst = store.at[nband + blk * groups + slot]
        return remote(piece(src, c), piece(dst, c), ssem.at[lane], rsem.at[blk, skip(slot, target), c], (band, target))

    def along(block, sem, device, c, src=None):
        dst = store.at[block]
        src = dst if src is None else src
        return remote(piece(src, c), piece(dst, c), sem, gsem.at[block, c], (device, me))

    def came(block, c):
        along(block, wsem, pair, c).wait_recv()

    lane = lax.broadcasted_iota(jnp.int32, (1, 128), 1)

    def moved(value, shift, low, high, under):
        out = pltpu.roll(value, shift % 128, 1) if shift % 128 else value
        return jnp.where(jnp.logical_and(lane >= low, lane < high), out, under)

    def gather_in(read, want, blank):
        for y0 in range(8):
            chunks = [None, None, None]
            for h in range(2):
                for b in range(bands):
                    for target, start, stop, base in ((h, 0, 128, 0), (2, 128, bands * ng, 64 * h)):
                        first, final = max(start, b * ng), min(stop, b * ng + ng)
                        if first >= final:
                            continue
                        source = y0 * ng + first - b * ng
                        place_at = first - start + base
                        while first < final:
                            q, off = source // 128, source % 128
                            size = min(final - first, 128 - off)
                            under = chunks[target]
                            under = blank if under is None else under
                            chunks[target] = moved(read(b, h, q), place_at - off, place_at, place_at + size, under)
                            first, source, place_at = first + size, source + size, place_at + size
            for j, value in enumerate(chunks):
                want(j, y0, value)

    def scatter_out(read, write, blank):
        for h in range(2):
            chunks = [blank] * 3
            for y0 in range(8):
                value = read(y0)
                source, at, left = h * ng, y0 * ng, ng
                while left > 0:
                    q, off = at // 128, at % 128
                    size = min(left, 128 - off)
                    chunks[q] = moved(value, off - source, off, off + size, chunks[q])
                    source, at, left = source + size, at + size, left - size
            for q in range(3):
                write(h, q, chunks[q])

    group = flat // 8

    def packed(h, q):
        return pl.ds(q + 3 * group * h, group, stride=3)

    def spaced(y0):
        return pl.ds(y0, group, stride=8)

    def greet(device):
        pl.semaphore_signal(barrier, inc=1, device_id=device, device_id_type=mesh_id)

    barrier = pltpu.get_barrier_semaphore()
    for device in ((band, sib), (band, cross), (band, far), (pair, me)):
        greet(device)

    @pl.when(has_up)
    def _():
        greet((up, me))

    @pl.when(has_down)
    def _():
        greet((down, me))

    @pl.when(ends)
    def _():
        greet((wrap, me))

    count = 4 + has_up.astype(jnp.int32) + has_down.astype(jnp.int32) + ends.astype(jnp.int32)
    def own_copies(c):
        share(0, 1, me, own_ref, cross, c).start()
        share(0, 0, me, own_ref, sib, c).start()
        along(band, ysem.at[pos, c], pair, c, own_ref).start()

        @pl.when(has_up)
        def _():
            along(band, zsem.at[pos, c], up, c, own_ref).start()

        @pl.when(has_down)
        def _():
            along(band, dsem, down, c, own_ref).start()

    few = group // 2
    for c in range(2):
        pltpu.make_async_copy(nat_ref.at[c], nat_ref.at[c], isem.at[c]).wait()

        def put_own(j, y0, value):
            ebuf[0, j, pl.ds(c * part * ng + y0, few, stride=8), :] = value

        gather_in(
            lambda b, h, q: nat_ref[c, h, b, pl.ds(q, few, stride=3), :], put_own, jnp.zeros((few, 128), jnp.float32)
        )
        half_rows = pl.ds(c * part * ng, part * ng)
        own_ref[half_rows, :] = jnp.concatenate([ebuf[0, j, half_rows, :] for j in range(3)], axis=1)
        if c == 0:
            pl.semaphore_wait(barrier, count)
        own_copies(c)

    @pl.when(ends)
    def _():
        for c in range(2):
            along(band, wsem, wrap, c, own_ref).start()

    local = pltpu.make_async_copy(own_ref, store.at[band], lsem)
    local.start()

    def arrived(blk, slot, c):
        dst = piece(store.at[nband + blk * groups + slot], c)
        remote(dst, dst, ssem.at[0], rsem.at[blk, skip(slot, me), c], (band, sib)).wait_recv()

    def relay(blk, c):
        arrived(blk, cross, c)
        share(blk, 2, cross, store.at[nband + blk * groups + cross], sib, c).start()

    def spread(blk, c):
        came(partner(blk), c)
        share(blk, 1, me, store.at[partner(blk)], cross, c).start()
        share(blk, 0, me, store.at[partner(blk)], sib, c).start()

    def skipped(block):
        return jnp.logical_or(
            jnp.logical_and(pair == 0, block == nband - 1), jnp.logical_and(pair == nband - 1, block == 0)
        )

    def line(d, c, near, act):
        def pass_on(block, exists, on, device):
            @pl.when(exists)
            def _():
                if act == "go":
                    came(block, c)

                def one(copy):
                    copy.start() if act == "go" else copy.wait_send()

                @pl.when(jnp.logical_not(skipped(block)))
                def _():
                    one(along(block, ysem.at[block // 2, c], pair, c))

                @pl.when(on)
                def _():
                    one(along(block, zsem.at[block // 2, c], device, c))

        upward = (side == 1) == near
        pass_on(band - 2 * d, jnp.logical_and(upward, pos - d >= 0), has_up, up)
        pass_on(
            band + 2 * d, jnp.logical_and(jnp.logical_not(upward), pos + d <= length - 1), has_down, down
        )

    def serve(blk, c):
        @pl.when(blk < 2)
        def _():
            spread(blk + 1, c)

        line(blk + 1, c, True, "go")

    def ztrans(v):
        hi, lo = split(v)
        parts = []
        for h in range(2):
            a, b = (jnp.concatenate([t[:, 128 * h:128 * h + 128], t[:, 256:]], axis=1) for t in (hi, lo))
            high, low = (t_ref[pl.ds((2 * h + n) * zrow, zrow), :] for n in range(2))
            parts.append(mm(a, high) + mm(b, high) + mm(a, low))
        return jnp.concatenate([parts[0][:, :128], parts[1][:, :128], parts[0][:, 128:] + parts[1][:, 128:]], axis=1)

    def ytrans(v):
        hi, lo = split(v)
        return mm(t_ref[pl.ds(yrow, ng), pl.ds(0, 3 * ng)], jnp.concatenate([hi, lo, hi], axis=0))

    def amplitude(v):
        hi, lo = split(v)
        parts = []
        for h in range(2):
            a, b = (jnp.concatenate([t[:, 128 * h:128 * h + 128], t[:, 256:]], axis=1) for t in (hi, lo))
            parts.append(mm(a, sel[h]) + mm(b, sel[h]))
        return jnp.concatenate([parts[0][:, :128], parts[1][:, :128], parts[0][:, 128:] + parts[1][:, 128:]], axis=1)

    load_t.wait()
    for h in range(2):
        mark = (me + 1).astype(jnp.float32)
        sel[h] = jnp.where(t_ref[pl.ds(crow + zrow * h, zrow), :].astype(jnp.float32) == mark, 1.0, 0.0).astype(jnp.bfloat16)

    def transform(blk, slots, c):
        rows = pl.ds(c * part * ng, part * ng)

        @pl.when(blk == 0)
        def _():
            own = jnp.concatenate([store[place(0, slot), rows] for slot in slots], axis=0)
            out = amplitude(own).reshape(len(slots), part * ng, width)
            for n, slot in enumerate(slots):
                amp[slot, rows] = out[n]

        p = jnp.concatenate([amp[slot, rows] * store[place(blk, slot), rows] for slot in slots], axis=0)
        q = ztrans(p).reshape(len(slots), part, ng, width)
        for n, slot in enumerate(slots):
            for r in range(part):
                work[slot, c * part + r] = ytrans(q[n, r])

    def near(blk, c):
        arrived(blk, sib, c)

        @pl.when(jnp.logical_and(blk > 0, c == 1))
        def _():
            relay(blk, 0)

        transform(blk, (me, sib), c)

    def other(blk, i):
        c = i // 2

        @pl.when(jnp.logical_and(blk == 0, i == 0))
        def _():
            serve(blk, 0)
            relay(blk, 0)

        @pl.when(i == 1)
        def _():
            serve(blk, 1)
            relay(blk, 1)

        @pl.when(i % 2 == 1)
        def _():
            arrived(blk, far, c)

        @pl.when(jnp.logical_and(blk > 0, i == 2))
        def _():
            line(blk, 1, False, "go")

        transform(blk, (jnp.where(i % 2 == 0, cross, far),), c)

    def conv(vals, kern):
        n = len(vals)
        m = n // 3
        freq = {(k % 3, k % m): min(k, n - k) for k in range(n)}
        real, pairs = [], []
        for j in range(m):
            a, b, c = (vals[(m * i + 3 * j) % n] for i in range(3))
            s = b + c
            real.append(a + s)
            pairs.append((a - 0.5 * s, (c - b) * (np.sqrt(3.0) / 2)))
        spec = []
        for k, (re, im) in enumerate(rfft(real)):
            kv = kern(freq[0, k])
            spec.append((re * kv, None if im is None else im * kv))
        real = irfft(spec, m)
        spec = []
        for k, (re, im) in enumerate(cfft(pairs, -1)):
            kv = kern(freq[1, k])
            spec.append((re * kv, im * kv))
        pairs = cfft(spec, 1)
        out = [None] * n
        for j in range(m):
            u, (re, im) = real[j], pairs[j]
            base, t = u - re, im * np.sqrt(3.0)
            out[3 * j % n] = u + (re + re)
            out[(m + 3 * j) % n] = base - t
            out[(2 * m + 3 * j) % n] = base + t
        return out

    def xconv(t):
        order = [(g, h, r) for g in range(4) for h in range(2) for r in range(planes)]
        for i in range(2):
            rows = pl.ds(pl.multiple_of(t * 16 + 8 * i, 8), 8)
            res = conv([work[g, r, rows, h * 128:h * 128 + 128] for g, h, r in order],
                       lambda k: k_ref[k, rows, :])
            for (g, h, r), v in zip(order, res):
                work[g, r, rows, h * 128:h * 128 + 128] = v
        ra = pl.ds(pl.multiple_of(t * 16, 8), 8)
        rb = pl.ds(pl.multiple_of(t * 16 + 8, 8), 8)
        left = lax.broadcasted_iota(jnp.int32, (8, 128), 1) < 64

        def half(g, h, r):
            u, w = work[g, r, ra, 256:384], work[g, r, rb, 256:384]
            if h == 0:
                return jnp.where(left, u, pltpu.roll(w, 64, 1))
            return jnp.where(left, pltpu.roll(u, 64, 1), w)

        rk = pl.ds(pl.multiple_of(ng + t * 8, 8), 8)
        res = dict(zip(order, conv([half(*o) for o in order], lambda k: k_ref[k, rk, :])))
        for g in range(4):
            for r in range(planes):
                a, b = res[(g, 0, r)], res[(g, 1, r)]
                work[g, r, ra, 256:384] = jnp.where(left, a, pltpu.roll(b, 64, 1))
                work[g, r, rb, 256:384] = jnp.where(left, pltpu.roll(a, 64, 1), b)

    def push(slot):
        return remote(vec.at[slot], recv.at[me], osem, orsem.at[me], (band, slot))

    def inverse(blk, s):
        slot = ((chip + 1 - s // 2) % 2) * 2 + (core + s % 2 + s // 2) % 2
        q = jnp.concatenate([ytrans(work[slot, r]) for r in range(planes)], axis=0)
        w = ztrans(q) * store[place(blk, slot)]

        @pl.when(jnp.logical_and(blk < 2, s == 2))
        def _():
            serve(blk + 1, 0)
            line(blk + 1, 0, False, "go")

        @pl.when(blk == 0)
        def _():
            acc[slot] = w

        @pl.when(blk == 1)
        def _():
            acc[slot] += w

        @pl.when(blk == 2)
        def _():
            hi, lo = split(acc[slot] + w)
            s_tab = t_ref[pl.ds(srow, width), pl.ds(0, 128)]
            tmp[...] = -(mm(hi, s_tab) + mm(lo, s_tab))

            def put_vec(h, q, value):
                vec[slot, packed(h, q), :] = value

            scatter_out(lambda y0: tmp[spaced(y0), :], put_vec, jnp.zeros((group, 128), jnp.float32))

            @pl.when(s < 3)
            def _():
                push(slot).start()

    def block(blk, _):
        @pl.when(blk == 0)
        def _():
            local.wait()

        def fwd_near(c, _):
            near(blk, c)
            return 0

        def fwd_other(i, _):
            other(blk, i)
            return 0

        def mid(t, _):
            xconv(t)
            return 0

        def inv(s, _):
            inverse(blk, s)
            return 0

        lax.fori_loop(0, 2, fwd_near, 0)
        lax.fori_loop(0, 4, fwd_other, 0)

        @pl.when(blk == 0)
        def _():
            load_k.wait()

        lax.fori_loop(0, ng // 16, mid, 0, unroll=True)
        lax.fori_loop(0, 4, inv, 0, unroll=True)
        return 0

    lax.fori_loop(0, 3, block, 0)

    def later(d, _):
        for c in range(2):
            line(d, c, False, "go")
            line(d + 1, c, True, "go")
        return 0

    lax.fori_loop(3, length, later, 0)

    def emit(src, slot):
        return pltpu.make_async_copy(src.at[slot], o_ref.at[:, slot], esem)

    def spread_out(src, slot, n):
        def put(j, y0, value):
            ebuf[n, j, spaced(y0), :] = value

        values = {(h, q): src[slot, packed(h, q), :] for h in range(2) for q in range(3)}
        gather_in(lambda b, h, q: values[h, q], put, jnp.zeros((group, 128), jnp.float32))

    order = (me, sib, cross, far)

    def columns(block, slots):
        where = [next(n for n, s in enumerate(order) if s is slot) for slot in slots]
        parts = [[jnp.zeros((8, 128), jnp.float32) for _ in range(3)] for _ in slots]
        for r in range(flat // 8):
            for j in range(3):
                phi = store[block, pl.ds(8 * r, 8), pl.ds(128 * j, 128)]
                for n, p in zip(where, parts):
                    p[j] = p[j] + phi * ebuf[n, j, pl.ds(8 * r, 8)]
        for slot, p in zip(slots, parts):
            rows_buf[slot, pl.ds(block, 1), :] = jnp.sum(jnp.concatenate(p, axis=1), axis=0, keepdims=True)

    def ready(block):
        near_by = jnp.logical_or(block == pair, block == third)
        return jnp.logical_or(near_by, block % 2 == side)

    def early(slots):
        def body(block, _):
            @pl.when(ready(block))
            def _():
                columns(block, slots)

            return 0

        return body

    def late(block, _):
        @pl.when(jnp.logical_not(ready(block)))
        def _():
            for c in range(2):
                came(block, c)
            columns(block, (me, sib, cross, far))

        return 0

    def settle(slot):
        remote(vec.at[slot], recv.at[slot], osem, orsem.at[slot], (band, slot)).wait_recv()
        emit(recv, slot).start()

    emit(vec, me).start()
    spread_out(vec, me, 0)
    settle(sib)
    spread_out(recv, sib, 1)
    lax.fori_loop(0, nband, early((me, sib)), 0)
    settle(cross)
    spread_out(recv, cross, 2)
    lax.fori_loop(0, nband, early((cross,)), 0)
    settle(far)
    spread_out(recv, far, 3)
    lax.fori_loop(0, nband, early((far,)), 0)
    lax.fori_loop(0, nband, late, 0)

    lanes = rows_buf[...].reshape(groups * nband, width)
    left_over = lanes
    terms = jnp.zeros((groups * nband, 128), jnp.float32)
    for _ in range(3):
        hi = left_over.astype(jnp.bfloat16)
        terms += mm(hi, t_ref[pl.ds(srow, width), pl.ds(128, 128)])
        left_over = left_over - hi.astype(jnp.float32)
    terms = (terms / ncell).reshape(groups, nband, terms.shape[-1])
    each = nband // groups
    for slot in range(groups):
        total = jnp.zeros((groups, terms.shape[-1]), jnp.float32)
        for n in range(each):
            value = terms[:, slot * each + n]
            total += pltpu.roll(value, bands * n, 1) if n else value
        mine[slot] = total

    def give(slot):
        return remote(mine.at[slot], marg.at[me], msem, mrsem.at[me], (band, slot))

    for slot in (cross, far, sib):
        give(slot).start()
    pltpu.make_async_copy(o_ref, o_ref, esem).wait()
    others = pl.ds(0, groups - 1)
    remote(vec.at[others], recv.at[others], osem, orsem.at[me], (band, sib)).wait_send()
    remote(mine.at[others], marg.at[others], msem, mrsem.at[me], (band, sib)).wait_send()
    three = store.at[pl.ds(0, 3)]
    for n in range(3):
        remote(three, three, ssem.at[n], gsem.at[0, 0], (band, sib)).wait_send()
    whole = store.at[band]

    @pl.when(ends)
    def _():
        remote(whole, whole, wsem, gsem.at[0, 0], (wrap, me)).wait_send()

    @pl.when(has_down)
    def _():
        remote(whole, whole, dsem, gsem.at[0, 0], (down, me)).wait_send()

    for c in range(2):
        along(band, ysem.at[pos, c], pair, c).wait_send()

        @pl.when(has_up)
        def _():
            along(band, zsem.at[pos, c], up, c).wait_send()

    def finish_line(i, _):
        line(1 + i // 2, i % 2, True, "end")
        line(1 + i // 2, i % 2, False, "end")
        return 0

    lax.fori_loop(0, 2 * (length - 1), finish_line, 0)
    total = mine[me]
    for slot in (sib, cross, far):
        remote(mine.at[slot], marg.at[slot], msem, mrsem.at[slot], (band, slot)).wait_recv()
        total += marg[slot]
    m_ref[...] = total[:, :nband]


def lane_tables(ng, bands):
    w = bands * ng
    half, bz = [], []
    for lo, hi in ((0, 128), (128, w)):
        for h in range(2):
            half.append(np.full(hi - lo, h))
            bz.append(np.arange(lo, hi))
    half, bz = np.concatenate(half), np.concatenate(bz)
    return half, bz // ng, bz % ng


def tiles(table, half):
    out = []
    for h in range(2):
        pick = np.concatenate([np.arange(128 * h, 128 * h + 128), np.arange(256, len(half))])
        live = half[pick] == h
        out.append(np.where(live[:, None] & live[None, :], table[pick][:, pick], 0.0))
    return np.stack(out)


def solve(nat, ng, groups, nband):
    bands = nat.shape[1]
    width = 2 * bands * ng
    flat = nat.shape[0] * nat.shape[2] // (2 * ng)
    half, bnd, zed = lane_tables(ng, bands)
    ht = hartley(ng)
    th, tl = split_const(ht)
    same = (half[:, None] == half[None, :])
    zmat = np.where(same & (bnd[:, None] == bnd[None, :]), ht[zed[:, None], zed[None, :]], 0.0)
    zt = np.stack(split_const(tiles(zmat, half)), axis=1)
    ty = np.concatenate([th, th, tl], axis=1)
    cp = tiles(np.where(same & (zed[:, None] == zed[None, :]), bnd[:, None] + 1.0, 0.0), half)
    s = np.zeros((width, 128), np.float32)
    s[np.arange(width), half * ng + zed] = 1.0
    hot = np.zeros((width, 128), np.float32)
    hot[np.arange(width), bnd] = 1.0
    kv = kernel_values(ng).astype(np.float32) / np.float32(ng**3)
    kb = np.tile(kv, (1, 1, bands))
    k1 = kb[:, :, :128]
    rest = kb[:, :, 128:].reshape(kb.shape[0], ng // 16, 2, 8, 64)
    k2 = np.concatenate([rest[:, :, 0], rest[:, :, 1]], axis=-1).reshape(kb.shape[0], ng // 2, 128)
    b16 = jnp.bfloat16
    tyw = np.zeros((ng, 256), b16)
    tyw[:, : 3 * ng] = ty
    tab = [zt.reshape(-1, 256), cp.astype(b16).reshape(-1, 256), np.concatenate([s, hot], axis=1).astype(b16), tyw]
    consts = [np.concatenate([k1, k2], axis=1), np.concatenate(tab, axis=0)]
    full = (groups, flat, width)
    slim = (groups, nat.shape[0], nat.shape[2])
    f32, dma = jnp.float32, pltpu.SemaphoreType.DMA
    return pl.pallas_call(
        functools.partial(solve_kernel, ng, ng**3),
        out_shape=(
            jax.ShapeDtypeStruct(nat.shape, f32), jax.ShapeDtypeStruct((groups, nband), f32)
        ),
        in_specs=[pl.BlockSpec(memory_space=pl.ANY)] * (1 + len(consts)),
        out_specs=(pl.BlockSpec(memory_space=pl.ANY), pl.BlockSpec(memory_space=pltpu.VMEM)),
        scratch_shapes=[
            pltpu.VMEM((2, 2, bands, slim[1] // 4, 128), f32), *[pltpu.VMEM(c.shape, c.dtype) for c in consts],
            pltpu.VMEM(full[1:], f32), pltpu.VMEM((nband + 3 * groups,) + full[1:], f32),
            pltpu.VMEM(full, f32), pltpu.VMEM(full, f32), pltpu.VMEM((groups, flat // ng, ng, width), f32),
            pltpu.VMEM(slim, f32), pltpu.VMEM(slim, f32),
            pltpu.VMEM((2, 256, 256), b16), pltpu.VMEM((groups, nband, width), f32),
            pltpu.VMEM((groups, groups, 128), f32), pltpu.VMEM((groups, groups, 128), f32),
            dma((3, groups - 1, 2)), dma((3,)), dma((nband, 2)), dma((nband // 2, 2)), dma((nband // 2, 2)), dma(()), dma(()),
            dma(()), dma((groups,)), dma(()), dma((groups,)), dma(()), dma((2,)), dma(()), dma((2,)),
            pltpu.VMEM((flat, 128), f32), pltpu.VMEM((groups, 3, flat, 128), f32),
        ],
        compiler_params=pltpu.CompilerParams(
            vmem_limit_bytes=55_800_000, collective_id=0, has_side_effects=True
        ),
        cost_estimate=pl.CostEstimate(flops=10**11, bytes_accessed=10**7, transcendentals=0),
        name="solve",
    )(nat, *[jnp.asarray(c) for c in consts])


def leave_kernel(a_ref, b_ref, c_ref, d_ref, sems):
    copies = [pltpu.make_async_copy(a_ref, c_ref, sems.at[0]), pltpu.make_async_copy(b_ref, d_ref, sems.at[1])]
    for copy in copies:
        copy.start()
    for copy in copies:
        copy.wait()


def leave(a, b):
    anywhere = pl.BlockSpec(memory_space=pl.ANY)
    return pl.pallas_call(
        leave_kernel,
        out_shape=(jax.ShapeDtypeStruct(a.shape, a.dtype), jax.ShapeDtypeStruct(b.shape, b.dtype)),
        in_specs=[pl.BlockSpec(memory_space=pltpu.VMEM)] * 2,
        out_specs=(anywhere, anywhere),
        scratch_shapes=[pltpu.SemaphoreType.DMA((2,))],
        compiler_params=pltpu.CompilerParams(vmem_limit_bytes=1 << 20),
        name="leave",
    )(a, b)


def on_device(orbitals):
    groups, nband = lax.axis_size("grid"), lax.axis_size("band")
    bands, local = orbitals.shape
    ncell = local * groups
    ng = round(ncell ** (1 / 3))
    nat = orbitals.reshape(bands, local // 128, 128).transpose(1, 0, 2)
    out, marg = leave(*solve(nat, ng, groups, nband))
    vectors = out.transpose(1, 0, 2).reshape(bands, local)
    margin = marg.T
    return (vectors, margin)


def solution(mesh):
    return jax.shard_map(
        on_device,
        mesh=mesh,
        in_specs=(P("band", "grid"),),
        out_specs=(P("band", "grid"), P("grid", "band")),
        check_vma=False,
    )
```
